256 devices in a mesh: lat: 8 (over y_lo, x), lon: 32 (over y_hi, z, core).
Axes of the slice: x: 4, y: 4 (y_hi: 2, y_lo: 2; y = y_hi * 2 + y_lo), z: 8, core: 2. Of those that a mesh axis runs over, the one named last changes fastest.
Arguments:
- forcing: float32 [512, 8192], P('lat', 'lon'), may hold values from -32 to 32
- depth_east: float32 [512, 8192], P('lat', 'lon'), may hold values from 0.25 to 4
- depth_north: float32 [512, 8192], P('lat', 'lon'), may hold values from 0.25 to 4
- surface_term: float32 [512, 8192], P('lat', 'lon'), may hold values from 0.02 to 0.5
- ocean_mask: int32 [512, 8192], P('lat', 'lon'), may hold values 0 or 1
- cost_weights: float32 [8, 512, 8192], P(None, 'lat', 'lon'), may hold values from -6 to 6
Outputs:
- forcing_adjoint: float32 [8, 512, 8192], P(None, 'lat', 'lon')
- east_gradient: float32 [8, 512, 8192], P(None, 'lat', 'lon')
- north_gradient: float32 [8, 512, 8192], P(None, 'lat', 'lon')
The draws below stay inside these ranges and needn't reach their ends.
Inputs may be any that keep to these rules, and one draw needn't show every extreme that they name: `ocean_mask`: 1 marks an ocean cell, 0 a land cell.
All inputs are finite; a program needn't handle non-finite values. No bound on the sum of `ocean_mask` on one device may be relied on, other than what follows from the above.
Results may differ from the reference program's by a relative error of at most 0.00018.
Values sent between devices are 32-bit elements; how exact they have to be, the bound alone decides.
No kernel may reach another device: no remote copies, remote signals or barrier semaphores. Data moves between devices by JAX's collectives and lax.ppermute only.
A program may use at most 64 MiB of HBM per device.

```python
import math
import jax
import jax.numpy as jnp
from jax import lax

COSTS = 8
ITERS = 6
NLAT = 512
NLON = 8192


def draw_forcing(key, part):
    first = jax.random.fold_in(key, 0)
    rows = jnp.arange(NLAT, dtype=jnp.float32) / NLAT
    cols = jnp.arange(NLON, dtype=jnp.float32) / NLON
    envelope = jnp.exp(jnp.log(3.0) * (0.5 * rows[:, None] + cols[None, :]))
    rough = jnp.clip(jax.random.normal(first, (NLAT, NLON), jnp.float32), -6.0, 6.0)
    return (rough * envelope).astype(jnp.float32)


def plant(values, key, least, high):
    index_at = [jax.random.randint(jax.random.fold_in(key, axis), (), 0, length) for axis, length in enumerate(values.shape)]
    longest = values.shape.index(max(values.shape))
    beside = index_at[:longest] + [(index_at[longest] + 1) % values.shape[longest]] + index_at[longest + 1:]
    return values.at[tuple(index_at)].set(least).at[tuple(beside)].set(high)


def block_scale(own_key, extent, shards, smallest, top_value):
    def one(dim, shards_of):
        heights = jax.random.uniform(jax.random.fold_in(jax.random.fold_in(own_key, 6), dim), (shards_of,), jnp.float32, smallest / len(shards), top_value / len(shards))
        return jnp.repeat(jnp.exp(heights), extent[dim] // shards_of).reshape((-1,) + (1,) * (len(extent) - dim - 1))

    level = one(*shards[0])
    for cut in shards[1:]:
        level = level * one(*cut)
    return level


def scatter_about(key, shape, scale, reach, shards=(), held_as=jnp.bfloat16):
    entries = scale * jax.random.normal(key, shape, jnp.float32)
    if shards:
        entries = entries * block_scale(key, shape, shards, -0.22, 0.18)
    return jnp.clip(entries, -reach, reach).astype(held_as)


def setup_inputs(seed: int = 0) -> dict:
    keys = jax.random.split(jax.random.key(seed), 7)
    forcing = draw_forcing(jax.random.fold_in(keys[6], 71), 0)
    depth_east = jnp.clip(jnp.exp(math.log(4.0) - 2.7725887 * jax.random.uniform(keys[1], (NLAT, NLON), jnp.float32) ** block_scale(keys[1], (NLAT, NLON), ((0, 8), (1, 32)), -0.2, 0.2)), 0.25, 4.0)
    depth_north = jnp.clip(jnp.exp(math.log(4.0) - 2.7725887 * jax.random.uniform(keys[2], (NLAT, NLON), jnp.float32) ** block_scale(keys[2], (NLAT, NLON), ((0, 8), (1, 32)), -0.2, 0.2)), 0.25, 4.0)
    surface_term = jnp.clip(jnp.exp(math.log(0.5) - 3.218876 * jax.random.uniform(keys[3], (NLAT, NLON), jnp.float32) ** block_scale(keys[3], (NLAT, NLON), ((0, 8), (1, 32)), -0.2, 0.2)), 0.02, 0.5)
    ocean_mask = plant((jax.random.randint(keys[4], (NLAT, NLON), 0, 5) < 4).astype(jnp.int32), jax.random.fold_in(keys[4], 1), 0, 1)
    cost_weights = scatter_about(keys[5], (COSTS, NLAT, NLON), 1.0, 6.0, ((1, 8), (2, 32)), jnp.float32)
    return {"forcing": forcing, "depth_east": depth_east, "depth_north": depth_north, "surface_term": surface_term, "ocean_mask": ocean_mask, "cost_weights": cost_weights}


def faces(ocean_mask, depth_east, depth_north, surface_term):
    wet = ocean_mask.astype(jnp.float32)
    wet_east = jnp.roll(wet, -1, axis=1)
    wet_north = jnp.concatenate([wet[1:], jnp.zeros((1, wet.shape[1]), jnp.float32)], axis=0)
    east_face = depth_east * wet * wet_east
    north_face = depth_north * wet * wet_north
    west_face = jnp.roll(east_face, 1, axis=1)
    south_face = jnp.concatenate([jnp.zeros((1, wet.shape[1]), jnp.float32), north_face[:-1]], axis=0)
    base = wet * surface_term + 1.0 - wet
    return (base, east_face, west_face, north_face, south_face)

def operate(field, coefs):
    base, east_face, west_face, north_face, south_face = coefs
    east = jnp.roll(field, -1, axis=1)
    west = jnp.roll(field, 1, axis=1)
    zero_row = jnp.zeros((1, field.shape[1]), jnp.float32)
    north = jnp.concatenate([field[1:], zero_row], axis=0)
    south = jnp.concatenate([zero_row, field[:-1]], axis=0)
    return base * field + east_face * (field - east) + west_face * (field - west) + north_face * (field - north) + south_face * (field - south)

def solve(forcing, depth_east, depth_north, surface_term, ocean_mask):
    coefs = faces(ocean_mask, depth_east, depth_north, surface_term)
    diagonal = coefs[0] + coefs[1] + coefs[2] + coefs[3] + coefs[4]
    iterate = jnp.zeros_like(forcing)
    residual = forcing
    precond = residual / diagonal
    direction = precond
    norm_now = jnp.sum(residual * precond)
    for step in range(ITERS):
        image = operate(direction, coefs)
        alpha = norm_now / jnp.sum(direction * image)
        iterate = iterate + alpha * direction
        residual = residual - alpha * image
        if step < ITERS - 1:
            precond = residual / diagonal
            norm_next = jnp.sum(residual * precond)
            direction = precond + norm_next / norm_now * direction
            norm_now = norm_next
    return iterate

def reference(forcing, depth_east, depth_north, surface_term, ocean_mask, cost_weights):

    def forward(rhs_field, east_depth, north_depth):
        return solve(rhs_field, east_depth, north_depth, surface_term, ocean_mask)
    _, pullback = jax.vjp(forward, forcing, depth_east, depth_north)
    grads = lax.map(lambda weight: pullback(weight), cost_weights)
    return (grads[0], grads[1], grads[2])
```

```python
import functools

import jax
import jax.numpy as jnp
from jax import lax
from jax.experimental import pallas as pl
from jax.experimental.pallas import tpu as pltpu
from jax.sharding import PartitionSpec as P

ITERS = 6
COSTS = 8
ROWS = 64
COLS = 256
LANES = 128
WIDE = 384
DEEP = 13
SLIM = 6
EDGE = 16
FIELDS = 5
FRAME = 80
TALL = 96
MSG_W = FIELDS * EDGE
MSG_C = MSG_W + COSTS * 8
MSG = MSG_C + EDGE
N_LAM = COSTS * ITERS
N_RHS = N_LAM
N_MAT = N_LAM + ITERS
F32 = jnp.float32
HIGH = lax.Precision.HIGHEST


def lane_index(rows):
    return lax.broadcasted_iota(jnp.int32, (rows, LANES), 1)


def turn(value, amount):
    return pltpu.roll(value, amount % value.shape[1], 1)


def east_of(value):
    return pltpu.roll(value, value.shape[1] - 1, 1)


def west_of(value):
    return pltpu.roll(value, 1, 1)


def strips_kernel(f, de, dn, st, mask, w, to_east, to_west):
    lane = lane_index(ROWS)
    fields = [f[...], de[...], dn[...], st[...], mask[...].astype(F32)]
    fields += [w[n] for n in range(COSTS)]
    east = jnp.zeros((ROWS, LANES), F32)
    west = jnp.zeros((ROWS, LANES), F32)
    at = 0
    for k, field in enumerate(fields):
        wide = DEEP if k < FIELDS else SLIM
        here = (lane >= at) & (lane < at + wide)
        east = jnp.where(here, turn(field[:, LANES:], at - (LANES - wide)), east)
        west = jnp.where(here, turn(field[:, :LANES], at), west)
        at += wide
    to_east[...] = east
    to_west[...] = west


def bands_kernel(*refs):
    ins, (to_north, to_south) = refs[:-2], refs[-2:]
    for out, (f, de, dn, st, mask, w, sw, se) in ((to_north, ins[:8]), (to_south, ins[8:])):
        for k, field in enumerate((f, de, dn, st, mask)):
            out[EDGE * k : EDGE * (k + 1), :] = field[...].astype(F32)
        for n in range(COSTS):
            out[MSG_W + 8 * n : MSG_W + 8 * (n + 1), :] = w[n]
        out[MSG_C:, :LANES] = sw[...]
        out[MSG_C:, LANES:] = se[...]


def side_tile(pw, pe, at, wide):
    lane = lane_index(pw.shape[0])
    west = jnp.where(lane >= LANES - wide, turn(pw, LANES - wide - at), 0.0)
    return jnp.where(lane < wide, turn(pe, -at), west)


def forward_kernel(
    flags, f, de, dn, st, mask, w, ls, ln, sw, se,
    vecs, coefs, wside, wet, dots,
    raw, face, vec, part,
):
    own = (f, de, dn, st, mask)
    for rb in range(TALL // 8):
        at = 8 + 8 * rb
        if rb < 2:
            src, off = ls, 8 * rb
        elif rb >= 10:
            src, off = ln, 8 * rb - 80
        else:
            src, off = None, 8 * rb - 16
        if src is None:
            pw, pe = sw[off : off + 8, :], se[off : off + 8, :]
        else:
            pw = src[MSG_C + off : MSG_C + off + 8, :LANES]
            pe = src[MSG_C + off : MSG_C + off + 8, LANES:]
        for k in range(FIELDS):
            if src is None:
                body = own[k][off : off + 8, :].astype(F32)
            else:
                body = src[EDGE * k + off : EDGE * k + off + 8, :]
            side = side_tile(pw, pe, DEEP * k, DEEP)
            if k == FIELDS - 1 and src is not None:
                inside = flags[0 if rb < 2 else 1] > 0
                body = jnp.where(inside, body, 0.0)
                side = jnp.where(inside, side, 0.0)
            raw[k, at : at + 8, :COLS] = body
            raw[k, at : at + 8, COLS:] = side
        if 1 <= rb < 11:
            for n in range(COSTS):
                wside[n, 8 * rb - 8 : 8 * rb, :] = side_tile(
                    pw, pe, FIELDS * DEEP + SLIM * n, SLIM
                )
    for rb in range(TALL // 8):
        at = 8 + 8 * rb
        m = raw[4, at : at + 8, :]
        me = m * east_of(m)
        mn = m * raw[4, at + 1 : at + 9, :]
        ex = raw[1, at : at + 8, :] * me
        face[0, at : at + 8, :] = ex
        face[1, at : at + 8, :] = west_of(ex)
        face[2, at : at + 8, :] = raw[2, at : at + 8, :] * mn
        if 2 <= rb < 10:
            wet[0, 8 * rb - 16 : 8 * rb - 8, :] = me[:, :COLS]
            wet[1, 8 * rb - 16 : 8 * rb - 8, :] = mn[:, :COLS]
    for rb in range(TALL // 8):
        at = 8 + 8 * rb
        m = raw[4, at : at + 8, :]
        ex = face[0, at : at + 8, :]
        exw = face[1, at : at + 8, :]
        ey = face[2, at : at + 8, :]
        eys = face[2, at - 1 : at + 7, :]
        diag = m * raw[3, at : at + 8, :] + 1.0 - m + ex + exw + ey + eys
        inv = 1.0 / diag
        face[3, at : at + 8, :] = inv
        forcing = raw[0, at : at + 8, :]
        v0 = forcing * inv
        vec[0, at : at + 8, :] = v0
        if 1 <= rb < 11:
            to = slice(8 * rb - 8, 8 * rb)
            vecs[0, to, :] = v0
            for k, value in enumerate((ex, exw, ey, eys, inv, diag, forcing)):
                coefs[k, to, :] = value
    for j in range(ITERS):
        for rb in range(TALL // 8):
            at = 8 + 8 * rb
            v = vec[j, at : at + 8, :]
            image = (
                face[0, at : at + 8, :] * east_of(v)
                + face[1, at : at + 8, :] * west_of(v)
                + face[2, at : at + 8, :] * vec[j, at + 1 : at + 9, :]
                + face[2, at - 1 : at + 7, :] * vec[j, at - 1 : at + 7, :]
            ) * face[3, at : at + 8, :]
            new = image if j == 0 else image + image - vec[j - 1, at : at + 8, :]
            vec[j + 1, at : at + 8, :] = new
            if j < ITERS - 1 and 1 <= rb < 11:
                vecs[j + 1, 8 * rb - 8 : 8 * rb, :] = new
    count = ITERS + ITERS * (ITERS + 1) // 2
    sums = [None] * count
    for rb in range(ROWS // 8):
        for lt in range(COLS // LANES):
            lanes = slice(LANES * lt, LANES * (lt + 1))
            at = 24 + 8 * rb
            vs = [vec[j, at : at + 8, lanes] for j in range(ITERS + 1)]
            diag = coefs[5, 8 + 8 * rb : 16 + 8 * rb, lanes]
            forcing = f[8 * rb : 8 * rb + 8, lanes]
            terms = [forcing * vs[j] for j in range(ITERS)]
            for j in range(ITERS):
                turned = vs[1] if j == 0 else 0.5 * (vs[j + 1] + vs[j - 1])
                image = diag * (vs[j] - turned)
                terms += [image * vs[i] for i in range(j + 1)]
            sums = [t if a is None else a + t for a, t in zip(sums, terms)]
    part[...] = jnp.zeros((LANES, LANES), F32)
    for k in range(count):
        part[N_RHS + k : N_RHS + k + 1, :] = jnp.sum(sums[k], axis=0, keepdims=True)
    for n in range(COSTS):
        sums = [None] * ITERS
        for rb in range(ROWS // 8):
            for lt in range(COLS // LANES):
                lanes = slice(LANES * lt, LANES * (lt + 1))
                weight = w[n, 8 * rb : 8 * rb + 8, lanes]
                at = 24 + 8 * rb
                for j in range(ITERS):
                    t = weight * vec[j, at : at + 8, lanes]
                    sums[j] = t if sums[j] is None else sums[j] + t
        for j in range(ITERS):
            k = COSTS * j + n
            part[k : k + 1, :] = jnp.sum(sums[j], axis=0, keepdims=True)
    dots[...] = lax.dot_general(
        jnp.ones(dots.shape, F32), part[...], (((1,), (1,)), ((), ())),
        precision=HIGH, preferred_element_type=F32,
    )


def small_solve(total):
    wide = lambda k: jnp.broadcast_to(total[k : k + 1, :], (8, LANES))
    mat = {}
    k = N_MAT
    for j in range(ITERS):
        for i in range(j + 1):
            mat[j, i] = wide(k)
            k += 1
    low, inv = {}, []
    for j in range(ITERS):
        pivot = mat[j, j]
        for k in range(j):
            pivot = pivot - low[j, k] * mat[j, k]
        inv.append(1.0 / pivot)
        for i in range(j + 1, ITERS):
            entry = mat[i, j]
            for k in range(j):
                entry = entry - low[j, k] * mat[i, k]
            mat[i, j] = entry
            low[i, j] = entry * inv[j]

    def solve(rhs):
        y = []
        for i in range(ITERS):
            t = rhs[i]
            for k in range(i):
                t = t - low[i, k] * y[k]
            y.append(t)
        out = [None] * ITERS
        for i in range(ITERS - 1, -1, -1):
            t = y[i] * inv[i]
            for k in range(i + 1, ITERS):
                t = t - low[k, i] * out[k]
            out[i] = t
        return out

    return (
        solve([wide(N_RHS + i) for i in range(ITERS)]),
        solve([total[COSTS * j : COSTS * (j + 1), :] for j in range(ITERS)]),
    )


def triple(row):
    return jnp.concatenate([row, row, row], axis=1)


def adjoint_kernel(
    all_dots, vecs, coefs, mask, w, wside, ws, wn,
    adj, east, north,
    lam, cs, side, xs, ys, ss, ps, acc,
):
    n = pl.program_id(0)
    blocks = range(FRAME // 8)

    @pl.when(n == 0)
    def _():
        total = lax.dot_general(
            all_dots[...], jnp.ones(all_dots.shape, F32), (((0,), (0,)), ((), ())),
            precision=HIGH, preferred_element_type=F32,
        )
        c, weights = small_solve(total)
        for j in range(ITERS):
            lam[COSTS * j : COSTS * (j + 1), :] = weights[j]
            cs[8 * j : 8 * j + 8, :] = c[j]
        for rb in blocks:
            at = 8 + 8 * rb
            x = None
            for j in range(ITERS):
                t = triple(cs[8 * j : 8 * j + 8, :]) * vecs[j, 8 * rb : 8 * rb + 8, :]
                x = t if x is None else x + t
            xs[0, at : at + 8, :] = x
        for rb in blocks:
            at = 8 + 8 * rb
            x = xs[0, at : at + 8, :]
            xe, xn = east_of(x), xs[0, at + 1 : at + 9, :]
            here = slice(8 * rb, 8 * rb + 8)
            image = coefs[5, here, :] * x - (
                coefs[0, here, :] * xe + coefs[1, here, :] * west_of(x)
                + coefs[2, here, :] * xn + coefs[3, here, :] * xs[0, at - 1 : at + 7, :]
            )
            xs[1, at : at + 8, :] = coefs[6, here, :] - image
            if 1 <= rb < 9:
                own = slice(8 * rb - 8, 8 * rb)
                side[0, ITERS - 1, own, :] = xe[:, :COLS]
                side[1, ITERS - 1, own, :] = xn[:, :COLS]
                for j in range(ITERS - 1):
                    side[0, j, own, :] = east_of(vecs[j, here, :])[:, :COLS]
                    side[1, j, own, :] = vecs[j, 8 * rb + 1 : 8 * rb + 9, :COLS]

    rows = [triple(lam[pl.ds(COSTS * j + n, 1), :]) for j in range(ITERS)]

    def stencil(field, rb, ref_at):
        at = 8 + 8 * rb
        here = slice(8 * rb, 8 * rb + 8)
        fe, fw = east_of(field), west_of(field)
        fn, fs = ref_at(at + 1), ref_at(at - 1)
        image = (
            coefs[0, here, :] * fe + coefs[1, here, :] * fw
            + coefs[2, here, :] * fn + coefs[3, here, :] * fs
        )
        return image, fe, fn

    def gather(rb, field, fe, fn, slot, near, turned, first):
        at = 8 + 8 * rb
        if 1 <= rb < 9:
            own = slice(8 * rb - 8, 8 * rb)
            mid = field[:, :COLS]
            q = near[:, :COLS]
            e = mid * side[0, slot, own, :] + fe[:, :COLS] * q
            m = mid * side[1, slot, own, :] + fn[:, :COLS] * q
            acc[0, at : at + 8, :COLS] = e if first else acc[0, at : at + 8, :COLS] + e
            acc[1, at : at + 8, :COLS] = m if first else acc[1, at : at + 8, :COLS] + m
        if rb >= 1:
            d = field * turned
            acc[2, at : at + 8, :] = d if first else acc[2, at : at + 8, :] + d

    for rb in blocks:
        y = None
        for j in range(ITERS):
            t = rows[j] * vecs[j, 8 * rb : 8 * rb + 8, :]
            y = t if y is None else y + t
        ys[8 + 8 * rb : 16 + 8 * rb, :] = y
    for rb in blocks:
        at = 8 + 8 * rb
        here = slice(8 * rb, 8 * rb + 8)
        y = ys[at : at + 8, :]
        image, ye, yn = stencil(y, rb, lambda r: ys[r : r + 8, :])
        x = xs[0, at : at + 8, :]
        gather(rb, y, ye, yn, ITERS - 1, x, x, True)
        if rb == 0:
            weight = ws[...]
        elif rb == 9:
            weight = wn[...]
        else:
            weight = w[0, 8 * rb - 8 : 8 * rb, :]
        weight = jnp.concatenate([weight, wside[0, here, :]], axis=1)
        s = weight - coefs[5, here, :] * y + image
        ss[8 * rb : 8 * rb + 8, :] = s
        inv = coefs[4, here, :]
        bar = triple(cs[8 * ITERS - 8 : 8 * ITERS, :]) * s + rows[ITERS - 1] * xs[1, at : at + 8, :]
        ps[ITERS - 2, at : at + 8, :] = 2.0 * inv * bar
    for j in range(ITERS - 2, -1, -1):
        for rb in blocks:
            if j == 0 and rb == 0:
                continue
            at = 8 + 8 * rb
            here = slice(8 * rb, 8 * rb + 8)
            p = ps[j, at : at + 8, :]
            image, pe, pn = stencil(p, rb, lambda r: ps[j, r : r + 8, :])
            v = vecs[j, here, :]
            turned = vecs[1, here, :] if j == 0 else 0.5 * (vecs[j + 1, here, :] + vecs[j - 1, here, :])
            gather(rb, p, pe, pn, j, v, turned, False)
            u = triple(cs[8 * j : 8 * j + 8, :]) * ss[here, :] + rows[j] * xs[1, at : at + 8, :] + image
            scaled = coefs[4, here, :] * u
            if j >= 2:
                new = scaled + scaled
                if j + 1 <= ITERS - 2:
                    new = new - ps[j + 1, at : at + 8, :]
                ps[j - 1, at : at + 8, :] = new
            elif j == 1:
                ps[0, at : at + 8, :] = scaled - 0.5 * ps[2, at : at + 8, :]
            else:
                g = scaled - 0.5 * ps[1, at : at + 8, :]
                if rb < 9:
                    adj[0, 8 * rb - 8 : 8 * rb, :] = (ys[at : at + 8, :] + g)[:, :COLS]
                acc[2, at : at + 8, :] = acc[2, at : at + 8, :] + g * vecs[0, here, :]
    for rb in range(1, 9):
        at = 8 + 8 * rb
        own = slice(8 * rb - 8, 8 * rb)
        d = acc[2, at : at + 8, :]
        de = east_of(d)[:, :COLS]
        dn = acc[2, at + 1 : at + 9, :COLS]
        d = d[:, :COLS]
        east[0, own, :] = mask[0, own, :] * (acc[0, at : at + 8, :COLS] - d - de)
        north[0, own, :] = mask[1, own, :] * (acc[1, at : at + 8, :COLS] - d - dn)


def ring(axis, steps):
    count = lax.axis_size(axis)
    return [(source, (source + steps) % count) for source in range(count)]


def struct(*shape):
    return jax.ShapeDtypeStruct(shape, F32)


def whole():
    return pl.BlockSpec(memory_space=pltpu.VMEM)


def body(forcing, depth_east, depth_north, surface_term, ocean_mask, cost_weights):
    args = (forcing, depth_east, depth_north, surface_term, ocean_mask, cost_weights)
    lats = lax.axis_size("lat")
    devices = lats * lax.axis_size("lon")
    to_east, to_west = pl.pallas_call(
        strips_kernel,
        out_shape=(struct(ROWS, LANES), struct(ROWS, LANES)),
        name="strips",
    )(*args)
    side_w = lax.ppermute(to_east, "lon", ring("lon", 1))
    side_e = lax.ppermute(to_west, "lon", ring("lon", -1))

    def band_specs(top):
        field = pl.BlockSpec((EDGE, COLS), lambda i: (ROWS // EDGE - 1 if top else 0, 0))
        strip = pl.BlockSpec((EDGE, LANES), lambda i: (ROWS // EDGE - 1 if top else 0, 0))
        weights = pl.BlockSpec((COSTS, 8, COLS), lambda i: (0, ROWS // 8 - 1 if top else 0, 0))
        return [field] * 5 + [weights, strip, strip]

    sources = (*args, side_w, side_e)
    to_north, to_south = pl.pallas_call(
        bands_kernel,
        grid=(1,),
        in_specs=band_specs(True) + band_specs(False),
        out_specs=[pl.BlockSpec((MSG, COLS), lambda i: (0, 0))] * 2,
        out_shape=(struct(MSG, COLS), struct(MSG, COLS)),
        name="bands",
    )(*sources, *sources)
    band_s = lax.ppermute(to_north, "lat", ring("lat", 1))
    band_n = lax.ppermute(to_south, "lat", ring("lat", -1))
    row = lax.axis_index("lat")
    flags = jnp.stack([row > 0, row < lats - 1]).astype(jnp.int32)
    vecs, coefs, wside, wet, dots = pl.pallas_call(
        forward_kernel,
        in_specs=[pl.BlockSpec(memory_space=pltpu.SMEM)] + [whole()] * 10,
        out_specs=[whole()] * 5,
        out_shape=(
            struct(ITERS, FRAME, WIDE), struct(7, FRAME, WIDE),
            struct(COSTS, FRAME, LANES), struct(2, ROWS, COLS), struct(devices, LANES),
        ),
        scratch_shapes=[
            pltpu.VMEM((FIELDS, TALL + 16, WIDE), F32),
            pltpu.VMEM((4, TALL + 16, WIDE), F32),
            pltpu.VMEM((ITERS + 1, TALL + 16, WIDE), F32),
            pltpu.VMEM((LANES, LANES), F32),
        ],
        name="forward",
    )(flags, *args, band_s, band_n, side_w, side_e)
    all_dots = lax.all_to_all(dots, ("lat", "lon"), 0, 0, tiled=True)
    out_spec = pl.BlockSpec((1, ROWS, COLS), lambda n: (n, 0, 0))
    const3 = lambda a, b, c: pl.BlockSpec((a, b, c), lambda n: (0, 0, 0))
    return pl.pallas_call(
        adjoint_kernel,
        grid=(COSTS,),
        in_specs=[
            pl.BlockSpec((devices, LANES), lambda n: (0, 0)),
            const3(ITERS, FRAME, WIDE),
            const3(7, FRAME, WIDE),
            const3(2, ROWS, COLS),
            pl.BlockSpec((1, ROWS, COLS), lambda n: (n, 0, 0)),
            pl.BlockSpec((1, FRAME, LANES), lambda n: (n, 0, 0)),
            pl.BlockSpec((8, COLS), lambda n: (MSG_W // 8 + n, 0)),
            pl.BlockSpec((8, COLS), lambda n: (MSG_W // 8 + n, 0)),
        ],
        out_specs=[out_spec] * 3,
        out_shape=(struct(COSTS, ROWS, COLS),) * 3,
        scratch_shapes=[
            pltpu.VMEM((N_LAM, LANES), F32),
            pltpu.VMEM((8 * ITERS, LANES), F32),
            pltpu.VMEM((2, ITERS, ROWS, COLS), F32),
            pltpu.VMEM((2, FRAME + 16, WIDE), F32),
            pltpu.VMEM((FRAME + 16, WIDE), F32),
            pltpu.VMEM((FRAME, WIDE), F32),
            pltpu.VMEM((ITERS - 1, FRAME + 16, WIDE), F32),
            pltpu.VMEM((3, FRAME + 16, WIDE), F32),
        ],
        compiler_params=pltpu.CompilerParams(dimension_semantics=("arbitrary",)),
        name="adjoint",
    )(all_dots, vecs, coefs, wet, cost_weights, wside, band_s, band_n)


def solution(mesh):
    return jax.shard_map(
        body,
        mesh=mesh,
        in_specs=(P("lat", "lon"),) * 5 + (P(None, "lat", "lon"),),
        out_specs=(P(None, "lat", "lon"),) * 3,
        check_vma=False,
    )
```

```python
import functools

import jax
import jax.numpy as jnp
from jax import lax
from jax.experimental import pallas as pl
from jax.experimental.pallas import tpu as pltpu
from jax.sharding import PartitionSpec as P

ITERS = 6
COSTS = 8
ROWS = 64
COLS = 256
LANES = 128
WIDE = 384
DEEP = 13
SLIM = 6
EDGE = 16
FIELDS = 5
FRAME = 80
TALL = 96
MSG_W = FIELDS * EDGE
MSG_C = MSG_W + COSTS * 8
MSG = MSG_C + EDGE
N_LAM = COSTS * ITERS
N_RHS = N_LAM
N_MAT = N_LAM + ITERS
F32 = jnp.float32
HIGH = lax.Precision.HIGHEST


def lane_index(rows):
    return lax.broadcasted_iota(jnp.int32, (rows, LANES), 1)


def turn(value, amount):
    return pltpu.roll(value, amount % value.shape[1], 1)


def east_of(value):
    return pltpu.roll(value, value.shape[1] - 1, 1)


def west_of(value):
    return pltpu.roll(value, 1, 1)


def strips_kernel(f, de, dn, st, mask, w, to_east, to_west):
    lane = lane_index(ROWS)
    fields = [f[...], de[...], dn[...], st[...], mask[...].astype(F32)]
    fields += [w[n] for n in range(COSTS)]
    east = jnp.zeros((ROWS, LANES), F32)
    west = jnp.zeros((ROWS, LANES), F32)
    at = 0
    for k, field in enumerate(fields):
        wide = DEEP if k < FIELDS else SLIM
        here = (lane >= at) & (lane < at + wide)
        east = jnp.where(here, turn(field[:, LANES:], at - (LANES - wide)), east)
        west = jnp.where(here, turn(field[:, :LANES], at), west)
        at += wide
    to_east[...] = east
    to_west[...] = west


def bands_kernel(*refs):
    ins, (to_north, to_south) = refs[:-2], refs[-2:]
    for out, (f, de, dn, st, mask, w, sw, se) in ((to_north, ins[:8]), (to_south, ins[8:])):
        for k, field in enumerate((f, de, dn, st, mask)):
            out[EDGE * k : EDGE * (k + 1), :] = field[...].astype(F32)
        for n in range(COSTS):
            out[MSG_W + 8 * n : MSG_W + 8 * (n + 1), :] = w[n]
        out[MSG_C:, :LANES] = sw[...]
        out[MSG_C:, LANES:] = se[...]


def side_tile(pw, pe, at, wide):
    lane = lane_index(pw.shape[0])
    west = jnp.where(lane >= LANES - wide, turn(pw, LANES - wide - at), 0.0)
    return jnp.where(lane < wide, turn(pe, -at), west)


def forward_kernel(
    flags, f, de, dn, st, mask, w, ls, ln, sw, se,
    vecs, coefs, wside, wet, dots,
    raw, face, vec, part,
):
    own = (f, de, dn, st, mask)
    for rb in range(TALL // 8):
        at = 8 + 8 * rb
        if rb < 2:
            src, off = ls, 8 * rb
        elif rb >= 10:
            src, off = ln, 8 * rb - 80
        else:
            src, off = None, 8 * rb - 16
        if src is None:
            pw, pe = sw[off : off + 8, :], se[off : off + 8, :]
        else:
            pw = src[MSG_C + off : MSG_C + off + 8, :LANES]
            pe = src[MSG_C + off : MSG_C + off + 8, LANES:]
        for k in range(FIELDS):
            if src is None:
                body = own[k][off : off + 8, :].astype(F32)
            else:
                body = src[EDGE * k + off : EDGE * k + off + 8, :]
            side = side_tile(pw, pe, DEEP * k, DEEP)
            if k == FIELDS - 1 and src is not None:
                inside = flags[0 if rb < 2 else 1] > 0
                body = jnp.where(inside, body, 0.0)
                side = jnp.where(inside, side, 0.0)
            raw[k, at : at + 8, :COLS] = body
            raw[k, at : at + 8, COLS:] = side
        if 1 <= rb < 11:
            for n in range(COSTS):
                wside[n, 8 * rb - 8 : 8 * rb, :] = side_tile(
                    pw, pe, FIELDS * DEEP + SLIM * n, SLIM
                )
    for rb in range(TALL // 8):
        at = 8 + 8 * rb
        m = raw[4, at : at + 8, :]
        me = m * east_of(m)
        mn = m * raw[4, at + 1 : at + 9, :]
        ex = raw[1, at : at + 8, :] * me
        face[0, at : at + 8, :] = ex
        face[1, at : at + 8, :] = west_of(ex)
        face[2, at : at + 8, :] = raw[2, at : at + 8, :] * mn
        if 2 <= rb < 10:
            wet[0, 8 * rb - 16 : 8 * rb - 8, :] = me[:, :COLS]
            wet[1, 8 * rb - 16 : 8 * rb - 8, :] = mn[:, :COLS]
    for rb in range(TALL // 8):
        at = 8 + 8 * rb
        m = raw[4, at : at + 8, :]
        ex = face[0, at : at + 8, :]
        exw = face[1, at : at + 8, :]
        ey = face[2, at : at + 8, :]
        eys = face[2, at - 1 : at + 7, :]
        diag = m * raw[3, at : at + 8, :] + 1.0 - m + ex + exw + ey + eys
        inv = 1.0 / diag
        face[3, at : at + 8, :] = inv
        forcing = raw[0, at : at + 8, :]
        v0 = forcing * inv
        vec[0, at : at + 8, :] = v0
        if 1 <= rb < 11:
            to = slice(8 * rb - 8, 8 * rb)
            vecs[0, to, :] = v0
            for k, value in enumerate((ex, exw, ey, eys, inv, diag, forcing)):
                coefs[k, to, :] = value
    for j in range(ITERS):
        for rb in range(TALL // 8):
            at = 8 + 8 * rb
            v = vec[j, at : at + 8, :]
            image = (
                face[0, at : at + 8, :] * east_of(v)
                + face[1, at : at + 8, :] * west_of(v)
                + face[2, at : at + 8, :] * vec[j, at + 1 : at + 9, :]
                + face[2, at - 1 : at + 7, :] * vec[j, at - 1 : at + 7, :]
            ) * face[3, at : at + 8, :]
            new = image if j == 0 else image + image - vec[j - 1, at : at + 8, :]
            vec[j + 1, at : at + 8, :] = new
            if j < ITERS - 1 and 1 <= rb < 11:
                vecs[j + 1, 8 * rb - 8 : 8 * rb, :] = new
    count = ITERS + ITERS * (ITERS + 1) // 2
    sums = [None] * count
    for rb in range(ROWS // 8):
        for lt in range(COLS // LANES):
            lanes = slice(LANES * lt, LANES * (lt + 1))
            at = 24 + 8 * rb
            vs = [vec[j, at : at + 8, lanes] for j in range(ITERS + 1)]
            diag = coefs[5, 8 + 8 * rb : 16 + 8 * rb, lanes]
            forcing = f[8 * rb : 8 * rb + 8, lanes]
            terms = [forcing * vs[j] for j in range(ITERS)]
            for j in range(ITERS):
                turned = vs[1] if j == 0 else 0.5 * (vs[j + 1] + vs[j - 1])
                image = diag * (vs[j] - turned)
                terms += [image * vs[i] for i in range(j + 1)]
            sums = [t if a is None else a + t for a, t in zip(sums, terms)]
    part[...] = jnp.zeros((LANES, LANES), F32)
    for k in range(count):
        part[N_RHS + k : N_RHS + k + 1, :] = jnp.sum(sums[k], axis=0, keepdims=True)
    for n in range(COSTS):
        sums = [None] * ITERS
        for rb in range(ROWS // 8):
            for lt in range(COLS // LANES):
                lanes = slice(LANES * lt, LANES * (lt + 1))
                weight = w[n, 8 * rb : 8 * rb + 8, lanes]
                at = 24 + 8 * rb
                for j in range(ITERS):
                    t = weight * vec[j, at : at + 8, lanes]
                    sums[j] = t if sums[j] is None else sums[j] + t
        for j in range(ITERS):
            k = COSTS * j + n
            part[k : k + 1, :] = jnp.sum(sums[j], axis=0, keepdims=True)
    dots[...] = lax.dot_general(
        jnp.ones(dots.shape, F32), part[...], (((1,), (1,)), ((), ())),
        precision=HIGH, preferred_element_type=F32,
    )


def small_solve(total):
    wide = lambda k: jnp.broadcast_to(total[k : k + 1, :], (8, LANES))
    mat = {}
    k = N_MAT
    for j in range(ITERS):
        for i in range(j + 1):
            mat[j, i] = wide(k)
            k += 1
    low, inv = {}, []
    for j in range(ITERS):
        pivot = mat[j, j]
        for k in range(j):
            pivot = pivot - low[j, k] * mat[j, k]
        inv.append(1.0 / pivot)
        for i in range(j + 1, ITERS):
            entry = mat[i, j]
            for k in range(j):
                entry = entry - low[j, k] * mat[i, k]
            mat[i, j] = entry
            low[i, j] = entry * inv[j]

    def solve(rhs):
        y = []
        for i in range(ITERS):
            t = rhs[i]
            for k in range(i):
                t = t - low[i, k] * y[k]
            y.append(t)
        out = [None] * ITERS
        for i in range(ITERS - 1, -1, -1):
            t = y[i] * inv[i]
            for k in range(i + 1, ITERS):
                t = t - low[k, i] * out[k]
            out[i] = t
        return out

    return (
        solve([wide(N_RHS + i) for i in range(ITERS)]),
        solve([total[COSTS * j : COSTS * (j + 1), :] for j in range(ITERS)]),
    )


def triple(row):
    return jnp.concatenate([row, row, row], axis=1)


def adjoint_kernel(
    all_dots, vecs, coefs, mask, w, wside, ws, wn,
    adj, east, north,
    lam, cs, side, xs, ys, ss, ps, acc,
):
    n = pl.program_id(0)
    blocks = range(FRAME // 8)

    @pl.when(n == 0)
    def _():
        total = lax.dot_general(
            all_dots[...], jnp.ones(all_dots.shape, F32), (((0,), (0,)), ((), ())),
            precision=HIGH, preferred_element_type=F32,
        )
        c, weights = small_solve(total)
        for j in range(ITERS):
            lam[COSTS * j : COSTS * (j + 1), :] = weights[j]
            cs[8 * j : 8 * j + 8, :] = c[j]
        for rb in blocks:
            at = 8 + 8 * rb
            x = None
            for j in range(ITERS):
                t = triple(cs[8 * j : 8 * j + 8, :]) * vecs[j, 8 * rb : 8 * rb + 8, :]
                x = t if x is None else x + t
            xs[0, at : at + 8, :] = x
        for rb in blocks:
            at = 8 + 8 * rb
            x = xs[0, at : at + 8, :]
            xe, xn = east_of(x), xs[0, at + 1 : at + 9, :]
            here = slice(8 * rb, 8 * rb + 8)
            image = coefs[5, here, :] * x - (
                coefs[0, here, :] * xe + coefs[1, here, :] * west_of(x)
                + coefs[2, here, :] * xn + coefs[3, here, :] * xs[0, at - 1 : at + 7, :]
            )
            xs[1, at : at + 8, :] = coefs[6, here, :] - image
            if 1 <= rb < 9:
                own = slice(8 * rb - 8, 8 * rb)
                side[0, ITERS - 1, own, :] = xe[:, :COLS]
                side[1, ITERS - 1, own, :] = xn[:, :COLS]
                for j in range(ITERS - 1):
                    side[0, j, own, :] = east_of(vecs[j, here, :])[:, :COLS]
                    side[1, j, own, :] = vecs[j, 8 * rb + 1 : 8 * rb + 9, :COLS]

    rows = [triple(lam[pl.ds(COSTS * j + n, 1), :]) for j in range(ITERS)]

    def stencil(field, rb, ref_at):
        at = 8 + 8 * rb
        here = slice(8 * rb, 8 * rb + 8)
        fe, fw = east_of(field), west_of(field)
        fn, fs = ref_at(at + 1), ref_at(at - 1)
        image = (
            coefs[0, here, :] * fe + coefs[1, here, :] * fw
            + coefs[2, here, :] * fn + coefs[3, here, :] * fs
        )
        return image, fe, fn

    def gather(rb, field, fe, fn, slot, near, turned, first):
        at = 8 + 8 * rb
        if 1 <= rb < 9:
            own = slice(8 * rb - 8, 8 * rb)
            mid = field[:, :COLS]
            q = near[:, :COLS]
            e = mid * side[0, slot, own, :] + fe[:, :COLS] * q
            m = mid * side[1, slot, own, :] + fn[:, :COLS] * q
            acc[0, at : at + 8, :COLS] = e if first else acc[0, at : at + 8, :COLS] + e
            acc[1, at : at + 8, :COLS] = m if first else acc[1, at : at + 8, :COLS] + m
        if rb >= 1:
            d = field * turned
            acc[2, at : at + 8, :] = d if first else acc[2, at : at + 8, :] + d

    for rb in blocks:
        y = None
        for j in range(ITERS):
            t = rows[j] * vecs[j, 8 * rb : 8 * rb + 8, :]
            y = t if y is None else y + t
        ys[8 + 8 * rb : 16 + 8 * rb, :] = y
    for rb in blocks:
        at = 8 + 8 * rb
        here = slice(8 * rb, 8 * rb + 8)
        y = ys[at : at + 8, :]
        image, ye, yn = stencil(y, rb, lambda r: ys[r : r + 8, :])
        x = xs[0, at : at + 8, :]
        gather(rb, y, ye, yn, ITERS - 1, x, x, True)
        if rb == 0:
            weight = ws[...]
        elif rb == 9:
            weight = wn[...]
        else:
            weight = w[0, 8 * rb - 8 : 8 * rb, :]
        weight = jnp.concatenate([weight, wside[0, here, :]], axis=1)
        s = weight - coefs[5, here, :] * y + image
        ss[8 * rb : 8 * rb + 8, :] = s
        inv = coefs[4, here, :]
        bar = triple(cs[8 * ITERS - 8 : 8 * ITERS, :]) * s + rows[ITERS - 1] * xs[1, at : at + 8, :]
        ps[ITERS - 2, at : at + 8, :] = 2.0 * inv * bar
    for j in range(ITERS - 2, -1, -1):
        for rb in blocks:
            if j == 0 and rb == 0:
                continue
            at = 8 + 8 * rb
            here = slice(8 * rb, 8 * rb + 8)
            p = ps[j, at : at + 8, :]
            image, pe, pn = stencil(p, rb, lambda r: ps[j, r : r + 8, :])
            v = vecs[j, here, :]
            turned = vecs[1, here, :] if j == 0 else 0.5 * (vecs[j + 1, here, :] + vecs[j - 1, here, :])
            gather(rb, p, pe, pn, j, v, turned, False)
            u = triple(cs[8 * j : 8 * j + 8, :]) * ss[here, :] + rows[j] * xs[1, at : at + 8, :] + image
            scaled = coefs[4, here, :] * u
            if j >= 2:
                new = scaled + scaled
                if j + 1 <= ITERS - 2:
                    new = new - ps[j + 1, at : at + 8, :]
                ps[j - 1, at : at + 8, :] = new
            elif j == 1:
                ps[0, at : at + 8, :] = scaled - 0.5 * ps[2, at : at + 8, :]
            else:
                g = scaled - 0.5 * ps[1, at : at + 8, :]
                if rb < 9:
                    adj[0, 8 * rb - 8 : 8 * rb, :] = (ys[at : at + 8, :] + g)[:, :COLS]
                acc[2, at : at + 8, :] = acc[2, at : at + 8, :] + g * vecs[0, here, :]
    for rb in range(1, 9):
        at = 8 + 8 * rb
        own = slice(8 * rb - 8, 8 * rb)
        d = acc[2, at : at + 8, :]
        de = east_of(d)[:, :COLS]
        dn = acc[2, at + 1 : at + 9, :COLS]
        d = d[:, :COLS]
        east[0, own, :] = mask[0, own, :] * (acc[0, at : at + 8, :COLS] - d - de)
        north[0, own, :] = mask[1, own, :] * (acc[1, at : at + 8, :COLS] - d - dn)


def ring(axis, steps):
    count = lax.axis_size(axis)
    return [(source, (source + steps) % count) for source in range(count)]


def struct(*shape):
    return jax.ShapeDtypeStruct(shape, F32)


def whole():
    return pl.BlockSpec(memory_space=pltpu.VMEM)


def body(forcing, depth_east, depth_north, surface_term, ocean_mask, cost_weights):
    args = (forcing, depth_east, depth_north, surface_term, ocean_mask, cost_weights)
    lats = lax.axis_size("lat")
    devices = lats * lax.axis_size("lon")
    to_east, to_west = pl.pallas_call(
        strips_kernel,
        out_shape=(struct(ROWS, LANES), struct(ROWS, LANES)),
        compiler_params=pltpu.CompilerParams(vmem_limit_bytes=4 << 20),
        name="strips",
    )(*args)
    side_w = lax.ppermute(to_east, "lon", ring("lon", 1))
    side_e = lax.ppermute(to_west, "lon", ring("lon", -1))

    def band_specs(top):
        field = pl.BlockSpec((EDGE, COLS), lambda i: (ROWS // EDGE - 1 if top else 0, 0))
        strip = pl.BlockSpec((EDGE, LANES), lambda i: (ROWS // EDGE - 1 if top else 0, 0))
        weights = pl.BlockSpec((COSTS, 8, COLS), lambda i: (0, ROWS // 8 - 1 if top else 0, 0))
        return [field] * 5 + [weights, strip, strip]

    sources = (*args, side_w, side_e)
    to_north, to_south = pl.pallas_call(
        bands_kernel,
        grid=(1,),
        in_specs=band_specs(True) + band_specs(False),
        out_specs=[pl.BlockSpec((MSG, COLS), lambda i: (0, 0))] * 2,
        out_shape=(struct(MSG, COLS), struct(MSG, COLS)),
        compiler_params=pltpu.CompilerParams(vmem_limit_bytes=4 << 20),
        name="bands",
    )(*sources, *sources)
    band_s = lax.ppermute(to_north, "lat", ring("lat", 1))
    band_n = lax.ppermute(to_south, "lat", ring("lat", -1))
    row = lax.axis_index("lat")
    flags = jnp.stack([row > 0, row < lats - 1]).astype(jnp.int32)
    vecs, coefs, wside, wet, dots = pl.pallas_call(
        forward_kernel,
        in_specs=[pl.BlockSpec(memory_space=pltpu.SMEM)] + [whole()] * 10,
        out_specs=[whole()] * 5,
        out_shape=(
            struct(ITERS, FRAME, WIDE), struct(7, FRAME, WIDE),
            struct(COSTS, FRAME, LANES), struct(2, ROWS, COLS), struct(devices, LANES),
        ),
        scratch_shapes=[
            pltpu.VMEM((FIELDS, TALL + 16, WIDE), F32),
            pltpu.VMEM((4, TALL + 16, WIDE), F32),
            pltpu.VMEM((ITERS + 1, TALL + 16, WIDE), F32),
            pltpu.VMEM((LANES, LANES), F32),
        ],
        compiler_params=pltpu.CompilerParams(vmem_limit_bytes=12 << 20),
        name="forward",
    )(flags, *args, band_s, band_n, side_w, side_e)
    all_dots = lax.all_to_all(dots, ("lat", "lon"), 0, 0, tiled=True)
    out_spec = pl.BlockSpec((1, ROWS, COLS), lambda n: (n, 0, 0))
    const3 = lambda a, b, c: pl.BlockSpec((a, b, c), lambda n: (0, 0, 0))
    return pl.pallas_call(
        adjoint_kernel,
        grid=(COSTS,),
        in_specs=[
            pl.BlockSpec((devices, LANES), lambda n: (0, 0)),
            const3(ITERS, FRAME, WIDE),
            const3(7, FRAME, WIDE),
            const3(2, ROWS, COLS),
            pl.BlockSpec((1, ROWS, COLS), lambda n: (n, 0, 0)),
            pl.BlockSpec((1, FRAME, LANES), lambda n: (n, 0, 0)),
            pl.BlockSpec((8, COLS), lambda n: (MSG_W // 8 + n, 0)),
            pl.BlockSpec((8, COLS), lambda n: (MSG_W // 8 + n, 0)),
        ],
        out_specs=[out_spec] * 3,
        out_shape=(struct(COSTS, ROWS, COLS),) * 3,
        scratch_shapes=[
            pltpu.VMEM((N_LAM, LANES), F32),
            pltpu.VMEM((8 * ITERS, LANES), F32),
            pltpu.VMEM((2, ITERS, ROWS, COLS), F32),
            pltpu.VMEM((2, FRAME + 16, WIDE), F32),
            pltpu.VMEM((FRAME + 16, WIDE), F32),
            pltpu.VMEM((FRAME, WIDE), F32),
            pltpu.VMEM((ITERS - 1, FRAME + 16, WIDE), F32),
            pltpu.VMEM((3, FRAME + 16, WIDE), F32),
        ],
        compiler_params=pltpu.CompilerParams(dimension_semantics=("arbitrary",), vmem_limit_bytes=14 << 20),
        name="adjoint",
    )(all_dots, vecs, coefs, wet, cost_weights, wside, band_s, band_n)


def solution(mesh):
    return jax.shard_map(
        body,
        mesh=mesh,
        in_specs=(P("lat", "lon"),) * 5 + (P(None, "lat", "lon"),),
        out_specs=(P(None, "lat", "lon"),) * 3,
        check_vma=False,
    )
```

```python
import functools

import jax
import jax.numpy as jnp
from jax import lax
from jax.experimental import pallas as pl
from jax.experimental.pallas import tpu as pltpu
from jax.sharding import PartitionSpec as P

ITERS = 6
COSTS = 8
ROWS = 64
COLS = 256
LANES = 128
WIDE = 384
DEEP = 13
SLIM = 6
EDGE = 16
FIELDS = 5
FRAME = 80
TALL = 96
MSG_W = FIELDS * EDGE
MSG = MSG_W + COSTS * 8
N_LAM = COSTS * ITERS
N_RHS = N_LAM
N_MAT = N_LAM + ITERS
F32 = jnp.float32
HIGH = lax.Precision.HIGHEST


def lane_index(rows):
    return lax.broadcasted_iota(jnp.int32, (rows, LANES), 1)


def turn(value, amount):
    return pltpu.roll(value, amount % value.shape[1], 1)


def east_of(value):
    return pltpu.roll(value, value.shape[1] - 1, 1)


def west_of(value):
    return pltpu.roll(value, 1, 1)


def pack(rows, tiles):
    lane = lane_index(rows)
    out = jnp.zeros((rows, LANES), F32)
    at = 0
    for tile, first, wide in tiles:
        if tile is not None:
            here = (lane >= at) & (lane < at + wide)
            out = jnp.where(here, turn(tile, at - first), out)
        at += wide
    return out


def bands_kernel(f, de, dn, st, mask, w, to_north, to_south, whole_mask, sems):
    copies = []
    for side, out in enumerate((to_north, to_south)):
        low = ROWS - EDGE if side == 0 else 0
        rows = pl.ds(low, EDGE)
        for k, field in enumerate((f, de, dn, st)):
            copies.append((field.at[rows, :], out.at[pl.ds(EDGE * k, EDGE), :]))
        copies.append((mask.at[rows, :], whole_mask.at[side]))
        low = ROWS - 8 if side == 0 else 0
        for n in range(COSTS):
            copies.append((w.at[n, pl.ds(low, 8), :], out.at[pl.ds(MSG_W + 8 * n, 8), :]))
    copies = [
        pltpu.make_async_copy(src, dst, sems.at[i]) for i, (src, dst) in enumerate(copies)
    ]
    for copy in copies:
        copy.start()
    for copy in copies:
        copy.wait()
    to_north[MSG_W - EDGE : MSG_W, :] = whole_mask[0].astype(F32)
    to_south[MSG_W - EDGE : MSG_W, :] = whole_mask[1].astype(F32)


def strips_kernel(f, de, dn, st, mask, w, east, west):
    fields = [f[...], de[...], dn[...], st[...], mask[...].astype(F32)]
    right = [(v[:, LANES:], LANES - DEEP, DEEP) for v in fields]
    left = [(v[:, :LANES], 0, DEEP) for v in fields]
    right += [(w[n, :, LANES:], LANES - SLIM, SLIM) for n in range(COSTS)]
    left += [(w[n, :, :LANES], 0, SLIM) for n in range(COSTS)]
    east[...] = pack(ROWS, right)
    west[...] = pack(ROWS, left)


def corners_kernel(east, west, bs, bn, to_east, to_west):
    for own, out, lanes, first in ((east, to_east, slice(LANES, COLS), True), (west, to_west, slice(0, LANES), False)):
        out[EDGE : EDGE + ROWS, :] = own[...]
        for band, low, slim in ((bs, 0, 1), (bn, EDGE + ROWS, 0)):
            for half in range(2):
                tiles = []
                for k in range(FIELDS):
                    at = EDGE * k + 8 * half
                    tiles.append((band[at : at + 8, lanes], LANES - DEEP if first else 0, DEEP))
                for n in range(COSTS):
                    at = MSG_W + 8 * n
                    tile = band[at : at + 8, lanes] if half == slim else None
                    tiles.append((tile, LANES - SLIM if first else 0, SLIM))
                out[low + 8 * half : low + 8 * half + 8, :] = pack(8, tiles)


def side_tile(pw, pe, at, wide):
    lane = lane_index(pw.shape[0])
    west = jnp.where(lane >= LANES - wide, turn(pw, LANES - wide - at), 0.0)
    return jnp.where(lane < wide, turn(pe, -at), west)


def forward_kernel(
    flags, f, de, dn, st, mask, w, ls, ln, sw, se,
    vecs, coefs, wside, wet, dots,
    raw, face, vec, part,
):
    own = (f, de, dn, st, mask)
    for rb in range(TALL // 8):
        at = 8 + 8 * rb
        if rb < 2:
            src, off = ls, 8 * rb
        elif rb >= 10:
            src, off = ln, 8 * rb - 80
        else:
            src, off = None, 8 * rb - 16
        pw, pe = sw[8 * rb : 8 * rb + 8, :], se[8 * rb : 8 * rb + 8, :]
        for k in range(FIELDS):
            if src is None:
                body = own[k][off : off + 8, :].astype(F32)
            else:
                body = src[EDGE * k + off : EDGE * k + off + 8, :]
            side = side_tile(pw, pe, DEEP * k, DEEP)
            if k == FIELDS - 1 and src is not None:
                inside = flags[0 if rb < 2 else 1] > 0
                body = jnp.where(inside, body, 0.0)
                side = jnp.where(inside, side, 0.0)
            raw[k, at : at + 8, :COLS] = body
            raw[k, at : at + 8, COLS:] = side
        if 1 <= rb < 11:
            for n in range(COSTS):
                wside[n, 8 * rb - 8 : 8 * rb, :] = side_tile(
                    pw, pe, FIELDS * DEEP + SLIM * n, SLIM
                )
    for rb in range(TALL // 8):
        at = 8 + 8 * rb
        m = raw[4, at : at + 8, :]
        me = m * east_of(m)
        mn = m * raw[4, at + 1 : at + 9, :]
        ex = raw[1, at : at + 8, :] * me
        face[0, at : at + 8, :] = ex
        face[1, at : at + 8, :] = west_of(ex)
        face[2, at : at + 8, :] = raw[2, at : at + 8, :] * mn
        if 2 <= rb < 10:
            wet[0, 8 * rb - 16 : 8 * rb - 8, :] = me[:, :COLS]
            wet[1, 8 * rb - 16 : 8 * rb - 8, :] = mn[:, :COLS]
    for rb in range(TALL // 8):
        at = 8 + 8 * rb
        m = raw[4, at : at + 8, :]
        ex = face[0, at : at + 8, :]
        exw = face[1, at : at + 8, :]
        ey = face[2, at : at + 8, :]
        eys = face[2, at - 1 : at + 7, :]
        diag = m * raw[3, at : at + 8, :] + 1.0 - m + ex + exw + ey + eys
        inv = 1.0 / diag
        face[3, at : at + 8, :] = inv
        forcing = raw[0, at : at + 8, :]
        v0 = forcing * inv
        vec[0, at : at + 8, :] = v0
        if 1 <= rb < 11:
            to = slice(8 * rb - 8, 8 * rb)
            vecs[0, to, :] = v0
            for k, value in enumerate((ex, exw, ey, eys, inv, diag, forcing)):
                coefs[k, to, :] = value
    for j in range(ITERS):
        for rb in range(TALL // 8):
            at = 8 + 8 * rb
            v = vec[j, at : at + 8, :]
            image = (
                face[0, at : at + 8, :] * east_of(v)
                + face[1, at : at + 8, :] * west_of(v)
                + face[2, at : at + 8, :] * vec[j, at + 1 : at + 9, :]
                + face[2, at - 1 : at + 7, :] * vec[j, at - 1 : at + 7, :]
            ) * face[3, at : at + 8, :]
            new = image if j == 0 else image + image - vec[j - 1, at : at + 8, :]
            vec[j + 1, at : at + 8, :] = new
            if j < ITERS - 1 and 1 <= rb < 11:
                vecs[j + 1, 8 * rb - 8 : 8 * rb, :] = new
    count = ITERS + ITERS * (ITERS + 1) // 2
    sums = [None] * count
    for rb in range(ROWS // 8):
        for lt in range(COLS // LANES):
            lanes = slice(LANES * lt, LANES * (lt + 1))
            at = 24 + 8 * rb
            vs = [vec[j, at : at + 8, lanes] for j in range(ITERS + 1)]
            diag = coefs[5, 8 + 8 * rb : 16 + 8 * rb, lanes]
            forcing = f[8 * rb : 8 * rb + 8, lanes]
            terms = [forcing * vs[j] for j in range(ITERS)]
            for j in range(ITERS):
                turned = vs[1] if j == 0 else 0.5 * (vs[j + 1] + vs[j - 1])
                image = diag * (vs[j] - turned)
                terms += [image * vs[i] for i in range(j + 1)]
            sums = [t if a is None else a + t for a, t in zip(sums, terms)]
    part[...] = jnp.zeros((LANES, LANES), F32)
    for k in range(count):
        part[N_RHS + k : N_RHS + k + 1, :] = jnp.sum(sums[k], axis=0, keepdims=True)
    for n in range(COSTS):
        sums = [None] * ITERS
        for rb in range(ROWS // 8):
            for lt in range(COLS // LANES):
                lanes = slice(LANES * lt, LANES * (lt + 1))
                weight = w[n, 8 * rb : 8 * rb + 8, lanes]
                at = 24 + 8 * rb
                for j in range(ITERS):
                    t = weight * vec[j, at : at + 8, lanes]
                    sums[j] = t if sums[j] is None else sums[j] + t
        for j in range(ITERS):
            k = COSTS * j + n
            part[k : k + 1, :] = jnp.sum(sums[j], axis=0, keepdims=True)
    dots[...] = lax.dot_general(
        jnp.ones(dots.shape, F32), part[...], (((1,), (1,)), ((), ())),
        precision=HIGH, preferred_element_type=F32,
    )


def small_solve(total):
    wide = lambda k: jnp.broadcast_to(total[k : k + 1, :], (8, LANES))
    mat = {}
    k = N_MAT
    for j in range(ITERS):
        for i in range(j + 1):
            mat[j, i] = wide(k)
            k += 1
    low, inv = {}, []
    for j in range(ITERS):
        pivot = mat[j, j]
        for k in range(j):
            pivot = pivot - low[j, k] * mat[j, k]
        inv.append(1.0 / pivot)
        for i in range(j + 1, ITERS):
            entry = mat[i, j]
            for k in range(j):
                entry = entry - low[j, k] * mat[i, k]
            mat[i, j] = entry
            low[i, j] = entry * inv[j]

    def solve(rhs):
        y = []
        for i in range(ITERS):
            t = rhs[i]
            for k in range(i):
                t = t - low[i, k] * y[k]
            y.append(t)
        out = [None] * ITERS
        for i in range(ITERS - 1, -1, -1):
            t = y[i] * inv[i]
            for k in range(i + 1, ITERS):
                t = t - low[k, i] * out[k]
            out[i] = t
        return out

    return (
        solve([wide(N_RHS + i) for i in range(ITERS)]),
        solve([total[COSTS * j : COSTS * (j + 1), :] for j in range(ITERS)]),
    )


def triple(row):
    return jnp.concatenate([row, row, row], axis=1)


def adjoint_kernel(
    all_dots, vecs, coefs, mask, w, wside, ws, wn,
    adj, east, north,
    lam, cs, side, xs, ys, ss, ps, acc,
):
    n = pl.program_id(0)
    blocks = range(FRAME // 8)

    @pl.when(n == 0)
    def _():
        total = lax.dot_general(
            all_dots[...], jnp.ones(all_dots.shape, F32), (((0,), (0,)), ((), ())),
            precision=HIGH, preferred_element_type=F32,
        )
        c, weights = small_solve(total)
        for j in range(ITERS):
            lam[COSTS * j : COSTS * (j + 1), :] = weights[j]
            cs[8 * j : 8 * j + 8, :] = c[j]
        for rb in blocks:
            at = 8 + 8 * rb
            x = None
            for j in range(ITERS):
                t = triple(cs[8 * j : 8 * j + 8, :]) * vecs[j, 8 * rb : 8 * rb + 8, :]
                x = t if x is None else x + t
            xs[0, at : at + 8, :] = x
        for rb in blocks:
            at = 8 + 8 * rb
            x = xs[0, at : at + 8, :]
            xe, xn = east_of(x), xs[0, at + 1 : at + 9, :]
            here = slice(8 * rb, 8 * rb + 8)
            image = coefs[5, here, :] * x - (
                coefs[0, here, :] * xe + coefs[1, here, :] * west_of(x)
                + coefs[2, here, :] * xn + coefs[3, here, :] * xs[0, at - 1 : at + 7, :]
            )
            xs[1, at : at + 8, :] = coefs[6, here, :] - image
            if 1 <= rb < 9:
                own = slice(8 * rb - 8, 8 * rb)
                side[0, ITERS - 1, own, :] = xe[:, :COLS]
                side[1, ITERS - 1, own, :] = xn[:, :COLS]
                for j in range(ITERS - 1):
                    side[0, j, own, :] = east_of(vecs[j, here, :])[:, :COLS]
                    side[1, j, own, :] = vecs[j, 8 * rb + 1 : 8 * rb + 9, :COLS]

    rows = [triple(lam[pl.ds(COSTS * j + n, 1), :]) for j in range(ITERS)]

    def stencil(field, rb, ref_at):
        at = 8 + 8 * rb
        here = slice(8 * rb, 8 * rb + 8)
        fe, fw = east_of(field), west_of(field)
        fn, fs = ref_at(at + 1), ref_at(at - 1)
        image = (
            coefs[0, here, :] * fe + coefs[1, here, :] * fw
            + coefs[2, here, :] * fn + coefs[3, here, :] * fs
        )
        return image, fe, fn

    def gather(rb, field, fe, fn, slot, near, turned, first):
        at = 8 + 8 * rb
        if 1 <= rb < 9:
            own = slice(8 * rb - 8, 8 * rb)
            mid = field[:, :COLS]
            q = near[:, :COLS]
            e = mid * side[0, slot, own, :] + fe[:, :COLS] * q
            m = mid * side[1, slot, own, :] + fn[:, :COLS] * q
            acc[0, at : at + 8, :COLS] = e if first else acc[0, at : at + 8, :COLS] + e
            acc[1, at : at + 8, :COLS] = m if first else acc[1, at : at + 8, :COLS] + m
        if rb >= 1:
            d = field * turned
            acc[2, at : at + 8, :] = d if first else acc[2, at : at + 8, :] + d

    for rb in blocks:
        y = None
        for j in range(ITERS):
            t = rows[j] * vecs[j, 8 * rb : 8 * rb + 8, :]
            y = t if y is None else y + t
        ys[8 + 8 * rb : 16 + 8 * rb, :] = y
    for rb in blocks:
        at = 8 + 8 * rb
        here = slice(8 * rb, 8 * rb + 8)
        y = ys[at : at + 8, :]
        image, ye, yn = stencil(y, rb, lambda r: ys[r : r + 8, :])
        x = xs[0, at : at + 8, :]
        gather(rb, y, ye, yn, ITERS - 1, x, x, True)
        if rb == 0:
            weight = ws[...]
        elif rb == 9:
            weight = wn[...]
        else:
            weight = w[0, 8 * rb - 8 : 8 * rb, :]
        weight = jnp.concatenate([weight, wside[0, here, :]], axis=1)
        s = weight - coefs[5, here, :] * y + image
        ss[8 * rb : 8 * rb + 8, :] = s
        inv = coefs[4, here, :]
        bar = triple(cs[8 * ITERS - 8 : 8 * ITERS, :]) * s + rows[ITERS - 1] * xs[1, at : at + 8, :]
        ps[ITERS - 2, at : at + 8, :] = 2.0 * inv * bar
    for j in range(ITERS - 2, -1, -1):
        for rb in blocks:
            if j == 0 and rb == 0:
                continue
            at = 8 + 8 * rb
            here = slice(8 * rb, 8 * rb + 8)
            p = ps[j, at : at + 8, :]
            image, pe, pn = stencil(p, rb, lambda r: ps[j, r : r + 8, :])
            v = vecs[j, here, :]
            turned = vecs[1, here, :] if j == 0 else 0.5 * (vecs[j + 1, here, :] + vecs[j - 1, here, :])
            gather(rb, p, pe, pn, j, v, turned, False)
            u = triple(cs[8 * j : 8 * j + 8, :]) * ss[here, :] + rows[j] * xs[1, at : at + 8, :] + image
            scaled = coefs[4, here, :] * u
            if j >= 2:
                new = scaled + scaled
                if j + 1 <= ITERS - 2:
                    new = new - ps[j + 1, at : at + 8, :]
                ps[j - 1, at : at + 8, :] = new
            elif j == 1:
                ps[0, at : at + 8, :] = scaled - 0.5 * ps[2, at : at + 8, :]
            else:
                g = scaled - 0.5 * ps[1, at : at + 8, :]
                if rb < 9:
                    adj[0, 8 * rb - 8 : 8 * rb, :] = (ys[at : at + 8, :] + g)[:, :COLS]
                acc[2, at : at + 8, :] = acc[2, at : at + 8, :] + g * vecs[0, here, :]
    for rb in range(1, 9):
        at = 8 + 8 * rb
        own = slice(8 * rb - 8, 8 * rb)
        d = acc[2, at : at + 8, :]
        de = east_of(d)[:, :COLS]
        dn = acc[2, at + 1 : at + 9, :COLS]
        d = d[:, :COLS]
        east[0, own, :] = mask[0, own, :] * (acc[0, at : at + 8, :COLS] - d - de)
        north[0, own, :] = mask[1, own, :] * (acc[1, at : at + 8, :COLS] - d - dn)


def ring(axis, steps):
    count = lax.axis_size(axis)
    return [(source, (source + steps) % count) for source in range(count)]


def struct(*shape):
    return jax.ShapeDtypeStruct(shape, F32)


def whole():
    return pl.BlockSpec(memory_space=pltpu.VMEM)


def body(forcing, depth_east, depth_north, surface_term, ocean_mask, cost_weights):
    args = (forcing, depth_east, depth_north, surface_term, ocean_mask, cost_weights)
    lats = lax.axis_size("lat")
    devices = lats * lax.axis_size("lon")
    small = pltpu.CompilerParams(vmem_limit_bytes=4 << 20)
    to_north, to_south = pl.pallas_call(
        bands_kernel,
        in_specs=[pl.BlockSpec(memory_space=pltpu.HBM)] * 6,
        out_specs=[whole()] * 2,
        out_shape=(struct(MSG, COLS),) * 2,
        scratch_shapes=[
            pltpu.VMEM((2, EDGE, COLS), jnp.int32),
            pltpu.SemaphoreType.DMA((2 * (FIELDS + COSTS),)),
        ],
        compiler_params=small,
        name="bands",
    )(*[pltpu.with_memory_space_constraint(arg, pltpu.HBM) for arg in args])
    band_s = lax.ppermute(to_north, "lat", ring("lat", 1))
    band_n = lax.ppermute(to_south, "lat", ring("lat", -1))
    east, west = pl.pallas_call(
        strips_kernel,
        in_specs=[whole()] * 6,
        out_specs=[whole()] * 2,
        out_shape=(struct(ROWS, LANES),) * 2,
        compiler_params=small,
        name="strips",
    )(*args)
    to_east, to_west = pl.pallas_call(
        corners_kernel,
        in_specs=[whole()] * 4,
        out_specs=[whole()] * 2,
        out_shape=(struct(TALL, LANES),) * 2,
        compiler_params=small,
        name="corners",
    )(east, west, band_s, band_n)
    side_w = lax.ppermute(to_east, "lon", ring("lon", 1))
    side_e = lax.ppermute(to_west, "lon", ring("lon", -1))
    row = lax.axis_index("lat")
    flags = jnp.stack([row > 0, row < lats - 1]).astype(jnp.int32)
    vecs, coefs, wside, wet, dots = pl.pallas_call(
        forward_kernel,
        in_specs=[pl.BlockSpec(memory_space=pltpu.SMEM)] + [whole()] * 10,
        out_specs=[whole()] * 5,
        out_shape=(
            struct(ITERS, FRAME, WIDE), struct(7, FRAME, WIDE),
            struct(COSTS, FRAME, LANES), struct(2, ROWS, COLS), struct(devices, LANES),
        ),
        scratch_shapes=[
            pltpu.VMEM((FIELDS, TALL + 16, WIDE), F32),
            pltpu.VMEM((4, TALL + 16, WIDE), F32),
            pltpu.VMEM((ITERS + 1, TALL + 16, WIDE), F32),
            pltpu.VMEM((LANES, LANES), F32),
        ],
        compiler_params=pltpu.CompilerParams(vmem_limit_bytes=12 << 20),
        name="forward",
    )(flags, *args, band_s, band_n, side_w, side_e)
    all_dots = lax.all_to_all(dots, ("lat", "lon"), 0, 0, tiled=True)
    out_spec = pl.BlockSpec((1, ROWS, COLS), lambda n: (n, 0, 0))
    const3 = lambda a, b, c: pl.BlockSpec((a, b, c), lambda n: (0, 0, 0))
    return pl.pallas_call(
        adjoint_kernel,
        grid=(COSTS,),
        in_specs=[
            pl.BlockSpec((devices, LANES), lambda n: (0, 0)),
            const3(ITERS, FRAME, WIDE),
            const3(7, FRAME, WIDE),
            const3(2, ROWS, COLS),
            pl.BlockSpec((1, ROWS, COLS), lambda n: (n, 0, 0)),
            pl.BlockSpec((1, FRAME, LANES), lambda n: (n, 0, 0)),
            pl.BlockSpec((8, COLS), lambda n: (MSG_W // 8 + n, 0)),
            pl.BlockSpec((8, COLS), lambda n: (MSG_W // 8 + n, 0)),
        ],
        out_specs=[out_spec] * 3,
        out_shape=(struct(COSTS, ROWS, COLS),) * 3,
        scratch_shapes=[
            pltpu.VMEM((N_LAM, LANES), F32),
            pltpu.VMEM((8 * ITERS, LANES), F32),
            pltpu.VMEM((2, ITERS, ROWS, COLS), F32),
            pltpu.VMEM((2, FRAME + 16, WIDE), F32),
            pltpu.VMEM((FRAME + 16, WIDE), F32),
            pltpu.VMEM((FRAME, WIDE), F32),
            pltpu.VMEM((ITERS - 1, FRAME + 16, WIDE), F32),
            pltpu.VMEM((3, FRAME + 16, WIDE), F32),
        ],
        compiler_params=pltpu.CompilerParams(dimension_semantics=("arbitrary",), vmem_limit_bytes=14 << 20),
        name="adjoint",
    )(all_dots, vecs, coefs, wet, cost_weights, wside, band_s, band_n)


def solution(mesh):
    return jax.shard_map(
        body,
        mesh=mesh,
        in_specs=(P("lat", "lon"),) * 5 + (P(None, "lat", "lon"),),
        out_specs=(P(None, "lat", "lon"),) * 3,
        check_vma=False,
    )
```

```python
import functools

import jax
import jax.numpy as jnp
from jax import lax
from jax.experimental import pallas as pl
from jax.experimental.pallas import tpu as pltpu
from jax.sharding import PartitionSpec as P

ITERS = 6
COSTS = 8
ROWS = 64
COLS = 256
LANES = 128
TILES = 3
DEEP = 13
SLIM = 6
EDGE = 16
FIELDS = 5
FRAME = 80
TALL = 96
MSG_W = FIELDS * EDGE
MSG = MSG_W + COSTS * 8
N_LAM = COSTS * ITERS
N_RHS = N_LAM
N_MAT = N_LAM + ITERS
F32 = jnp.float32
HIGH = lax.Precision.HIGHEST


def lane_index(rows):
    return lax.broadcasted_iota(jnp.int32, (rows, LANES), 1)


def turn(value, amount):
    return pltpu.roll(value, amount % value.shape[1], 1)


def pack(rows, tiles):
    lane = lane_index(rows)
    out = jnp.zeros((rows, LANES), F32)
    at = 0
    for tile, first, wide in tiles:
        if tile is not None:
            here = (lane >= at) & (lane < at + wide)
            out = jnp.where(here, turn(tile, at - first), out)
        at += wide
    return out


def bands_kernel(f, de, dn, st, mask, w, to_north, to_south, whole_mask, sems):
    copies = []
    for side, out in enumerate((to_north, to_south)):
        low = ROWS - EDGE if side == 0 else 0
        rows = pl.ds(low, EDGE)
        for k, field in enumerate((f, de, dn, st)):
            copies.append((field.at[rows, :], out.at[pl.ds(EDGE * k, EDGE), :]))
        copies.append((mask.at[rows, :], whole_mask.at[side]))
        low = ROWS - 8 if side == 0 else 0
        for n in range(COSTS):
            copies.append((w.at[n, pl.ds(low, 8), :], out.at[pl.ds(MSG_W + 8 * n, 8), :]))
    copies = [
        pltpu.make_async_copy(src, dst, sems.at[i]) for i, (src, dst) in enumerate(copies)
    ]
    for copy in copies:
        copy.start()
    for copy in copies:
        copy.wait()
    to_north[MSG_W - EDGE : MSG_W, :] = whole_mask[0].astype(F32)
    to_south[MSG_W - EDGE : MSG_W, :] = whole_mask[1].astype(F32)


def strips_kernel(f, de, dn, st, mask, w, east, west):
    fields = [f[...], de[...], dn[...], st[...], mask[...].astype(F32)]
    right = [(v[:, LANES:], LANES - DEEP, DEEP) for v in fields]
    left = [(v[:, :LANES], 0, DEEP) for v in fields]
    right += [(w[n, :, LANES:], LANES - SLIM, SLIM) for n in range(COSTS)]
    left += [(w[n, :, :LANES], 0, SLIM) for n in range(COSTS)]
    east[...] = pack(ROWS, right)
    west[...] = pack(ROWS, left)


def corners_kernel(east, west, bs, bn, to_east, to_west):
    for own, out, lanes, first in ((east, to_east, slice(LANES, COLS), True), (west, to_west, slice(0, LANES), False)):
        out[EDGE : EDGE + ROWS, :] = own[...]
        for band, low, slim in ((bs, 0, 1), (bn, EDGE + ROWS, 0)):
            for half in range(2):
                tiles = []
                for k in range(FIELDS):
                    at = EDGE * k + 8 * half
                    tiles.append((band[at : at + 8, lanes], LANES - DEEP if first else 0, DEEP))
                for n in range(COSTS):
                    at = MSG_W + 8 * n
                    tile = band[at : at + 8, lanes] if half == slim else None
                    tiles.append((tile, LANES - SLIM if first else 0, SLIM))
                out[low + 8 * half : low + 8 * half + 8, :] = pack(8, tiles)


def side_tile(pw, pe, at, wide):
    lane = lane_index(pw.shape[0])
    west = jnp.where(lane >= LANES - wide, turn(pw, LANES - wide - at), 0.0)
    return jnp.where(lane < wide, turn(pe, -at), west)


def east_of(tiles):
    last = lane_index(8) == LANES - 1
    turned = [pltpu.roll(tile, LANES - 1, 1) for tile in tiles]
    return [jnp.where(last, turned[(t + 1) % TILES], turned[t]) for t in range(TILES)]


def west_of(tiles):
    first = lane_index(8) == 0
    turned = [pltpu.roll(tile, 1, 1) for tile in tiles]
    return [jnp.where(first, turned[t - 1], turned[t]) for t in range(TILES)]


def forward_kernel(
    flags, f, de, dn, st, mask, w, ls, ln, sw, se,
    vecs, links, inv2, wside, wet, dots,
    raw, north, vec, link, diag, part,
):
    own = (f, de, dn, st, mask)
    blocks = range(TALL // 8)
    tiles = range(TILES)
    for rb in blocks:
        at = 8 + 8 * rb
        src, off = None, 8 * rb - EDGE
        if rb < 2:
            src, off = ls, 8 * rb
        elif rb >= 10:
            src, off = ln, 8 * rb - 80
        pw, pe = sw[8 * rb : 8 * rb + 8, :], se[8 * rb : 8 * rb + 8, :]
        for k in range(FIELDS):
            values = []
            for t in range(2):
                lanes = slice(LANES * t, LANES * (t + 1))
                if src is None:
                    values.append(own[k][off : off + 8, lanes].astype(F32))
                else:
                    values.append(src[EDGE * k + off : EDGE * k + off + 8, lanes])
            values.append(side_tile(pw, pe, DEEP * k, DEEP))
            if k == FIELDS - 1 and src is not None:
                inside = flags[0 if rb < 2 else 1] > 0
                values = [jnp.where(inside, value, 0.0) for value in values]
            for t in tiles:
                raw[k, t, at : at + 8, :] = values[t]
        if 1 <= rb < 11:
            for n in range(COSTS):
                wside[n, 8 * rb - 8 : 8 * rb, :] = side_tile(
                    pw, pe, FIELDS * DEEP + SLIM * n, SLIM
                )
    for rb in blocks:
        here = slice(8 + 8 * rb, 16 + 8 * rb)
        above = slice(9 + 8 * rb, 17 + 8 * rb)
        for t in tiles:
            mn = raw[4, t, here, :] * raw[4, t, above, :]
            north[t, here, :] = raw[2, t, here, :] * mn
            if 2 <= rb < 10 and t < 2:
                wet[1, 8 * rb - 16 : 8 * rb - 8, LANES * t : LANES * (t + 1)] = mn
    for rb in blocks:
        here = slice(8 + 8 * rb, 16 + 8 * rb)
        below = slice(7 + 8 * rb, 15 + 8 * rb)
        m = [raw[4, t, here, :] for t in tiles]
        me = [a * b for a, b in zip(m, east_of(m))]
        ex = [raw[1, t, here, :] * me[t] for t in tiles]
        exw = west_of(ex)
        for t in tiles:
            ey, eys = north[t, here, :], north[t, below, :]
            total = m[t] * raw[3, t, here, :] + 1.0 - m[t] + ex[t] + exw[t] + ey + eys
            inv = 1.0 / total
            twice = inv + inv
            v0 = raw[0, t, here, :] * inv
            vec[0, t, here, :] = v0
            values = [twice * face for face in (ex[t], exw[t], ey, eys)]
            for k in range(4):
                link[k, t, here, :] = values[k]
            if 1 <= rb < 11:
                to = slice(8 * rb - 8, 8 * rb)
                vecs[0, t, to, :] = v0
                inv2[t, to, :] = twice
                for k in range(4):
                    links[k, t, to, :] = values[k]
            if 2 <= rb < 10 and t < 2:
                to, lanes = slice(8 * rb - 16, 8 * rb - 8), slice(LANES * t, LANES * (t + 1))
                wet[0, to, lanes] = me[t]
                diag[to, lanes] = total
    for j in range(ITERS):
        for rb in blocks:
            here = slice(8 + 8 * rb, 16 + 8 * rb)
            above = slice(9 + 8 * rb, 17 + 8 * rb)
            below = slice(7 + 8 * rb, 15 + 8 * rb)
            v = [vec[j, t, here, :] for t in tiles]
            ve, vw = east_of(v), west_of(v)
            for t in tiles:
                new = (
                    link[0, t, here, :] * ve[t]
                    + link[1, t, here, :] * vw[t]
                    + link[2, t, here, :] * vec[j, t, above, :]
                    + link[3, t, here, :] * vec[j, t, below, :]
                )
                new = 0.5 * new if j == 0 else new - vec[j - 1, t, here, :]
                vec[j + 1, t, here, :] = new
                if 1 <= rb < 11:
                    vecs[j + 1, t, 8 * rb - 8 : 8 * rb, :] = new
    count = ITERS + ITERS * (ITERS + 1) // 2
    own_tiles = [(rb, t) for rb in range(ROWS // 8) for t in range(2)]
    sums = [None] * count
    for rb, t in own_tiles:
        here, lanes = slice(8 * rb, 8 * rb + 8), slice(LANES * t, LANES * (t + 1))
        vs = [vec[j, t, 24 + 8 * rb : 32 + 8 * rb, :] for j in range(ITERS + 1)]
        total = diag[here, lanes]
        forcing = f[here, lanes]
        terms = [forcing * vs[j] for j in range(ITERS)]
        for j in range(ITERS):
            turned = vs[1] if j == 0 else 0.5 * (vs[j + 1] + vs[j - 1])
            image = total * (vs[j] - turned)
            terms += [image * vs[i] for i in range(j + 1)]
        sums = [b if a is None else a + b for a, b in zip(sums, terms)]
    part[N_RHS + count :, :] = jnp.zeros((LANES - N_RHS - count, LANES), F32)
    for k in range(count):
        part[N_RHS + k : N_RHS + k + 1, :] = jnp.sum(sums[k], axis=0, keepdims=True)
    for n in range(COSTS):
        sums = [None] * ITERS
        for rb, t in own_tiles:
            weight = w[n, 8 * rb : 8 * rb + 8, LANES * t : LANES * (t + 1)]
            for j in range(ITERS):
                term = weight * vec[j, t, 24 + 8 * rb : 32 + 8 * rb, :]
                sums[j] = term if sums[j] is None else sums[j] + term
        for j in range(ITERS):
            k = COSTS * j + n
            part[k : k + 1, :] = jnp.sum(sums[j], axis=0, keepdims=True)
    row = lax.dot_general(
        jnp.ones((8, LANES), F32), part[...], (((1,), (1,)), ((), ())),
        precision=HIGH, preferred_element_type=F32,
    )
    for at in range(0, dots.shape[0], 8):
        dots[at : at + 8, :] = row


def small_solve(total):
    wide = lambda k: jnp.broadcast_to(total[k : k + 1, :], (8, LANES))
    mat = {}
    k = N_MAT
    for j in range(ITERS):
        for i in range(j + 1):
            mat[j, i] = wide(k)
            k += 1
    low, inv = {}, []
    for j in range(ITERS):
        pivot = mat[j, j]
        for k in range(j):
            pivot = pivot - low[j, k] * mat[j, k]
        inv.append(1.0 / pivot)
        for i in range(j + 1, ITERS):
            entry = mat[i, j]
            for k in range(j):
                entry = entry - low[j, k] * mat[i, k]
            mat[i, j] = entry
            low[i, j] = entry * inv[j]

    def solve(rhs):
        y = []
        for i in range(ITERS):
            t = rhs[i]
            for k in range(i):
                t = t - low[i, k] * y[k]
            y.append(t)
        out = [None] * ITERS
        for i in range(ITERS - 1, -1, -1):
            t = y[i] * inv[i]
            for k in range(i + 1, ITERS):
                t = t - low[k, i] * out[k]
            out[i] = t
        return out

    return (
        solve([wide(N_RHS + i) for i in range(ITERS)]),
        solve([total[COSTS * j : COSTS * (j + 1), :] for j in range(ITERS)]),
    )


def imaged(coef):
    get = lambda k: coef[k] if 0 <= k < ITERS else None
    out = []
    for k in range(ITERS + 1):
        low, mid, high = get(k - 1), get(k), get(k + 1)
        value = jnp.zeros_like(coef[0]) if mid is None else mid + mid
        if low is not None:
            value = value - (low + low if k == 1 else low)
        if high is not None:
            value = value - high
        out.append(value)
    return out


def mixed(factors, values):
    total = None
    for factor, value in zip(factors, values):
        term = factor * value
        total = term if total is None else total + term
    return total


def adjoint_kernel(
    all_dots, vecs, links, inv2, wet, w, wside, ws, wn,
    adj, east, north,
    lam, lam2, cs, slope, lag, rs, ys, ss, ps, acc,
):
    n = pl.program_id(0)
    blocks = range(FRAME // 8)
    tiles = range(TILES)
    lanes_of = lambda t: slice(LANES * t, LANES * (t + 1))

    @pl.when(n == 0)
    def _():
        rows = [all_dots[at : at + 8, :] for at in range(0, all_dots.shape[0], 8)]
        while len(rows) > 1:
            rows = [a + b for a, b in zip(rows[::2], rows[1::2])]
        total = lax.dot_general(
            rows[0], jnp.ones((8, LANES), F32), (((0,), (0,)), ((), ())),
            precision=HIGH, preferred_element_type=F32,
        )
        c, weights = small_solve(total)
        for j in range(ITERS):
            lam[8 * j : 8 * j + 8, :] = weights[j]
            cs[8 * j : 8 * j + 8, :] = c[j]
        for k, value in enumerate(imaged(weights)):
            lam2[8 * k : 8 * k + 8, :] = value
        c2 = imaged(c)
        for rb in blocks:
            here = slice(8 * rb, 8 * rb + 8)
            for t in tiles:
                v = [vecs[k, t, here, :] for k in range(ITERS + 1)]
                rs[t, here, :] = v[0] + v[0] - mixed(c2, v)
                if rb >= 1:
                    lag[0, t, here, :] = v[1] - v[0]
                    for j in range(1, ITERS - 1):
                        lag[j, t, here, :] = 0.5 * (v[j + 1] + v[j - 1]) - v[j]
        for rb in range(1, 9):
            here = slice(8 * rb, 8 * rb + 8)
            above = slice(8 * rb + 1, 8 * rb + 9)
            to = slice(8 * rb - 8, 8 * rb)
            sums = [[None, None], [None, None]]
            for j in range(ITERS):
                v = [vecs[j, t, here, :] for t in tiles]
                ve = east_of(v)
                for t in range(2):
                    for d, near in enumerate((ve[t], vecs[j, t, above, :])):
                        step = v[t] - near
                        if j < ITERS - 1:
                            slope[d, j, t, to, :] = step
                        term = c[j] * step
                        sums[d][t] = term if j == 0 else sums[d][t] + term
            for d in range(2):
                for t in range(2):
                    slope[d, ITERS - 1, t, to, :] = sums[d][t]

    spread = lambda ref, k: jnp.broadcast_to(ref[pl.ds(8 * k + n, 1), :], (8, LANES))
    rows = [spread(lam, j) for j in range(ITERS)]
    rows2 = [spread(lam2, k) for k in range(ITERS + 1)]
    last = ITERS - 1
    c_last = cs[8 * last : 8 * last + 8, :]
    for rb in blocks:
        at = 8 + 8 * rb
        here = slice(8 * rb, 8 * rb + 8)
        for t in tiles:
            v = [vecs[k, t, here, :] for k in range(ITERS + 1)]
            if t == 2:
                weight = wside[0, here, :]
            elif rb == 0:
                weight = ws[:, lanes_of(t)]
            elif rb == 9:
                weight = wn[:, lanes_of(t)]
            else:
                weight = w[0, 8 * rb - 8 : 8 * rb, lanes_of(t)]
            s = inv2[t, here, :] * weight - mixed(rows2, v)
            ss[t, here, :] = s
            ps[last - 1, t, at : at + 8, :] = c_last * s + rows[last] * rs[t, here, :]
            if rb >= 1:
                ys[t, here, :] = mixed(rows, v)
    for rb in range(1, 9):
        here = slice(8 * rb, 8 * rb + 8)
        above = slice(8 * rb + 1, 8 * rb + 9)
        to = slice(8 * rb - 8, 8 * rb)
        y = [ys[t, here, :] for t in tiles]
        ye = east_of(y)
        for t in range(2):
            acc[0, t, to, :] = (y[t] - ye[t]) * slope[0, last, t, to, :]
            acc[1, t, to, :] = (y[t] - ys[t, above, :]) * slope[1, last, t, to, :]
    lagged = lambda rb: slice(8 * rb - 8, 8 * rb)
    for j in range(ITERS - 2, -1, -1):
        c_j = cs[8 * j : 8 * j + 8, :]
        for rb in blocks:
            if j == 0 and rb == 0:
                continue
            at = 8 + 8 * rb
            here = slice(8 * rb, 8 * rb + 8)
            p = [ps[j, t, at : at + 8, :] for t in tiles]
            pe, pw = east_of(p), west_of(p)
            for t in tiles:
                pn = ps[j, t, at + 1 : at + 9, :]
                bar = (
                    links[0, t, here, :] * pe[t]
                    + links[1, t, here, :] * pw[t]
                    + links[2, t, here, :] * pn
                    + links[3, t, here, :] * ps[j, t, at - 1 : at + 7, :]
                ) + (c_j * ss[t, here, :] + rows[j] * rs[t, here, :])
                if j < ITERS - 2:
                    bar = bar - ps[j + 1, t, at : at + 8, :]
                if j == 1:
                    bar = 0.5 * bar
                if j > 0:
                    ps[j - 1, t, at : at + 8, :] = bar
                if rb >= 1:
                    d = p[t] * lag[j, t, here, :]
                    if j < ITERS - 2:
                        d = acc[2, t, lagged(rb), :] + d
                    if j == 0:
                        g = 0.5 * bar
                        d = d + g * vecs[0, t, here, :]
                    acc[2, t, lagged(rb), :] = d
                if 1 <= rb < 9 and t < 2:
                    to = lagged(rb)
                    acc[0, t, to, :] = acc[0, t, to, :] + (p[t] - pe[t]) * slope[0, j, t, to, :]
                    acc[1, t, to, :] = acc[1, t, to, :] + (p[t] - pn) * slope[1, j, t, to, :]
                    if j == 0:
                        adj[0, to, lanes_of(t)] = ys[t, here, :] + g
    for rb in range(ROWS // 8):
        to = slice(8 * rb, 8 * rb + 8)
        d = [acc[2, t, to, :] for t in tiles]
        de = east_of(d)
        for t in range(2):
            above = acc[2, t, 8 * rb + 1 : 8 * rb + 9, :]
            east[0, to, lanes_of(t)] = -wet[0, to, lanes_of(t)] * (acc[0, t, to, :] + d[t] + de[t])
            north[0, to, lanes_of(t)] = -wet[1, to, lanes_of(t)] * (acc[1, t, to, :] + d[t] + above)


def ring(axis, steps):
    count = lax.axis_size(axis)
    return [(source, (source + steps) % count) for source in range(count)]


def struct(*shape):
    return jax.ShapeDtypeStruct(shape, F32)


def whole():
    return pl.BlockSpec(memory_space=pltpu.VMEM)


def body(forcing, depth_east, depth_north, surface_term, ocean_mask, cost_weights):
    args = (forcing, depth_east, depth_north, surface_term, ocean_mask, cost_weights)
    lats = lax.axis_size("lat")
    devices = lats * lax.axis_size("lon")
    small = pltpu.CompilerParams(vmem_limit_bytes=4 << 20)
    to_north, to_south = pl.pallas_call(
        bands_kernel,
        in_specs=[pl.BlockSpec(memory_space=pltpu.HBM)] * 6,
        out_specs=[whole()] * 2,
        out_shape=(struct(MSG, COLS),) * 2,
        scratch_shapes=[
            pltpu.VMEM((2, EDGE, COLS), jnp.int32),
            pltpu.SemaphoreType.DMA((2 * (FIELDS + COSTS),)),
        ],
        compiler_params=small,
        name="bands",
    )(*[pltpu.with_memory_space_constraint(arg, pltpu.HBM) for arg in args])
    band_s = lax.ppermute(to_north, "lat", ring("lat", 1))
    band_n = lax.ppermute(to_south, "lat", ring("lat", -1))
    east, west = pl.pallas_call(
        strips_kernel,
        in_specs=[whole()] * 6,
        out_specs=[whole()] * 2,
        out_shape=(struct(ROWS, LANES),) * 2,
        compiler_params=small,
        name="strips",
    )(*args)
    to_east, to_west = pl.pallas_call(
        corners_kernel,
        in_specs=[whole()] * 4,
        out_specs=[whole()] * 2,
        out_shape=(struct(TALL, LANES),) * 2,
        compiler_params=small,
        name="corners",
    )(east, west, band_s, band_n)
    side_w = lax.ppermute(to_east, "lon", ring("lon", 1))
    side_e = lax.ppermute(to_west, "lon", ring("lon", -1))
    row = lax.axis_index("lat")
    flags = jnp.stack([row > 0, row < lats - 1]).astype(jnp.int32)
    vecs, links, inv2, wside, wet, dots = pl.pallas_call(
        forward_kernel,
        in_specs=[pl.BlockSpec(memory_space=pltpu.SMEM)] + [whole()] * 10,
        out_specs=[whole()] * 6,
        out_shape=(
            struct(ITERS + 1, TILES, FRAME, LANES), struct(4, TILES, FRAME, LANES),
            struct(TILES, FRAME, LANES), struct(COSTS, FRAME, LANES),
            struct(2, ROWS, COLS), struct(devices, LANES),
        ),
        scratch_shapes=[
            pltpu.VMEM((FIELDS, TILES, TALL + 16, LANES), F32),
            pltpu.VMEM((TILES, TALL + 16, LANES), F32),
            pltpu.VMEM((ITERS + 1, TILES, TALL + 16, LANES), F32),
            pltpu.VMEM((4, TILES, TALL + 16, LANES), F32),
            pltpu.VMEM((ROWS, COLS), F32),
            pltpu.VMEM((LANES, LANES), F32),
        ],
        compiler_params=pltpu.CompilerParams(vmem_limit_bytes=14 << 20),
        name="forward",
    )(flags, *args, band_s, band_n, side_w, side_e)
    all_dots = lax.all_to_all(dots, ("lat", "lon"), 0, 0, tiled=True)
    out_spec = pl.BlockSpec((1, ROWS, COLS), lambda n: (n, 0, 0))
    full = lambda *shape: pl.BlockSpec(shape, lambda n: (0,) * len(shape))
    return pl.pallas_call(
        adjoint_kernel,
        grid=(COSTS,),
        in_specs=[
            full(devices, LANES),
            full(ITERS + 1, TILES, FRAME, LANES),
            full(4, TILES, FRAME, LANES),
            full(TILES, FRAME, LANES),
            full(2, ROWS, COLS),
            pl.BlockSpec((1, ROWS, COLS), lambda n: (n, 0, 0)),
            pl.BlockSpec((1, FRAME, LANES), lambda n: (n, 0, 0)),
            pl.BlockSpec((8, COLS), lambda n: (MSG_W // 8 + n, 0)),
            pl.BlockSpec((8, COLS), lambda n: (MSG_W // 8 + n, 0)),
        ],
        out_specs=[out_spec] * 3,
        out_shape=(struct(COSTS, ROWS, COLS),) * 3,
        scratch_shapes=[
            pltpu.VMEM((N_LAM, LANES), F32),
            pltpu.VMEM((N_LAM + 8, LANES), F32),
            pltpu.VMEM((8 * ITERS, LANES), F32),
            pltpu.VMEM((2, ITERS, 2, ROWS, LANES), F32),
            pltpu.VMEM((ITERS - 1, TILES, FRAME, LANES), F32),
            pltpu.VMEM((TILES, FRAME, LANES), F32),
            pltpu.VMEM((TILES, FRAME, LANES), F32),
            pltpu.VMEM((TILES, FRAME, LANES), F32),
            pltpu.VMEM((ITERS - 1, TILES, FRAME + 16, LANES), F32),
            pltpu.VMEM((3, TILES, FRAME - 8, LANES), F32),
        ],
        compiler_params=pltpu.CompilerParams(
            dimension_semantics=("arbitrary",), vmem_limit_bytes=18 << 20
        ),
        name="adjoint",
    )(all_dots, vecs, links, inv2, wet, cost_weights, wside, band_s, band_n)


def solution(mesh):
    return jax.shard_map(
        body,
        mesh=mesh,
        in_specs=(P("lat", "lon"),) * 5 + (P(None, "lat", "lon"),),
        out_specs=(P(None, "lat", "lon"),) * 3,
        check_vma=False,
    )
```

```python
import functools

import jax
import jax.numpy as jnp
from jax import lax
from jax.experimental import pallas as pl
from jax.experimental.pallas import tpu as pltpu
from jax.sharding import PartitionSpec as P

ITERS = 6
COSTS = 8
ROWS = 64
COLS = 256
LANES = 128
TILES = 3
DEEP = 13
SLIM = 6
EDGE = 16
FIELDS = 5
FRAME = 80
TALL = 96
MSG_W = FIELDS * EDGE
MSG = MSG_W + COSTS * 8
N_LAM = COSTS * ITERS
N_RHS = N_LAM
N_MAT = N_LAM + ITERS
F32 = jnp.float32
HIGH = lax.Precision.HIGHEST


def lane_index(rows):
    return lax.broadcasted_iota(jnp.int32, (rows, LANES), 1)


def turn(value, amount):
    return pltpu.roll(value, amount % value.shape[1], 1)


def pack(rows, tiles):
    lane = lane_index(rows)
    out = jnp.zeros((rows, LANES), F32)
    at = 0
    for tile, first, wide in tiles:
        if tile is not None:
            here = (lane >= at) & (lane < at + wide)
            out = jnp.where(here, turn(tile, at - first), out)
        at += wide
    return out


def bands_kernel(f, de, dn, st, mask, w, to_north, to_south, whole_mask, sems):
    copies = []
    for side, out in enumerate((to_north, to_south)):
        low = ROWS - EDGE if side == 0 else 0
        rows = pl.ds(low, EDGE)
        for k, field in enumerate((f, de, dn, st)):
            copies.append((field.at[rows, :], out.at[pl.ds(EDGE * k, EDGE), :]))
        copies.append((mask.at[rows, :], whole_mask.at[side]))
        low = ROWS - 8 if side == 0 else 0
        for n in range(COSTS):
            copies.append((w.at[n, pl.ds(low, 8), :], out.at[pl.ds(MSG_W + 8 * n, 8), :]))
    copies = [
        pltpu.make_async_copy(src, dst, sems.at[i]) for i, (src, dst) in enumerate(copies)
    ]
    for copy in copies:
        copy.start()
    for copy in copies:
        copy.wait()
    to_north[MSG_W - EDGE : MSG_W, :] = whole_mask[0].astype(F32)
    to_south[MSG_W - EDGE : MSG_W, :] = whole_mask[1].astype(F32)


def strips_kernel(f, de, dn, st, mask, w, east, west):
    fields = [f[...], de[...], dn[...], st[...], mask[...].astype(F32)]
    right = [(v[:, LANES:], LANES - DEEP, DEEP) for v in fields]
    left = [(v[:, :LANES], 0, DEEP) for v in fields]
    right += [(w[n, :, LANES:], LANES - SLIM, SLIM) for n in range(COSTS)]
    left += [(w[n, :, :LANES], 0, SLIM) for n in range(COSTS)]
    east[...] = pack(ROWS, right)
    west[...] = pack(ROWS, left)


def corners_kernel(east, west, bs, bn, to_east, to_west):
    for own, out, lanes, first in ((east, to_east, slice(LANES, COLS), True), (west, to_west, slice(0, LANES), False)):
        out[EDGE : EDGE + ROWS, :] = own[...]
        for band, low, slim in ((bs, 0, 1), (bn, EDGE + ROWS, 0)):
            for half in range(2):
                tiles = []
                for k in range(FIELDS):
                    at = EDGE * k + 8 * half
                    tiles.append((band[at : at + 8, lanes], LANES - DEEP if first else 0, DEEP))
                for n in range(COSTS):
                    at = MSG_W + 8 * n
                    tile = band[at : at + 8, lanes] if half == slim else None
                    tiles.append((tile, LANES - SLIM if first else 0, SLIM))
                out[low + 8 * half : low + 8 * half + 8, :] = pack(8, tiles)


def side_tile(pw, pe, at, wide):
    lane = lane_index(pw.shape[0])
    west = jnp.where(lane >= LANES - wide, turn(pw, LANES - wide - at), 0.0)
    return jnp.where(lane < wide, turn(pe, -at), west)


def east_of(tiles):
    last = lane_index(8) == LANES - 1
    turned = [pltpu.roll(tile, LANES - 1, 1) for tile in tiles]
    return [jnp.where(last, turned[(t + 1) % TILES], turned[t]) for t in range(TILES)]


def west_of(tiles):
    first = lane_index(8) == 0
    turned = [pltpu.roll(tile, 1, 1) for tile in tiles]
    return [jnp.where(first, turned[t - 1], turned[t]) for t in range(TILES)]


def forward_kernel(
    flags, f, de, dn, st, mask, w, ls, ln, sw, se,
    vecs, links, wside, wet, dots,
    raw, north, vec, link, diag, part,
):
    own = (f, de, dn, st, mask)
    blocks = range(TALL // 8)
    tiles = range(TILES)
    for rb in blocks:
        at = 8 + 8 * rb
        src, off = None, 8 * rb - EDGE
        if rb < 2:
            src, off = ls, 8 * rb
        elif rb >= 10:
            src, off = ln, 8 * rb - 80
        pw, pe = sw[8 * rb : 8 * rb + 8, :], se[8 * rb : 8 * rb + 8, :]
        for k in range(FIELDS):
            values = []
            for t in range(2):
                lanes = slice(LANES * t, LANES * (t + 1))
                if src is None:
                    values.append(own[k][off : off + 8, lanes].astype(F32))
                else:
                    values.append(src[EDGE * k + off : EDGE * k + off + 8, lanes])
            values.append(side_tile(pw, pe, DEEP * k, DEEP))
            if k == FIELDS - 1 and src is not None:
                inside = flags[0 if rb < 2 else 1] > 0
                values = [jnp.where(inside, value, 0.0) for value in values]
            for t in tiles:
                raw[k, t, at : at + 8, :] = values[t]
        if 1 <= rb < 11:
            for n in range(COSTS):
                wside[n, 8 * rb - 8 : 8 * rb, :] = side_tile(
                    pw, pe, FIELDS * DEEP + SLIM * n, SLIM
                )
    for rb in blocks:
        here = slice(8 + 8 * rb, 16 + 8 * rb)
        above = slice(9 + 8 * rb, 17 + 8 * rb)
        for t in tiles:
            mn = raw[4, t, here, :] * raw[4, t, above, :]
            north[t, here, :] = raw[2, t, here, :] * mn
            if 2 <= rb < 10 and t < 2:
                wet[1, 8 * rb - 16 : 8 * rb - 8, LANES * t : LANES * (t + 1)] = mn
    for rb in blocks:
        here = slice(8 + 8 * rb, 16 + 8 * rb)
        below = slice(7 + 8 * rb, 15 + 8 * rb)
        m = [raw[4, t, here, :] for t in tiles]
        me = [a * b for a, b in zip(m, east_of(m))]
        ex = [raw[1, t, here, :] * me[t] for t in tiles]
        exw = west_of(ex)
        for t in tiles:
            ey, eys = north[t, here, :], north[t, below, :]
            total = m[t] * raw[3, t, here, :] + 1.0 - m[t] + ex[t] + exw[t] + ey + eys
            inv = 1.0 / total
            twice = inv + inv
            v0 = raw[0, t, here, :] * inv
            vec[0, t, here, :] = v0
            values = [twice * face for face in (ex[t], exw[t], ey, eys)]
            for k in range(4):
                link[k, t, here, :] = values[k]
            if 1 <= rb < 11:
                to = slice(8 * rb - 8, 8 * rb)
                vecs[0, t, to, :] = v0
                vecs[ITERS + 1, t, to, :] = twice
                for k in range(4):
                    links[k, t, to, :] = values[k]
            if 2 <= rb < 10 and t < 2:
                to, lanes = slice(8 * rb - 16, 8 * rb - 8), slice(LANES * t, LANES * (t + 1))
                wet[0, to, lanes] = me[t]
                diag[to, lanes] = total
    for j in range(ITERS):
        for rb in blocks:
            here = slice(8 + 8 * rb, 16 + 8 * rb)
            above = slice(9 + 8 * rb, 17 + 8 * rb)
            below = slice(7 + 8 * rb, 15 + 8 * rb)
            v = [vec[j, t, here, :] for t in tiles]
            ve, vw = east_of(v), west_of(v)
            for t in tiles:
                new = (
                    link[0, t, here, :] * ve[t]
                    + link[1, t, here, :] * vw[t]
                    + link[2, t, here, :] * vec[j, t, above, :]
                    + link[3, t, here, :] * vec[j, t, below, :]
                )
                new = 0.5 * new if j == 0 else new - vec[j - 1, t, here, :]
                vec[j + 1, t, here, :] = new
                if 1 <= rb < 11:
                    vecs[j + 1, t, 8 * rb - 8 : 8 * rb, :] = new
    count = ITERS + ITERS * (ITERS + 1) // 2
    own_tiles = [(rb, t) for rb in range(ROWS // 8) for t in range(2)]
    sums = [None] * count
    for rb, t in own_tiles:
        here, lanes = slice(8 * rb, 8 * rb + 8), slice(LANES * t, LANES * (t + 1))
        vs = [vec[j, t, 24 + 8 * rb : 32 + 8 * rb, :] for j in range(ITERS + 1)]
        total = diag[here, lanes]
        forcing = f[here, lanes]
        terms = [forcing * vs[j] for j in range(ITERS)]
        for j in range(ITERS):
            turned = vs[1] if j == 0 else 0.5 * (vs[j + 1] + vs[j - 1])
            image = total * (vs[j] - turned)
            terms += [image * vs[i] for i in range(j + 1)]
        sums = [b if a is None else a + b for a, b in zip(sums, terms)]
    part[N_RHS + count :, :] = jnp.zeros((LANES - N_RHS - count, LANES), F32)
    for k in range(count):
        part[N_RHS + k : N_RHS + k + 1, :] = jnp.sum(sums[k], axis=0, keepdims=True)
    for n in range(COSTS):
        sums = [None] * ITERS
        for rb, t in own_tiles:
            weight = w[n, 8 * rb : 8 * rb + 8, LANES * t : LANES * (t + 1)]
            for j in range(ITERS):
                term = weight * vec[j, t, 24 + 8 * rb : 32 + 8 * rb, :]
                sums[j] = term if sums[j] is None else sums[j] + term
        for j in range(ITERS):
            k = COSTS * j + n
            part[k : k + 1, :] = jnp.sum(sums[j], axis=0, keepdims=True)
    row = lax.dot_general(
        jnp.ones((8, LANES), F32), part[...], (((1,), (1,)), ((), ())),
        precision=HIGH, preferred_element_type=F32,
    )
    for at in range(0, dots.shape[0], 8):
        dots[at : at + 8, :] = row


def small_solve(total):
    wide = lambda k: jnp.broadcast_to(total[k : k + 1, :], (8, LANES))
    mat = {}
    k = N_MAT
    for j in range(ITERS):
        for i in range(j + 1):
            mat[j, i] = wide(k)
            k += 1
    low, inv = {}, []
    for j in range(ITERS):
        pivot = mat[j, j]
        for k in range(j):
            pivot = pivot - low[j, k] * mat[j, k]
        inv.append(1.0 / pivot)
        for i in range(j + 1, ITERS):
            entry = mat[i, j]
            for k in range(j):
                entry = entry - low[j, k] * mat[i, k]
            mat[i, j] = entry
            low[i, j] = entry * inv[j]

    def solve(rhs):
        y = []
        for i in range(ITERS):
            t = rhs[i]
            for k in range(i):
                t = t - low[i, k] * y[k]
            y.append(t)
        out = [None] * ITERS
        for i in range(ITERS - 1, -1, -1):
            t = y[i] * inv[i]
            for k in range(i + 1, ITERS):
                t = t - low[k, i] * out[k]
            out[i] = t
        return out

    return (
        solve([wide(N_RHS + i) for i in range(ITERS)]),
        solve([total[COSTS * j : COSTS * (j + 1), :] for j in range(ITERS)]),
    )


def imaged(coef):
    get = lambda k: coef[k] if 0 <= k < ITERS else None
    out = []
    for k in range(ITERS + 1):
        low, mid, high = get(k - 1), get(k), get(k + 1)
        value = jnp.zeros_like(coef[0]) if mid is None else mid + mid
        if low is not None:
            value = value - (low + low if k == 1 else low)
        if high is not None:
            value = value - high
        out.append(value)
    return out


def mixed(factors, values):
    total = None
    for factor, value in zip(factors, values):
        term = factor * value
        total = term if total is None else total + term
    return total


def adjoint_kernel(
    all_dots, vecs, links, wet, w, wside, ws, wn,
    adj, east, north,
    lam, lam2, cs, slope, lag, rs, ys, ss, ps, acc,
):
    n = pl.program_id(0)
    blocks = range(FRAME // 8)
    tiles = range(TILES)
    lanes_of = lambda t: slice(LANES * t, LANES * (t + 1))

    @pl.when(n == 0)
    def _():
        rows = [all_dots[at : at + 8, :] for at in range(0, all_dots.shape[0], 8)]
        while len(rows) > 1:
            rows = [a + b for a, b in zip(rows[::2], rows[1::2])]
        total = lax.dot_general(
            rows[0], jnp.ones((8, LANES), F32), (((0,), (0,)), ((), ())),
            precision=HIGH, preferred_element_type=F32,
        )
        c, weights = small_solve(total)
        for j in range(ITERS):
            lam[8 * j : 8 * j + 8, :] = weights[j]
            cs[8 * j : 8 * j + 8, :] = c[j]
        for k, value in enumerate(imaged(weights)):
            lam2[8 * k : 8 * k + 8, :] = value
        c2 = imaged(c)
        for rb in blocks:
            here = slice(8 * rb, 8 * rb + 8)
            for t in tiles:
                v = [vecs[k, t, here, :] for k in range(ITERS + 1)]
                rs[t, here, :] = v[0] + v[0] - mixed(c2, v)
                if rb >= 1:
                    lag[0, t, here, :] = v[1] - v[0]
                    for j in range(1, ITERS - 1):
                        lag[j, t, here, :] = 0.5 * (v[j + 1] + v[j - 1]) - v[j]
        for rb in range(1, 9):
            here = slice(8 * rb, 8 * rb + 8)
            above = slice(8 * rb + 1, 8 * rb + 9)
            to = slice(8 * rb - 8, 8 * rb)
            sums = [[None, None], [None, None]]
            for j in range(ITERS):
                v = [vecs[j, t, here, :] for t in tiles]
                ve = east_of(v)
                for t in range(2):
                    for d, near in enumerate((ve[t], vecs[j, t, above, :])):
                        step = v[t] - near
                        if j < ITERS - 1:
                            slope[d, j, t, to, :] = step
                        term = c[j] * step
                        sums[d][t] = term if j == 0 else sums[d][t] + term
            for d in range(2):
                for t in range(2):
                    slope[d, ITERS - 1, t, to, :] = sums[d][t]

    spread = lambda ref, k: jnp.broadcast_to(ref[pl.ds(8 * k + n, 1), :], (8, LANES))
    rows = [spread(lam, j) for j in range(ITERS)]
    rows2 = [spread(lam2, k) for k in range(ITERS + 1)]
    last = ITERS - 1
    c_last = cs[8 * last : 8 * last + 8, :]
    for rb in blocks:
        at = 8 + 8 * rb
        here = slice(8 * rb, 8 * rb + 8)
        for t in tiles:
            v = [vecs[k, t, here, :] for k in range(ITERS + 1)]
            if t == 2:
                weight = wside[0, here, :]
            elif rb == 0:
                weight = ws[:, lanes_of(t)]
            elif rb == 9:
                weight = wn[:, lanes_of(t)]
            else:
                weight = w[0, 8 * rb - 8 : 8 * rb, lanes_of(t)]
            s = vecs[ITERS + 1, t, here, :] * weight - mixed(rows2, v)
            ss[t, here, :] = s
            ps[last - 1, t, at : at + 8, :] = c_last * s + rows[last] * rs[t, here, :]
            if rb >= 1:
                ys[t, here, :] = mixed(rows, v)
    for rb in range(1, 9):
        here = slice(8 * rb, 8 * rb + 8)
        above = slice(8 * rb + 1, 8 * rb + 9)
        to = slice(8 * rb - 8, 8 * rb)
        y = [ys[t, here, :] for t in tiles]
        ye = east_of(y)
        for t in range(2):
            acc[0, t, to, :] = (y[t] - ye[t]) * slope[0, last, t, to, :]
            acc[1, t, to, :] = (y[t] - ys[t, above, :]) * slope[1, last, t, to, :]
    lagged = lambda rb: slice(8 * rb - 8, 8 * rb)
    for j in range(ITERS - 2, -1, -1):
        c_j = cs[8 * j : 8 * j + 8, :]
        for rb in blocks:
            if j == 0 and rb == 0:
                continue
            at = 8 + 8 * rb
            here = slice(8 * rb, 8 * rb + 8)
            p = [ps[j, t, at : at + 8, :] for t in tiles]
            pe, pw = east_of(p), west_of(p)
            for t in tiles:
                pn = ps[j, t, at + 1 : at + 9, :]
                bar = (
                    links[0, t, here, :] * pe[t]
                    + links[1, t, here, :] * pw[t]
                    + links[2, t, here, :] * pn
                    + links[3, t, here, :] * ps[j, t, at - 1 : at + 7, :]
                ) + (c_j * ss[t, here, :] + rows[j] * rs[t, here, :])
                if j < ITERS - 2:
                    bar = bar - ps[j + 1, t, at : at + 8, :]
                if j == 1:
                    bar = 0.5 * bar
                if j > 0:
                    ps[j - 1, t, at : at + 8, :] = bar
                if rb >= 1:
                    d = p[t] * lag[j, t, here, :]
                    if j < ITERS - 2:
                        d = acc[2, t, lagged(rb), :] + d
                    if j == 0:
                        g = 0.5 * bar
                        d = d + g * vecs[0, t, here, :]
                    acc[2, t, lagged(rb), :] = d
                if 1 <= rb < 9 and t < 2:
                    to = lagged(rb)
                    acc[0, t, to, :] = acc[0, t, to, :] + (p[t] - pe[t]) * slope[0, j, t, to, :]
                    acc[1, t, to, :] = acc[1, t, to, :] + (p[t] - pn) * slope[1, j, t, to, :]
                    if j == 0:
                        adj[0, to, lanes_of(t)] = ys[t, here, :] + g
    for rb in range(ROWS // 8):
        to = slice(8 * rb, 8 * rb + 8)
        d = [acc[2, t, to, :] for t in tiles]
        de = east_of(d)
        for t in range(2):
            above = acc[2, t, 8 * rb + 1 : 8 * rb + 9, :]
            east[0, to, lanes_of(t)] = -wet[0, to, lanes_of(t)] * (acc[0, t, to, :] + d[t] + de[t])
            north[0, to, lanes_of(t)] = -wet[1, to, lanes_of(t)] * (acc[1, t, to, :] + d[t] + above)


def ring(axis, steps):
    count = lax.axis_size(axis)
    return [(source, (source + steps) % count) for source in range(count)]


def struct(*shape):
    return jax.ShapeDtypeStruct(shape, F32)


def whole():
    return pl.BlockSpec(memory_space=pltpu.VMEM)


def body(forcing, depth_east, depth_north, surface_term, ocean_mask, cost_weights):
    args = (forcing, depth_east, depth_north, surface_term, ocean_mask, cost_weights)
    lats = lax.axis_size("lat")
    devices = lats * lax.axis_size("lon")
    small = pltpu.CompilerParams(vmem_limit_bytes=4 << 20)
    to_north, to_south = pl.pallas_call(
        bands_kernel,
        in_specs=[pl.BlockSpec(memory_space=pltpu.HBM)] * 6,
        out_specs=[whole()] * 2,
        out_shape=(struct(MSG, COLS),) * 2,
        scratch_shapes=[
            pltpu.VMEM((2, EDGE, COLS), jnp.int32),
            pltpu.SemaphoreType.DMA((2 * (FIELDS + COSTS),)),
        ],
        compiler_params=small,
        name="bands",
    )(*[pltpu.with_memory_space_constraint(arg, pltpu.HBM) for arg in args])
    band_s = lax.ppermute(to_north, "lat", ring("lat", 1))
    band_n = lax.ppermute(to_south, "lat", ring("lat", -1))
    east, west = pl.pallas_call(
        strips_kernel,
        in_specs=[whole()] * 6,
        out_specs=[whole()] * 2,
        out_shape=(struct(ROWS, LANES),) * 2,
        compiler_params=small,
        name="strips",
    )(*args)
    to_east, to_west = pl.pallas_call(
        corners_kernel,
        in_specs=[whole()] * 4,
        out_specs=[whole()] * 2,
        out_shape=(struct(TALL, LANES),) * 2,
        compiler_params=small,
        name="corners",
    )(east, west, band_s, band_n)
    side_w = lax.ppermute(to_east, "lon", ring("lon", 1))
    side_e = lax.ppermute(to_west, "lon", ring("lon", -1))
    row = lax.axis_index("lat")
    flags = jnp.stack([row > 0, row < lats - 1]).astype(jnp.int32)
    vecs, links, wside, wet, dots = pl.pallas_call(
        forward_kernel,
        in_specs=[pl.BlockSpec(memory_space=pltpu.SMEM)] + [whole()] * 10,
        out_specs=[whole()] * 5,
        out_shape=(
            struct(ITERS + 2, TILES, FRAME, LANES), struct(4, TILES, FRAME, LANES),
            struct(COSTS, FRAME, LANES),
            struct(2, ROWS, COLS), struct(devices, LANES),
        ),
        scratch_shapes=[
            pltpu.VMEM((FIELDS, TILES, TALL + 16, LANES), F32),
            pltpu.VMEM((TILES, TALL + 16, LANES), F32),
            pltpu.VMEM((ITERS + 1, TILES, TALL + 16, LANES), F32),
            pltpu.VMEM((4, TILES, TALL + 16, LANES), F32),
            pltpu.VMEM((ROWS, COLS), F32),
            pltpu.VMEM((LANES, LANES), F32),
        ],
        compiler_params=pltpu.CompilerParams(vmem_limit_bytes=14 << 20),
        name="forward",
    )(flags, *args, band_s, band_n, side_w, side_e)
    all_dots = lax.all_to_all(dots, ("lat", "lon"), 0, 0, tiled=True)
    out_spec = pl.BlockSpec((1, ROWS, COLS), lambda n: (n, 0, 0))
    return pl.pallas_call(
        adjoint_kernel,
        grid=(COSTS,),
        in_specs=[
            whole(),
            whole(),
            whole(),
            whole(),
            pl.BlockSpec((1, ROWS, COLS), lambda n: (n, 0, 0)),
            pl.BlockSpec((1, FRAME, LANES), lambda n: (n, 0, 0)),
            pl.BlockSpec((8, COLS), lambda n: (MSG_W // 8 + n, 0)),
            pl.BlockSpec((8, COLS), lambda n: (MSG_W // 8 + n, 0)),
        ],
        out_specs=[out_spec] * 3,
        out_shape=(struct(COSTS, ROWS, COLS),) * 3,
        scratch_shapes=[
            pltpu.VMEM((N_LAM, LANES), F32),
            pltpu.VMEM((N_LAM + 8, LANES), F32),
            pltpu.VMEM((8 * ITERS, LANES), F32),
            pltpu.VMEM((2, ITERS, 2, ROWS, LANES), F32),
            pltpu.VMEM((ITERS - 1, TILES, FRAME, LANES), F32),
            pltpu.VMEM((TILES, FRAME, LANES), F32),
            pltpu.VMEM((TILES, FRAME, LANES), F32),
            pltpu.VMEM((TILES, FRAME, LANES), F32),
            pltpu.VMEM((ITERS - 1, TILES, FRAME + 16, LANES), F32),
            pltpu.VMEM((3, TILES, FRAME - 8, LANES), F32),
        ],
        compiler_params=pltpu.CompilerParams(
            dimension_semantics=("arbitrary",), vmem_limit_bytes=18 << 20
        ),
        name="adjoint",
    )(all_dots, vecs, links, wet, cost_weights, wside, band_s, band_n)


def solution(mesh):
    return jax.shard_map(
        body,
        mesh=mesh,
        in_specs=(P("lat", "lon"),) * 5 + (P(None, "lat", "lon"),),
        out_specs=(P(None, "lat", "lon"),) * 3,
        check_vma=False,
    )
```

```python
import functools

import jax
import jax.numpy as jnp
from jax import lax
from jax.experimental import pallas as pl
from jax.experimental.pallas import tpu as pltpu
from jax.sharding import PartitionSpec as P

ITERS = 6
COSTS = 8
ROWS = 64
COLS = 256
LANES = 128
TILES = 3
PAIR = 2
DEEP = 13
SLIM = 6
EDGE = 16
FIELDS = 5
FRAME = 80
TALL = 96
MSG_W = FIELDS * EDGE
MSG = MSG_W + COSTS * 8
N_LAM = COSTS * ITERS
N_RHS = N_LAM
N_MAT = N_LAM + ITERS
F32 = jnp.float32
HIGH = lax.Precision.HIGHEST


def lane_index(rows):
    return lax.broadcasted_iota(jnp.int32, (rows, LANES), 1)


def turn(value, amount):
    return pltpu.roll(value, amount % value.shape[1], 1)


def starts(shift):
    wides = [DEEP] * FIELDS + [SLIM] * COSTS
    firsts = [sum(wides[:k]) - (wides[k] if shift else 0) for k in range(len(wides))]
    return list(zip(firsts, wides))


def pack(rows, tiles, shift):
    lane = lane_index(rows)
    out = jnp.zeros((rows, LANES), F32)
    for entry, (at, wide) in zip(tiles, starts(shift)):
        if entry is not None:
            tile, first = entry
            here = (lane >= at) & (lane < at + wide) if at >= 0 else lane >= at + LANES
            out = jnp.where(here, turn(tile, at - first), out)
    return out


def bands_kernel(f, de, dn, st, mask, w, to_north, to_south, whole_mask, sems):
    copies = []
    for side, out in enumerate((to_north, to_south)):
        low = ROWS - EDGE if side == 0 else 0
        rows = pl.ds(low, EDGE)
        for k, field in enumerate((f, de, dn, st)):
            copies.append((field.at[rows, :], out.at[pl.ds(EDGE * k, EDGE), :]))
        copies.append((mask.at[rows, :], whole_mask.at[side]))
        low = ROWS - 8 if side == 0 else 0
        for n in range(COSTS):
            copies.append((w.at[n, pl.ds(low, 8), :], out.at[pl.ds(MSG_W + 8 * n, 8), :]))
    copies = [
        pltpu.make_async_copy(src, dst, sems.at[i]) for i, (src, dst) in enumerate(copies)
    ]
    for copy in copies:
        copy.start()
    for copy in copies:
        copy.wait()
    to_north[MSG_W - EDGE : MSG_W, :] = whole_mask[0].astype(F32)
    to_south[MSG_W - EDGE : MSG_W, :] = whole_mask[1].astype(F32)


def strips_kernel(f, de, dn, st, mask, w, east, west):
    fields = [f[...], de[...], dn[...], st[...], mask[...].astype(F32)]
    right = [(v[:, LANES:], LANES - DEEP) for v in fields]
    left = [(v[:, :LANES], 0) for v in fields]
    right += [(w[n, :, LANES:], LANES - SLIM) for n in range(COSTS)]
    left += [(w[n, :, :LANES], 0) for n in range(COSTS)]
    east[...] = pack(ROWS, right, True)
    west[...] = pack(ROWS, left, False)


def corners_kernel(east, west, bs, bn, to_east, to_west):
    for own, out, lanes, first in ((east, to_east, slice(LANES, COLS), True), (west, to_west, slice(0, LANES), False)):
        out[EDGE : EDGE + ROWS, :] = own[...]
        for band, low, slim in ((bs, 0, 1), (bn, EDGE + ROWS, 0)):
            for half in range(2):
                tiles = []
                for k in range(FIELDS):
                    at = EDGE * k + 8 * half
                    tiles.append((band[at : at + 8, lanes], LANES - DEEP if first else 0))
                for n in range(COSTS):
                    at = MSG_W + 8 * n
                    entry = (band[at : at + 8, lanes], LANES - SLIM if first else 0)
                    tiles.append(entry if half == slim else None)
                out[low + 8 * half : low + 8 * half + 8, :] = pack(8, tiles, first)


def side_tile(pw, pe, k):
    lane = lane_index(pw.shape[0])
    at, wide = starts(False)[k]
    both = jnp.where((lane >= at) & (lane < at + wide), pe, pw)
    return jnp.where((lane < wide) | (lane >= LANES - wide), turn(both, -at), 0.0)


def east_of(tiles):
    last = lane_index(8) == LANES - 1
    turned = [pltpu.roll(tile, LANES - 1, 1) for tile in tiles]
    return [jnp.where(last, turned[(t + 1) % TILES], turned[t]) for t in range(TILES)]


def west_of(tiles):
    first = lane_index(8) == 0
    turned = [pltpu.roll(tile, 1, 1) for tile in tiles]
    return [jnp.where(first, turned[t - 1], turned[t]) for t in range(TILES)]


def forward_kernel(
    flags, f, de, dn, st, mask, w, ls, ln, sw, se,
    vecs, links, wside, wet, dots,
    raw, north, vec, link, diag, part,
):
    own = (f, de, dn, st, mask)
    blocks = range(TALL // 8)
    tiles = range(TILES)
    for rb in blocks:
        at = 8 + 8 * rb
        src, off = None, 8 * rb - EDGE
        if rb < 2:
            src, off = ls, 8 * rb
        elif rb >= 10:
            src, off = ln, 8 * rb - 80
        pw, pe = sw[8 * rb : 8 * rb + 8, :], se[8 * rb : 8 * rb + 8, :]
        for k in range(FIELDS):
            values = []
            for t in range(2):
                lanes = slice(LANES * t, LANES * (t + 1))
                if src is None:
                    values.append(own[k][off : off + 8, lanes].astype(F32))
                else:
                    values.append(src[EDGE * k + off : EDGE * k + off + 8, lanes])
            values.append(side_tile(pw, pe, k))
            if k == FIELDS - 1 and src is not None:
                inside = flags[0 if rb < 2 else 1] > 0
                values = [jnp.where(inside, value, 0.0) for value in values]
            for t in tiles:
                raw[k, t, at : at + 8, :] = values[t]
        if 1 <= rb < 11:
            for n in range(COSTS):
                wside[n, 8 * rb - 8 : 8 * rb, :] = side_tile(pw, pe, FIELDS + n)
    for rb in blocks:
        here = slice(8 + 8 * rb, 16 + 8 * rb)
        above = slice(9 + 8 * rb, 17 + 8 * rb)
        for t in tiles:
            mn = raw[4, t, here, :] * raw[4, t, above, :]
            north[t, here, :] = raw[2, t, here, :] * mn
            if 2 <= rb < 10 and t < 2:
                wet[1, 8 * rb - 16 : 8 * rb - 8, LANES * t : LANES * (t + 1)] = mn
    for rb in blocks:
        here = slice(8 + 8 * rb, 16 + 8 * rb)
        below = slice(7 + 8 * rb, 15 + 8 * rb)
        m = [raw[4, t, here, :] for t in tiles]
        me = [a * b for a, b in zip(m, east_of(m))]
        ex = [raw[1, t, here, :] * me[t] for t in tiles]
        exw = west_of(ex)
        for t in tiles:
            ey, eys = north[t, here, :], north[t, below, :]
            total = m[t] * raw[3, t, here, :] + 1.0 - m[t] + ex[t] + exw[t] + ey + eys
            inv = 1.0 / total
            twice = inv + inv
            v0 = raw[0, t, here, :] * inv
            vec[0, t, here, :] = v0
            values = [twice * face for face in (ex[t], exw[t], ey, eys)]
            for k in range(4):
                link[k, t, here, :] = values[k]
            if 1 <= rb < 11:
                to = slice(8 * rb - 8, 8 * rb)
                vecs[0, t, to, :] = v0
                vecs[ITERS + 1, t, to, :] = twice
                for k in range(4):
                    links[k, t, to, :] = values[k]
            if 2 <= rb < 10 and t < 2:
                to, lanes = slice(8 * rb - 16, 8 * rb - 8), slice(LANES * t, LANES * (t + 1))
                wet[0, to, lanes] = me[t]
                diag[to, lanes] = total
    for j in range(ITERS):
        for rb in blocks:
            here = slice(8 + 8 * rb, 16 + 8 * rb)
            above = slice(9 + 8 * rb, 17 + 8 * rb)
            below = slice(7 + 8 * rb, 15 + 8 * rb)
            v = [vec[j, t, here, :] for t in tiles]
            ve, vw = east_of(v), west_of(v)
            for t in tiles:
                new = (
                    link[0, t, here, :] * ve[t]
                    + link[1, t, here, :] * vw[t]
                    + link[2, t, here, :] * vec[j, t, above, :]
                    + link[3, t, here, :] * vec[j, t, below, :]
                )
                new = 0.5 * new if j == 0 else new - vec[j - 1, t, here, :]
                vec[j + 1, t, here, :] = new
                if 1 <= rb < 11:
                    vecs[j + 1, t, 8 * rb - 8 : 8 * rb, :] = new
    count = ITERS + ITERS * (ITERS + 1) // 2
    own_tiles = [(rb, t) for rb in range(ROWS // 8) for t in range(2)]
    sums = [None] * count
    for rb, t in own_tiles:
        here, lanes = slice(8 * rb, 8 * rb + 8), slice(LANES * t, LANES * (t + 1))
        vs = [vec[j, t, 24 + 8 * rb : 32 + 8 * rb, :] for j in range(ITERS + 1)]
        total = diag[here, lanes]
        forcing = f[here, lanes]
        terms = [forcing * vs[j] for j in range(ITERS)]
        for j in range(ITERS):
            turned = vs[1] if j == 0 else 0.5 * (vs[j + 1] + vs[j - 1])
            image = total * (vs[j] - turned)
            terms += [image * vs[i] for i in range(j + 1)]
        sums = [b if a is None else a + b for a, b in zip(sums, terms)]
    part[N_RHS + count :, :] = jnp.zeros((LANES - N_RHS - count, LANES), F32)
    for k in range(count):
        part[N_RHS + k : N_RHS + k + 1, :] = jnp.sum(sums[k], axis=0, keepdims=True)
    for n in range(COSTS):
        sums = [None] * ITERS
        for rb, t in own_tiles:
            weight = w[n, 8 * rb : 8 * rb + 8, LANES * t : LANES * (t + 1)]
            for j in range(ITERS):
                term = weight * vec[j, t, 24 + 8 * rb : 32 + 8 * rb, :]
                sums[j] = term if sums[j] is None else sums[j] + term
        for j in range(ITERS):
            k = COSTS * j + n
            part[k : k + 1, :] = jnp.sum(sums[j], axis=0, keepdims=True)
    row = lax.dot_general(
        jnp.ones((8, LANES), F32), part[...], (((1,), (1,)), ((), ())),
        precision=HIGH, preferred_element_type=F32,
    )
    for at in range(0, dots.shape[0], 8):
        dots[at : at + 8, :] = row


def small_solve(total):
    wide = lambda k: jnp.broadcast_to(total[k : k + 1, :], (8, LANES))
    mat = {}
    k = N_MAT
    for j in range(ITERS):
        for i in range(j + 1):
            mat[j, i] = wide(k)
            k += 1
    low, inv = {}, []
    for j in range(ITERS):
        pivot = mat[j, j]
        for k in range(j):
            pivot = pivot - low[j, k] * mat[j, k]
        inv.append(1.0 / pivot)
        for i in range(j + 1, ITERS):
            entry = mat[i, j]
            for k in range(j):
                entry = entry - low[j, k] * mat[i, k]
            mat[i, j] = entry
            low[i, j] = entry * inv[j]

    def solve(rhs):
        y = []
        for i in range(ITERS):
            t = rhs[i]
            for k in range(i):
                t = t - low[i, k] * y[k]
            y.append(t)
        out = [None] * ITERS
        for i in range(ITERS - 1, -1, -1):
            t = y[i] * inv[i]
            for k in range(i + 1, ITERS):
                t = t - low[k, i] * out[k]
            out[i] = t
        return out

    return (
        solve([wide(N_RHS + i) for i in range(ITERS)]),
        solve([total[COSTS * j : COSTS * (j + 1), :] for j in range(ITERS)]),
    )


def imaged(coef):
    get = lambda k: coef[k] if 0 <= k < ITERS else None
    out = []
    for k in range(ITERS + 1):
        low, mid, high = get(k - 1), get(k), get(k + 1)
        value = jnp.zeros_like(coef[0]) if mid is None else mid + mid
        if low is not None:
            value = value - (low + low if k == 1 else low)
        if high is not None:
            value = value - high
        out.append(value)
    return out


def mixed(factors, values):
    total = None
    for factor, value in zip(factors, values):
        term = factor * value
        total = term if total is None else total + term
    return total


def adjoint_kernel(
    all_dots, vecs, links, wet, w, wside, ws, wn,
    adj, east, north,
    lam, lam2, cs, slope, lag, rs, ys, ss, ps, acc,
):
    n = pl.program_id(0)
    blocks = range(FRAME // 8)
    tiles = range(TILES)
    lanes_of = lambda t: slice(LANES * t, LANES * (t + 1))

    @pl.when(n == 0)
    def _():
        rows = [all_dots[at : at + 8, :] for at in range(0, all_dots.shape[0], 8)]
        while len(rows) > 1:
            rows = [a + b for a, b in zip(rows[::2], rows[1::2])]
        total = lax.dot_general(
            rows[0], jnp.ones((8, LANES), F32), (((0,), (0,)), ((), ())),
            precision=HIGH, preferred_element_type=F32,
        )
        c, weights = small_solve(total)
        for j in range(ITERS):
            lam[8 * j : 8 * j + 8, :] = weights[j]
            cs[8 * j : 8 * j + 8, :] = c[j]
        for k, value in enumerate(imaged(weights)):
            lam2[8 * k : 8 * k + 8, :] = value
        c2 = imaged(c)
        for rb in blocks:
            here = slice(8 * rb, 8 * rb + 8)
            for t in tiles:
                v = [vecs[k, t, here, :] for k in range(ITERS + 1)]
                rs[t, here, :] = v[0] + v[0] - mixed(c2, v)
                if rb >= 1:
                    lag[0, t, here, :] = v[1] - v[0]
                    for j in range(1, ITERS - 1):
                        lag[j, t, here, :] = 0.5 * (v[j + 1] + v[j - 1]) - v[j]
        for rb in range(1, 9):
            here = slice(8 * rb, 8 * rb + 8)
            above = slice(8 * rb + 1, 8 * rb + 9)
            to = slice(8 * rb - 8, 8 * rb)
            sums = [[None, None], [None, None]]
            for j in range(ITERS):
                v = [vecs[j, t, here, :] for t in tiles]
                ve = east_of(v)
                for t in range(2):
                    for d, near in enumerate((ve[t], vecs[j, t, above, :])):
                        step = v[t] - near
                        if j < ITERS - 1:
                            slope[d, j, t, to, :] = step
                        term = c[j] * step
                        sums[d][t] = term if j == 0 else sums[d][t] + term
            for d in range(2):
                for t in range(2):
                    slope[d, ITERS - 1, t, to, :] = sums[d][t]

    pair = range(PAIR)
    spread = lambda ref, k, h: jnp.broadcast_to(ref[pl.ds(8 * k + PAIR * n + h, 1), :], (8, LANES))
    rows = [[spread(lam, j, h) for j in range(ITERS)] for h in pair]
    rows2 = [[spread(lam2, k, h) for k in range(ITERS + 1)] for h in pair]
    last = ITERS - 1
    c_last = cs[8 * last : 8 * last + 8, :]
    lagged = lambda rb: slice(8 * rb - 8, 8 * rb)
    for rb in blocks:
        at = 8 + 8 * rb
        here = slice(8 * rb, 8 * rb + 8)
        for t in tiles:
            v = [vecs[k, t, here, :] for k in range(ITERS + 1)]
            scale, res = vecs[ITERS + 1, t, here, :], rs[t, here, :]
            for h in pair:
                if t == 2:
                    weight = wside[h, here, :]
                elif rb == 0:
                    weight = ws[8 * h : 8 * h + 8, lanes_of(t)]
                elif rb == 9:
                    weight = wn[8 * h : 8 * h + 8, lanes_of(t)]
                else:
                    weight = w[h, lagged(rb), lanes_of(t)]
                s = scale * weight - mixed(rows2[h], v)
                ss[h, t, here, :] = s
                ps[h, last - 1, t, at : at + 8, :] = c_last * s + rows[h][last] * res
                if rb >= 1:
                    ys[h, t, here, :] = mixed(rows[h], v)
    for rb in range(1, 9):
        here = slice(8 * rb, 8 * rb + 8)
        above = slice(8 * rb + 1, 8 * rb + 9)
        to = lagged(rb)
        for h in pair:
            y = [ys[h, t, here, :] for t in tiles]
            ye = east_of(y)
            for t in range(2):
                acc[h, 0, t, to, :] = (y[t] - ye[t]) * slope[0, last, t, to, :]
                acc[h, 1, t, to, :] = (y[t] - ys[h, t, above, :]) * slope[1, last, t, to, :]
    for j in range(ITERS - 2, -1, -1):
        c_j = cs[8 * j : 8 * j + 8, :]
        for rb in blocks:
            if j == 0 and rb == 0:
                continue
            at = 8 + 8 * rb
            here = slice(8 * rb, 8 * rb + 8)
            p = [[ps[h, j, t, at : at + 8, :] for t in tiles] for h in pair]
            pe, pw = [east_of(q) for q in p], [west_of(q) for q in p]
            for t in tiles:
                link = [links[k, t, here, :] for k in range(4)]
                res = rs[t, here, :]
                if rb >= 1:
                    late = lag[j, t, here, :]
                    if j == 0:
                        v0 = vecs[0, t, here, :]
                inside = 1 <= rb < 9 and t < 2
                if inside:
                    to = lagged(rb)
                    slope_e, slope_n = slope[0, j, t, to, :], slope[1, j, t, to, :]
                for h in pair:
                    here_p = p[h][t]
                    pn = ps[h, j, t, at + 1 : at + 9, :]
                    bar = (
                        link[0] * pe[h][t] + link[1] * pw[h][t]
                        + link[2] * pn + link[3] * ps[h, j, t, at - 1 : at + 7, :]
                    ) + (c_j * ss[h, t, here, :] + rows[h][j] * res)
                    if j < ITERS - 2:
                        bar = bar - ps[h, j + 1, t, at : at + 8, :]
                    if j == 1:
                        bar = 0.5 * bar
                    if j > 0:
                        ps[h, j - 1, t, at : at + 8, :] = bar
                    if rb >= 1:
                        d = here_p * late
                        if j < ITERS - 2:
                            d = acc[h, 2, t, lagged(rb), :] + d
                        if j == 0:
                            g = 0.5 * bar
                            d = d + g * v0
                        acc[h, 2, t, lagged(rb), :] = d
                    if inside:
                        acc[h, 0, t, to, :] = acc[h, 0, t, to, :] + (here_p - pe[h][t]) * slope_e
                        acc[h, 1, t, to, :] = acc[h, 1, t, to, :] + (here_p - pn) * slope_n
                        if j == 0:
                            adj[h, to, lanes_of(t)] = ys[h, t, here, :] + g
    for rb in range(ROWS // 8):
        to = slice(8 * rb, 8 * rb + 8)
        for h in pair:
            d = [acc[h, 2, t, to, :] for t in tiles]
            de = east_of(d)
            for t in range(2):
                above = acc[h, 2, t, 8 * rb + 1 : 8 * rb + 9, :]
                east[h, to, lanes_of(t)] = -wet[0, to, lanes_of(t)] * (acc[h, 0, t, to, :] + d[t] + de[t])
                north[h, to, lanes_of(t)] = -wet[1, to, lanes_of(t)] * (acc[h, 1, t, to, :] + d[t] + above)


def ring(axis, steps):
    count = lax.axis_size(axis)
    return [(source, (source + steps) % count) for source in range(count)]


def struct(*shape):
    return jax.ShapeDtypeStruct(shape, F32)


def whole():
    return pl.BlockSpec(memory_space=pltpu.VMEM)


def body(forcing, depth_east, depth_north, surface_term, ocean_mask, cost_weights):
    args = (forcing, depth_east, depth_north, surface_term, ocean_mask, cost_weights)
    lats = lax.axis_size("lat")
    devices = lats * lax.axis_size("lon")
    small = pltpu.CompilerParams(vmem_limit_bytes=4 << 20)
    to_north, to_south = pl.pallas_call(
        bands_kernel,
        in_specs=[pl.BlockSpec(memory_space=pltpu.HBM)] * 6,
        out_specs=[whole()] * 2,
        out_shape=(struct(MSG, COLS),) * 2,
        scratch_shapes=[
            pltpu.VMEM((2, EDGE, COLS), jnp.int32),
            pltpu.SemaphoreType.DMA((2 * (FIELDS + COSTS),)),
        ],
        compiler_params=small,
        name="bands",
    )(*[pltpu.with_memory_space_constraint(arg, pltpu.HBM) for arg in args])
    band_s = lax.ppermute(to_north, "lat", ring("lat", 1))
    band_n = lax.ppermute(to_south, "lat", ring("lat", -1))
    east, west = pl.pallas_call(
        strips_kernel,
        in_specs=[whole()] * 6,
        out_specs=[whole()] * 2,
        out_shape=(struct(ROWS, LANES),) * 2,
        compiler_params=small,
        name="strips",
    )(*args)
    to_east, to_west = pl.pallas_call(
        corners_kernel,
        in_specs=[whole()] * 4,
        out_specs=[whole()] * 2,
        out_shape=(struct(TALL, LANES),) * 2,
        compiler_params=small,
        name="corners",
    )(east, west, band_s, band_n)
    side_w = lax.ppermute(to_east, "lon", ring("lon", 1))
    side_e = lax.ppermute(to_west, "lon", ring("lon", -1))
    row = lax.axis_index("lat")
    flags = jnp.stack([row > 0, row < lats - 1]).astype(jnp.int32)
    vecs, links, wside, wet, dots = pl.pallas_call(
        forward_kernel,
        in_specs=[pl.BlockSpec(memory_space=pltpu.SMEM)] + [whole()] * 10,
        out_specs=[whole()] * 5,
        out_shape=(
            struct(ITERS + 2, TILES, FRAME, LANES), struct(4, TILES, FRAME, LANES),
            struct(COSTS, FRAME, LANES),
            struct(2, ROWS, COLS), struct(devices, LANES),
        ),
        scratch_shapes=[
            pltpu.VMEM((FIELDS, TILES, TALL + 16, LANES), F32),
            pltpu.VMEM((TILES, TALL + 16, LANES), F32),
            pltpu.VMEM((ITERS + 1, TILES, TALL + 16, LANES), F32),
            pltpu.VMEM((4, TILES, TALL + 16, LANES), F32),
            pltpu.VMEM((ROWS, COLS), F32),
            pltpu.VMEM((LANES, LANES), F32),
        ],
        compiler_params=pltpu.CompilerParams(vmem_limit_bytes=14 << 20),
        name="forward",
    )(flags, *args, band_s, band_n, side_w, side_e)
    all_dots = lax.all_to_all(dots, ("lat", "lon"), 0, 0, tiled=True)
    out_spec = pl.BlockSpec((PAIR, ROWS, COLS), lambda n: (n, 0, 0))
    return pl.pallas_call(
        adjoint_kernel,
        grid=(COSTS // PAIR,),
        in_specs=[
            whole(),
            whole(),
            whole(),
            whole(),
            pl.BlockSpec((PAIR, ROWS, COLS), lambda n: (n, 0, 0)),
            pl.BlockSpec((PAIR, FRAME, LANES), lambda n: (n, 0, 0)),
            pl.BlockSpec((8 * PAIR, COLS), lambda n: (MSG_W // (8 * PAIR) + n, 0)),
            pl.BlockSpec((8 * PAIR, COLS), lambda n: (MSG_W // (8 * PAIR) + n, 0)),
        ],
        out_specs=[out_spec] * 3,
        out_shape=(struct(COSTS, ROWS, COLS),) * 3,
        scratch_shapes=[
            pltpu.VMEM((N_LAM, LANES), F32),
            pltpu.VMEM((N_LAM + 8, LANES), F32),
            pltpu.VMEM((8 * ITERS, LANES), F32),
            pltpu.VMEM((2, ITERS, 2, ROWS, LANES), F32),
            pltpu.VMEM((ITERS - 1, TILES, FRAME, LANES), F32),
            pltpu.VMEM((TILES, FRAME, LANES), F32),
            pltpu.VMEM((PAIR, TILES, FRAME, LANES), F32),
            pltpu.VMEM((PAIR, TILES, FRAME, LANES), F32),
            pltpu.VMEM((PAIR, ITERS - 1, TILES, FRAME + 16, LANES), F32),
            pltpu.VMEM((PAIR, 3, TILES, FRAME - 8, LANES), F32),
        ],
        compiler_params=pltpu.CompilerParams(
            dimension_semantics=("arbitrary",), vmem_limit_bytes=18 << 20
        ),
        name="adjoint",
    )(all_dots, vecs, links, wet, cost_weights, wside, band_s, band_n)


def solution(mesh):
    return jax.shard_map(
        body,
        mesh=mesh,
        in_specs=(P("lat", "lon"),) * 5 + (P(None, "lat", "lon"),),
        out_specs=(P(None, "lat", "lon"),) * 3,
        check_vma=False,
    )
```

```python
import functools

import jax
import jax.numpy as jnp
from jax import lax
from jax.experimental import pallas as pl
from jax.experimental.pallas import tpu as pltpu
from jax.sharding import PartitionSpec as P

ITERS = 6
COSTS = 8
ROWS = 64
COLS = 256
LANES = 128
TILES = 3
PAIR = 2
DEEP = 13
SLIM = 6
EDGE = 16
FIELDS = 5
FRAME = 80
TALL = 96
MSG_W = FIELDS * EDGE
MSG = MSG_W + COSTS * 8
N_LAM = COSTS * ITERS
N_RHS = N_LAM
N_MAT = N_LAM + ITERS
F32 = jnp.float32
HIGH = lax.Precision.HIGHEST


def lane_index(rows):
    return lax.broadcasted_iota(jnp.int32, (rows, LANES), 1)


def turn(value, amount):
    return pltpu.roll(value, amount % value.shape[1], 1)


def starts(shift):
    wides = [DEEP] * FIELDS + [SLIM] * COSTS
    firsts = [sum(wides[:k]) - (wides[k] if shift else 0) for k in range(len(wides))]
    return list(zip(firsts, wides))


def pack(rows, tiles, shift):
    lane = lane_index(rows)
    out = jnp.zeros((rows, LANES), F32)
    for entry, (at, wide) in zip(tiles, starts(shift)):
        if entry is not None:
            tile, first = entry
            here = (lane >= at) & (lane < at + wide) if at >= 0 else lane >= at + LANES
            out = jnp.where(here, turn(tile, at - first), out)
    return out


def bands_kernel(f, de, dn, st, mask, w, to_north, to_south, whole_mask, sems):
    copies = []
    for side, out in enumerate((to_north, to_south)):
        low = ROWS - EDGE if side == 0 else 0
        rows = pl.ds(low, EDGE)
        for k, field in enumerate((f, de, dn, st)):
            copies.append((field.at[rows, :], out.at[pl.ds(EDGE * k, EDGE), :]))
        copies.append((mask.at[rows, :], whole_mask.at[side]))
        low = ROWS - 8 if side == 0 else 0
        copies.append((w.at[:, pl.ds(low, 8), :], out.at[pl.ds(MSG_W, 8 * COSTS), :].reshape(COSTS, 8, COLS)))
    copies = [
        pltpu.make_async_copy(src, dst, sems.at[i]) for i, (src, dst) in enumerate(copies)
    ]
    for copy in copies:
        copy.start()
    for copy in copies:
        copy.wait()
    to_north[MSG_W - EDGE : MSG_W, :] = whole_mask[0].astype(F32)
    to_south[MSG_W - EDGE : MSG_W, :] = whole_mask[1].astype(F32)


def strips_kernel(f, de, dn, st, mask, w, east, west):
    fields = [f[...], de[...], dn[...], st[...], mask[...].astype(F32)]
    right = [(v[:, LANES:], LANES - DEEP) for v in fields]
    left = [(v[:, :LANES], 0) for v in fields]
    right += [(w[n, :, LANES:], LANES - SLIM) for n in range(COSTS)]
    left += [(w[n, :, :LANES], 0) for n in range(COSTS)]
    east[...] = pack(ROWS, right, True)
    west[...] = pack(ROWS, left, False)


def corners_kernel(east, west, bs, bn, to_east, to_west):
    for own, out, lanes, first in ((east, to_east, slice(LANES, COLS), True), (west, to_west, slice(0, LANES), False)):
        out[EDGE : EDGE + ROWS, :] = own[...]
        for band, low, slim in ((bs, 0, 1), (bn, EDGE + ROWS, 0)):
            for half in range(2):
                tiles = []
                for k in range(FIELDS):
                    at = EDGE * k + 8 * half
                    tiles.append((band[at : at + 8, lanes], LANES - DEEP if first else 0))
                for n in range(COSTS):
                    at = MSG_W + 8 * n
                    entry = (band[at : at + 8, lanes], LANES - SLIM if first else 0)
                    tiles.append(entry if half == slim else None)
                out[low + 8 * half : low + 8 * half + 8, :] = pack(8, tiles, first)


def side_tile(pw, pe, k):
    lane = lane_index(pw.shape[0])
    at, wide = starts(False)[k]
    both = jnp.where((lane >= at) & (lane < at + wide), pe, pw)
    return jnp.where((lane < wide) | (lane >= LANES - wide), turn(both, -at), 0.0)


def east_of(tiles):
    last = lane_index(8) == LANES - 1
    turned = [pltpu.roll(tile, LANES - 1, 1) for tile in tiles]
    return [jnp.where(last, turned[(t + 1) % TILES], turned[t]) for t in range(TILES)]


def west_of(tiles):
    first = lane_index(8) == 0
    turned = [pltpu.roll(tile, 1, 1) for tile in tiles]
    return [jnp.where(first, turned[t - 1], turned[t]) for t in range(TILES)]


def forward_kernel(
    flags, f, de, dn, st, mask, w, ls, ln, sw, se,
    vecs, links, wside, wet, dots,
    raw, north, vec, link, diag, part,
):
    own = (f, de, dn, st, mask)
    blocks = range(TALL // 8)
    tiles = range(TILES)
    for rb in blocks:
        at = 8 + 8 * rb
        src, off = None, 8 * rb - EDGE
        if rb < 2:
            src, off = ls, 8 * rb
        elif rb >= 10:
            src, off = ln, 8 * rb - 80
        pw, pe = sw[8 * rb : 8 * rb + 8, :], se[8 * rb : 8 * rb + 8, :]
        for k in range(FIELDS):
            values = []
            for t in range(2):
                lanes = slice(LANES * t, LANES * (t + 1))
                if src is None:
                    values.append(own[k][off : off + 8, lanes].astype(F32))
                else:
                    values.append(src[EDGE * k + off : EDGE * k + off + 8, lanes])
            values.append(side_tile(pw, pe, k))
            if k == FIELDS - 1 and src is not None:
                inside = flags[0 if rb < 2 else 1]
                values = [inside * value for value in values]
            for t in tiles:
                raw[k, t, at : at + 8, :] = values[t]
        if 1 <= rb < 11:
            for n in range(COSTS):
                wside[n, 8 * rb - 8 : 8 * rb, :] = side_tile(pw, pe, FIELDS + n)
    for rb in blocks:
        here = slice(8 + 8 * rb, 16 + 8 * rb)
        above = slice(9 + 8 * rb, 17 + 8 * rb)
        for t in tiles:
            mn = raw[4, t, here, :] * raw[4, t, above, :]
            north[t, here, :] = raw[2, t, here, :] * mn
            if 2 <= rb < 10 and t < 2:
                wet[1, 8 * rb - 16 : 8 * rb - 8, LANES * t : LANES * (t + 1)] = mn
    for rb in blocks:
        here = slice(8 + 8 * rb, 16 + 8 * rb)
        below = slice(7 + 8 * rb, 15 + 8 * rb)
        m = [raw[4, t, here, :] for t in tiles]
        me = [a * b for a, b in zip(m, east_of(m))]
        ex = [raw[1, t, here, :] * me[t] for t in tiles]
        exw = west_of(ex)
        for t in tiles:
            ey, eys = north[t, here, :], north[t, below, :]
            total = m[t] * raw[3, t, here, :] + 1.0 - m[t] + ex[t] + exw[t] + ey + eys
            inv = 1.0 / total
            twice = inv + inv
            v0 = raw[0, t, here, :] * inv
            vec[0, t, here, :] = v0
            values = [twice * face for face in (ex[t], exw[t], ey, eys)]
            for k in range(4):
                link[k, t, here, :] = values[k]
            if 1 <= rb < 11:
                to = slice(8 * rb - 8, 8 * rb)
                vecs[0, t, to, :] = v0
                vecs[ITERS + 1, t, to, :] = twice
                for k in range(4):
                    links[k, t, to, :] = values[k]
            if 2 <= rb < 10 and t < 2:
                to, lanes = slice(8 * rb - 16, 8 * rb - 8), slice(LANES * t, LANES * (t + 1))
                wet[0, to, lanes] = me[t]
                diag[to, lanes] = total
    for j in range(ITERS):
        for rb in blocks:
            here = slice(8 + 8 * rb, 16 + 8 * rb)
            above = slice(9 + 8 * rb, 17 + 8 * rb)
            below = slice(7 + 8 * rb, 15 + 8 * rb)
            v = [vec[j, t, here, :] for t in tiles]
            ve, vw = east_of(v), west_of(v)
            for t in tiles:
                new = (
                    link[0, t, here, :] * ve[t]
                    + link[1, t, here, :] * vw[t]
                    + link[2, t, here, :] * vec[j, t, above, :]
                    + link[3, t, here, :] * vec[j, t, below, :]
                )
                new = 0.5 * new if j == 0 else new - vec[j - 1, t, here, :]
                vec[j + 1, t, here, :] = new
                if 1 <= rb < 11:
                    vecs[j + 1, t, 8 * rb - 8 : 8 * rb, :] = new
    count = ITERS + ITERS * (ITERS + 1) // 2
    own_tiles = [(rb, t) for rb in range(ROWS // 8) for t in range(2)]
    sums = [None] * count
    for rb, t in own_tiles:
        here, lanes = slice(8 * rb, 8 * rb + 8), slice(LANES * t, LANES * (t + 1))
        vs = [vec[j, t, 24 + 8 * rb : 32 + 8 * rb, :] for j in range(ITERS + 1)]
        total = diag[here, lanes]
        forcing = f[here, lanes]
        terms = [forcing * vs[j] for j in range(ITERS)]
        for j in range(ITERS):
            turned = vs[1] if j == 0 else 0.5 * (vs[j + 1] + vs[j - 1])
            image = total * (vs[j] - turned)
            terms += [image * vs[i] for i in range(j + 1)]
        sums = [b if a is None else a + b for a, b in zip(sums, terms)]
    part[N_RHS + count :, :] = jnp.zeros((LANES - N_RHS - count, LANES), F32)
    for k in range(count):
        part[N_RHS + k : N_RHS + k + 1, :] = jnp.sum(sums[k], axis=0, keepdims=True)
    for n in range(COSTS):
        sums = [None] * ITERS
        for rb, t in own_tiles:
            weight = w[n, 8 * rb : 8 * rb + 8, LANES * t : LANES * (t + 1)]
            for j in range(ITERS):
                term = weight * vec[j, t, 24 + 8 * rb : 32 + 8 * rb, :]
                sums[j] = term if sums[j] is None else sums[j] + term
        for j in range(ITERS):
            k = COSTS * j + n
            part[k : k + 1, :] = jnp.sum(sums[j], axis=0, keepdims=True)
    row = lax.dot_general(
        jnp.ones((8, LANES), F32), part[...], (((1,), (1,)), ((), ())),
        precision=HIGH, preferred_element_type=F32,
    )
    for at in range(0, dots.shape[0], 8):
        dots[at : at + 8, :] = row


def small_solve(total):
    wide = lambda k: jnp.broadcast_to(total[k : k + 1, :], (8, LANES))
    mat = {}
    k = N_MAT
    for j in range(ITERS):
        for i in range(j + 1):
            mat[j, i] = wide(k)
            k += 1
    low, inv = {}, []
    for j in range(ITERS):
        pivot = mat[j, j]
        for k in range(j):
            pivot = pivot - low[j, k] * mat[j, k]
        inv.append(1.0 / pivot)
        for i in range(j + 1, ITERS):
            entry = mat[i, j]
            for k in range(j):
                entry = entry - low[j, k] * mat[i, k]
            mat[i, j] = entry
            low[i, j] = entry * inv[j]

    def solve(rhs):
        y = []
        for i in range(ITERS):
            t = rhs[i]
            for k in range(i):
                t = t - low[i, k] * y[k]
            y.append(t)
        out = [None] * ITERS
        for i in range(ITERS - 1, -1, -1):
            t = y[i] * inv[i]
            for k in range(i + 1, ITERS):
                t = t - low[k, i] * out[k]
            out[i] = t
        return out

    return (
        solve([wide(N_RHS + i) for i in range(ITERS)]),
        solve([total[COSTS * j : COSTS * (j + 1), :] for j in range(ITERS)]),
    )


def imaged(coef):
    get = lambda k: coef[k] if 0 <= k < ITERS else None
    out = []
    for k in range(ITERS + 1):
        low, mid, high = get(k - 1), get(k), get(k + 1)
        value = jnp.zeros_like(coef[0]) if mid is None else mid + mid
        if low is not None:
            value = value - (low + low if k == 1 else low)
        if high is not None:
            value = value - high
        out.append(value)
    return out


def mixed(factors, values):
    total = None
    for factor, value in zip(factors, values):
        term = factor * value
        total = term if total is None else total + term
    return total


def adjoint_kernel(
    all_dots, vecs, links, wet, w, wside, ws, wn,
    adj, east, north,
    lam, lam2, cs, slope, lag, rs, ys, ss, ps, acc,
):
    n = pl.program_id(0)
    blocks = range(FRAME // 8)
    tiles = range(TILES)
    lanes_of = lambda t: slice(LANES * t, LANES * (t + 1))

    @pl.when(n == 0)
    def _():
        rows = [all_dots[at : at + 8, :] for at in range(0, all_dots.shape[0], 8)]
        while len(rows) > 1:
            rows = [a + b for a, b in zip(rows[::2], rows[1::2])]
        total = lax.dot_general(
            rows[0], jnp.ones((8, LANES), F32), (((0,), (0,)), ((), ())),
            precision=HIGH, preferred_element_type=F32,
        )
        for rb in range(1, 10):
            here = slice(8 * rb, 8 * rb + 8)
            above = slice(8 * rb + 1, 8 * rb + 9)
            to = slice(8 * rb - 8, 8 * rb)
            for j in range(ITERS):
                v = [vecs[j, t, here, :] for t in tiles]
                if j < ITERS - 1:
                    for t in tiles:
                        later = vecs[j + 1, t, here, :]
                        if j > 0:
                            later = 0.5 * (later + vecs[j - 1, t, here, :])
                        lag[j, t, here, :] = later - v[t]
                if rb < 9:
                    ve = east_of(v)
                    for t in range(2):
                        slope[0, j, t, to, :] = v[t] - ve[t]
                        slope[1, j, t, to, :] = v[t] - vecs[j, t, above, :]
        c, weights = small_solve(total)
        for j in range(ITERS):
            lam[8 * j : 8 * j + 8, :] = weights[j]
            cs[8 * j : 8 * j + 8, :] = c[j]
        for k, value in enumerate(imaged(weights)):
            lam2[8 * k : 8 * k + 8, :] = value
        c2 = imaged(c)
        for rb in blocks:
            here = slice(8 * rb, 8 * rb + 8)
            for t in tiles:
                v = [vecs[k, t, here, :] for k in range(ITERS + 1)]
                rs[t, here, :] = v[0] + v[0] - mixed(c2, v)
        for rb in range(ROWS // 8):
            to = slice(8 * rb, 8 * rb + 8)
            for d in range(2):
                for t in range(2):
                    steps = [slope[d, j, t, to, :] for j in range(ITERS)]
                    slope[d, ITERS - 1, t, to, :] = mixed(c, steps)

    pair = range(PAIR)
    spread = lambda ref, k, h: jnp.broadcast_to(ref[pl.ds(8 * k + PAIR * n + h, 1), :], (8, LANES))
    rows = [[spread(lam, j, h) for j in range(ITERS)] for h in pair]
    rows2 = [[spread(lam2, k, h) for k in range(ITERS + 1)] for h in pair]
    last = ITERS - 1
    c_last = cs[8 * last : 8 * last + 8, :]
    lagged = lambda rb: slice(8 * rb - 8, 8 * rb)
    for rb in blocks:
        at = 8 + 8 * rb
        here = slice(8 * rb, 8 * rb + 8)
        for t in tiles:
            v = [vecs[k, t, here, :] for k in range(ITERS + 1)]
            scale, res = vecs[ITERS + 1, t, here, :], rs[t, here, :]
            for h in pair:
                if t == 2:
                    weight = wside[h, here, :]
                elif rb == 0:
                    weight = ws[8 * h : 8 * h + 8, lanes_of(t)]
                elif rb == 9:
                    weight = wn[8 * h : 8 * h + 8, lanes_of(t)]
                else:
                    weight = w[h, lagged(rb), lanes_of(t)]
                s = scale * weight - mixed(rows2[h], v)
                ss[h, t, here, :] = s
                ps[h, last - 1, t, at : at + 8, :] = c_last * s + rows[h][last] * res
                if rb >= 1:
                    ys[h, t, here, :] = mixed(rows[h], v)
    for rb in range(1, 9):
        here = slice(8 * rb, 8 * rb + 8)
        above = slice(8 * rb + 1, 8 * rb + 9)
        to = lagged(rb)
        for h in pair:
            y = [ys[h, t, here, :] for t in tiles]
            ye = east_of(y)
            for t in range(2):
                acc[h, 0, t, to, :] = (y[t] - ye[t]) * slope[0, last, t, to, :]
                acc[h, 1, t, to, :] = (y[t] - ys[h, t, above, :]) * slope[1, last, t, to, :]
    for j in range(ITERS - 2, -1, -1):
        c_j = cs[8 * j : 8 * j + 8, :]
        for rb in blocks:
            if j == 0 and rb == 0:
                continue
            at = 8 + 8 * rb
            here = slice(8 * rb, 8 * rb + 8)
            p = [[ps[h, j, t, at : at + 8, :] for t in tiles] for h in pair]
            pe, pw = [east_of(q) for q in p], [west_of(q) for q in p]
            for t in tiles:
                link = [links[k, t, here, :] for k in range(4)]
                res = rs[t, here, :]
                if rb >= 1:
                    late = lag[j, t, here, :]
                    if j == 0:
                        v0 = vecs[0, t, here, :]
                inside = 1 <= rb < 9 and t < 2
                if inside:
                    to = lagged(rb)
                    slope_e, slope_n = slope[0, j, t, to, :], slope[1, j, t, to, :]
                for h in pair:
                    here_p = p[h][t]
                    pn = ps[h, j, t, at + 1 : at + 9, :]
                    bar = (
                        link[0] * pe[h][t] + link[1] * pw[h][t]
                        + link[2] * pn + link[3] * ps[h, j, t, at - 1 : at + 7, :]
                    ) + (c_j * ss[h, t, here, :] + rows[h][j] * res)
                    if j < ITERS - 2:
                        bar = bar - ps[h, j + 1, t, at : at + 8, :]
                    if j == 1:
                        bar = 0.5 * bar
                    if j > 0:
                        ps[h, j - 1, t, at : at + 8, :] = bar
                    if rb >= 1:
                        d = here_p * late
                        if j < ITERS - 2:
                            d = acc[h, 2, t, lagged(rb), :] + d
                        if j == 0:
                            g = 0.5 * bar
                            d = d + g * v0
                        acc[h, 2, t, lagged(rb), :] = d
                    if inside:
                        acc[h, 0, t, to, :] = acc[h, 0, t, to, :] + (here_p - pe[h][t]) * slope_e
                        acc[h, 1, t, to, :] = acc[h, 1, t, to, :] + (here_p - pn) * slope_n
                        if j == 0:
                            adj[h, to, lanes_of(t)] = ys[h, t, here, :] + g
    for rb in range(ROWS // 8):
        to = slice(8 * rb, 8 * rb + 8)
        for h in pair:
            d = [acc[h, 2, t, to, :] for t in tiles]
            de = east_of(d)
            for t in range(2):
                above = acc[h, 2, t, 8 * rb + 1 : 8 * rb + 9, :]
                east[h, to, lanes_of(t)] = -wet[0, to, lanes_of(t)] * (acc[h, 0, t, to, :] + d[t] + de[t])
                north[h, to, lanes_of(t)] = -wet[1, to, lanes_of(t)] * (acc[h, 1, t, to, :] + d[t] + above)


def ring(axis, steps):
    count = lax.axis_size(axis)
    return [(source, (source + steps) % count) for source in range(count)]


def struct(*shape):
    return jax.ShapeDtypeStruct(shape, F32)


def whole():
    return pl.BlockSpec(memory_space=pltpu.VMEM)


def body(forcing, depth_east, depth_north, surface_term, ocean_mask, cost_weights):
    args = (forcing, depth_east, depth_north, surface_term, ocean_mask, cost_weights)
    lats = lax.axis_size("lat")
    devices = lats * lax.axis_size("lon")
    small = pltpu.CompilerParams(vmem_limit_bytes=4 << 20)
    to_north, to_south = pl.pallas_call(
        bands_kernel,
        in_specs=[pl.BlockSpec(memory_space=pltpu.HBM)] * 6,
        out_specs=[whole()] * 2,
        out_shape=(struct(MSG, COLS),) * 2,
        scratch_shapes=[
            pltpu.VMEM((2, EDGE, COLS), jnp.int32),
            pltpu.SemaphoreType.DMA((2 * (FIELDS + 1),)),
        ],
        compiler_params=small,
        name="bands",
    )(*[pltpu.with_memory_space_constraint(arg, pltpu.HBM) for arg in args])
    band_s = lax.ppermute(to_north, "lat", ring("lat", 1))
    band_n = lax.ppermute(to_south, "lat", ring("lat", -1))
    east, west = pl.pallas_call(
        strips_kernel,
        in_specs=[whole()] * 6,
        out_specs=[whole()] * 2,
        out_shape=(struct(ROWS, LANES),) * 2,
        compiler_params=small,
        name="strips",
    )(*args)
    to_east, to_west = pl.pallas_call(
        corners_kernel,
        in_specs=[whole()] * 4,
        out_specs=[whole()] * 2,
        out_shape=(struct(TALL, LANES),) * 2,
        compiler_params=small,
        name="corners",
    )(east, west, band_s, band_n)
    side_w = lax.ppermute(to_east, "lon", ring("lon", 1))
    side_e = lax.ppermute(to_west, "lon", ring("lon", -1))
    row = lax.axis_index("lat")
    flags = jnp.stack([row > 0, row < lats - 1, row > 0, row > 0]).astype(F32)
    flags = jnp.broadcast_to(flags[:, None, None], (4, 8, LANES))
    vecs, links, wside, wet, dots = pl.pallas_call(
        forward_kernel,
        in_specs=[whole()] * 11,
        out_specs=[whole()] * 5,
        out_shape=(
            struct(ITERS + 2, TILES, FRAME, LANES), struct(4, TILES, FRAME, LANES),
            struct(COSTS, FRAME, LANES),
            struct(2, ROWS, COLS), struct(devices, LANES),
        ),
        scratch_shapes=[
            pltpu.VMEM((FIELDS, TILES, TALL + 16, LANES), F32),
            pltpu.VMEM((TILES, TALL + 16, LANES), F32),
            pltpu.VMEM((ITERS + 1, TILES, TALL + 16, LANES), F32),
            pltpu.VMEM((4, TILES, TALL + 16, LANES), F32),
            pltpu.VMEM((ROWS, COLS), F32),
            pltpu.VMEM((LANES, LANES), F32),
        ],
        compiler_params=pltpu.CompilerParams(vmem_limit_bytes=14 << 20),
        name="forward",
    )(flags, *args, band_s, band_n, side_w, side_e)
    all_dots = lax.all_to_all(dots, ("lat", "lon"), 0, 0, tiled=True)
    out_spec = pl.BlockSpec((PAIR, ROWS, COLS), lambda n: (n, 0, 0))
    return pl.pallas_call(
        adjoint_kernel,
        grid=(COSTS // PAIR,),
        in_specs=[
            whole(),
            whole(),
            whole(),
            whole(),
            pl.BlockSpec((PAIR, ROWS, COLS), lambda n: (n, 0, 0)),
            pl.BlockSpec((PAIR, FRAME, LANES), lambda n: (n, 0, 0)),
            pl.BlockSpec((8 * PAIR, COLS), lambda n: (MSG_W // (8 * PAIR) + n, 0)),
            pl.BlockSpec((8 * PAIR, COLS), lambda n: (MSG_W // (8 * PAIR) + n, 0)),
        ],
        out_specs=[out_spec] * 3,
        out_shape=(struct(COSTS, ROWS, COLS),) * 3,
        scratch_shapes=[
            pltpu.VMEM((N_LAM, LANES), F32),
            pltpu.VMEM((N_LAM + 8, LANES), F32),
            pltpu.VMEM((8 * ITERS, LANES), F32),
            pltpu.VMEM((2, ITERS, 2, ROWS, LANES), F32),
            pltpu.VMEM((ITERS - 1, TILES, FRAME, LANES), F32),
            pltpu.VMEM((TILES, FRAME, LANES), F32),
            pltpu.VMEM((PAIR, TILES, FRAME, LANES), F32),
            pltpu.VMEM((PAIR, TILES, FRAME, LANES), F32),
            pltpu.VMEM((PAIR, ITERS - 1, TILES, FRAME + 16, LANES), F32),
            pltpu.VMEM((PAIR, 3, TILES, FRAME - 8, LANES), F32),
        ],
        compiler_params=pltpu.CompilerParams(
            dimension_semantics=("arbitrary",), vmem_limit_bytes=18 << 20
        ),
        name="adjoint",
    )(all_dots, vecs, links, wet, cost_weights, wside, band_s, band_n)


def solution(mesh):
    return jax.shard_map(
        body,
        mesh=mesh,
        in_specs=(P("lat", "lon"),) * 5 + (P(None, "lat", "lon"),),
        out_specs=(P(None, "lat", "lon"),) * 3,
        check_vma=False,
    )
```

```python
import functools

import jax
import jax.numpy as jnp
from jax import lax
from jax.experimental import pallas as pl
from jax.experimental.pallas import tpu as pltpu
from jax.sharding import PartitionSpec as P

ITERS = 6
COSTS = 8
ROWS = 64
COLS = 256
LANES = 128
TILES = 3
PAIR = 2
DEEP = 13
SLIM = 6
EDGE = 16
FIELDS = 5
FRAME = 80
TALL = 96
MSG_W = FIELDS * EDGE
MSG = MSG_W + COSTS * 8
N_LAM = COSTS * ITERS
N_RHS = N_LAM
N_MAT = N_LAM + ITERS
F32 = jnp.float32
HIGH = lax.Precision.HIGHEST


def lane_index(rows):
    return lax.broadcasted_iota(jnp.int32, (rows, LANES), 1)


def turn(value, amount):
    return pltpu.roll(value, amount % value.shape[1], 1)


def starts(shift):
    wides = [DEEP] * FIELDS + [SLIM] * COSTS
    firsts = [sum(wides[:k]) - (wides[k] if shift else 0) for k in range(len(wides))]
    return list(zip(firsts, wides))


def pack(rows, tiles, shift):
    lane = lane_index(rows)
    out = jnp.zeros((rows, LANES), F32)
    for entry, (at, wide) in zip(tiles, starts(shift)):
        if entry is not None:
            tile, first = entry
            here = (lane >= at) & (lane < at + wide) if at >= 0 else lane >= at + LANES
            out = jnp.where(here, turn(tile, at - first), out)
    return out


def bands_kernel(f, de, dn, st, mask, w, to_north, to_south, whole_mask, sems):
    copies = []
    for side, out in enumerate((to_north, to_south)):
        low = ROWS - EDGE if side == 0 else 0
        rows = pl.ds(low, EDGE)
        for k, field in enumerate((f, de, dn, st)):
            copies.append((field.at[rows, :], out.at[pl.ds(EDGE * k, EDGE), :]))
        copies.append((mask.at[rows, :], whole_mask.at[side]))
        low = ROWS - 8 if side == 0 else 0
        copies.append((w.at[:, pl.ds(low, 8), :], out.at[pl.ds(MSG_W, 8 * COSTS), :].reshape(COSTS, 8, COLS)))
    copies = [
        pltpu.make_async_copy(src, dst, sems.at[i]) for i, (src, dst) in enumerate(copies)
    ]
    for copy in copies:
        copy.start()
    for copy in copies:
        copy.wait()
    to_north[MSG_W - EDGE : MSG_W, :] = whole_mask[0].astype(F32)
    to_south[MSG_W - EDGE : MSG_W, :] = whole_mask[1].astype(F32)


def strips_kernel(f, de, dn, st, mask, w, east, west):
    fields = [f[...], de[...], dn[...], st[...], mask[...].astype(F32)]
    right = [(v[:, LANES:], LANES - DEEP) for v in fields]
    left = [(v[:, :LANES], 0) for v in fields]
    right += [(w[n, :, LANES:], LANES - SLIM) for n in range(COSTS)]
    left += [(w[n, :, :LANES], 0) for n in range(COSTS)]
    east[...] = pack(ROWS, right, True)
    west[...] = pack(ROWS, left, False)


def corners_kernel(east, west, bs, bn, to_east, to_west):
    for own, out, lanes, first in ((east, to_east, slice(LANES, COLS), True), (west, to_west, slice(0, LANES), False)):
        out[EDGE : EDGE + ROWS, :] = own[...]
        for band, low, slim in ((bs, 0, 1), (bn, EDGE + ROWS, 0)):
            for half in range(2):
                tiles = []
                for k in range(FIELDS):
                    at = EDGE * k + 8 * half
                    tiles.append((band[at : at + 8, lanes], LANES - DEEP if first else 0))
                for n in range(COSTS):
                    at = MSG_W + 8 * n
                    entry = (band[at : at + 8, lanes], LANES - SLIM if first else 0)
                    tiles.append(entry if half == slim else None)
                out[low + 8 * half : low + 8 * half + 8, :] = pack(8, tiles, first)


def side_tile(pw, pe, k):
    lane = lane_index(pw.shape[0])
    at, wide = starts(False)[k]
    both = jnp.where((lane >= at) & (lane < at + wide), pe, pw)
    return jnp.where((lane < wide) | (lane >= LANES - wide), turn(both, -at), 0.0)


def east_of(tiles):
    last = lane_index(8) == LANES - 1
    turned = [pltpu.roll(tile, LANES - 1, 1) for tile in tiles]
    return [jnp.where(last, turned[(t + 1) % TILES], turned[t]) for t in range(TILES)]


def west_of(tiles):
    first = lane_index(8) == 0
    turned = [pltpu.roll(tile, 1, 1) for tile in tiles]
    return [jnp.where(first, turned[t - 1], turned[t]) for t in range(TILES)]


def forward_kernel(
    flags, f, de, dn, st, mask, w, ls, ln, sw, se,
    vecs, links, wside, wet, dots,
    raw, north, vec, link, diag, part,
):
    own = (f, de, dn, st, mask)
    blocks = range(TALL // 8)
    tiles = range(TILES)
    for rb in blocks:
        at = 8 + 8 * rb
        src, off = None, 8 * rb - EDGE
        if rb < 2:
            src, off = ls, 8 * rb
        elif rb >= 10:
            src, off = ln, 8 * rb - 80
        pw, pe = sw[8 * rb : 8 * rb + 8, :], se[8 * rb : 8 * rb + 8, :]
        for k in range(FIELDS):
            values = []
            for t in range(2):
                lanes = slice(LANES * t, LANES * (t + 1))
                if src is None:
                    values.append(own[k][off : off + 8, lanes].astype(F32))
                else:
                    values.append(src[EDGE * k + off : EDGE * k + off + 8, lanes])
            values.append(side_tile(pw, pe, k))
            if k == FIELDS - 1 and src is not None:
                inside = flags[0 if rb < 2 else 1]
                values = [inside * value for value in values]
            for t in tiles:
                raw[k, t, at : at + 8, :] = values[t]
        if 1 <= rb < 11:
            for n in range(COSTS):
                wside[n, 8 * rb - 8 : 8 * rb, :] = side_tile(pw, pe, FIELDS + n)
    for rb in blocks:
        here = slice(8 + 8 * rb, 16 + 8 * rb)
        above = slice(9 + 8 * rb, 17 + 8 * rb)
        for t in tiles:
            mn = raw[4, t, here, :] * raw[4, t, above, :]
            north[t, here, :] = raw[2, t, here, :] * mn
            if 2 <= rb < 10 and t < 2:
                wet[1, 8 * rb - 16 : 8 * rb - 8, LANES * t : LANES * (t + 1)] = mn
    for rb in blocks:
        here = slice(8 + 8 * rb, 16 + 8 * rb)
        below = slice(7 + 8 * rb, 15 + 8 * rb)
        m = [raw[4, t, here, :] for t in tiles]
        me = [a * b for a, b in zip(m, east_of(m))]
        ex = [raw[1, t, here, :] * me[t] for t in tiles]
        exw = west_of(ex)
        for t in tiles:
            ey, eys = north[t, here, :], north[t, below, :]
            total = m[t] * raw[3, t, here, :] + 1.0 - m[t] + ex[t] + exw[t] + ey + eys
            inv = 1.0 / total
            twice = inv + inv
            v0 = raw[0, t, here, :] * inv
            vec[0, t, here, :] = v0
            values = [twice * face for face in (ex[t], exw[t], ey, eys)]
            for k in range(4):
                link[k, t, here, :] = values[k]
            if 1 <= rb < 11:
                to = slice(8 * rb - 8, 8 * rb)
                vecs[0, t, to, :] = v0
                vecs[ITERS + 1, t, to, :] = twice
                for k in range(4):
                    links[k, t, to, :] = values[k]
            if 2 <= rb < 10 and t < 2:
                to, lanes = slice(8 * rb - 16, 8 * rb - 8), slice(LANES * t, LANES * (t + 1))
                wet[0, to, lanes] = me[t]
                diag[to, lanes] = total
    for j in range(ITERS):
        for rb in blocks if j < 3 else blocks[1:-1]:
            here = slice(8 + 8 * rb, 16 + 8 * rb)
            above = slice(9 + 8 * rb, 17 + 8 * rb)
            below = slice(7 + 8 * rb, 15 + 8 * rb)
            v = [vec[j, t, here, :] for t in tiles]
            ve, vw = east_of(v), west_of(v)
            for t in tiles:
                new = (
                    link[0, t, here, :] * ve[t]
                    + link[1, t, here, :] * vw[t]
                    + link[2, t, here, :] * vec[j, t, above, :]
                    + link[3, t, here, :] * vec[j, t, below, :]
                )
                new = 0.5 * new if j == 0 else new - vec[j - 1, t, here, :]
                vec[j + 1, t, here, :] = new
                if 1 <= rb < 11:
                    vecs[j + 1, t, 8 * rb - 8 : 8 * rb, :] = new
    count = ITERS + ITERS * (ITERS + 1) // 2
    own_tiles = [(rb, t) for rb in range(ROWS // 8) for t in range(2)]
    sums = [None] * count
    for rb, t in own_tiles:
        here, lanes = slice(8 * rb, 8 * rb + 8), slice(LANES * t, LANES * (t + 1))
        vs = [vec[j, t, 24 + 8 * rb : 32 + 8 * rb, :] for j in range(ITERS + 1)]
        total = diag[here, lanes]
        forcing = f[here, lanes]
        terms = [forcing * vs[j] for j in range(ITERS)]
        for j in range(ITERS):
            turned = vs[1] if j == 0 else 0.5 * (vs[j + 1] + vs[j - 1])
            image = total * (vs[j] - turned)
            terms += [image * vs[i] for i in range(j + 1)]
        sums = [b if a is None else a + b for a, b in zip(sums, terms)]
    part[N_RHS + count :, :] = jnp.zeros((LANES - N_RHS - count, LANES), F32)
    for k in range(count):
        part[N_RHS + k : N_RHS + k + 1, :] = jnp.sum(sums[k], axis=0, keepdims=True)
    for n in range(COSTS):
        sums = [None] * ITERS
        for rb, t in own_tiles:
            weight = w[n, 8 * rb : 8 * rb + 8, LANES * t : LANES * (t + 1)]
            for j in range(ITERS):
                term = weight * vec[j, t, 24 + 8 * rb : 32 + 8 * rb, :]
                sums[j] = term if sums[j] is None else sums[j] + term
        for j in range(ITERS):
            k = COSTS * j + n
            part[k : k + 1, :] = jnp.sum(sums[j], axis=0, keepdims=True)
    row = lax.dot_general(
        jnp.ones((8, LANES), F32), part[...], (((1,), (1,)), ((), ())),
        precision=HIGH, preferred_element_type=F32,
    )
    for at in range(0, dots.shape[0], 8):
        dots[at : at + 8, :] = row


def small_solve(total):
    wide = lambda k: jnp.broadcast_to(total[k : k + 1, :], (8, LANES))
    mat = {}
    k = N_MAT
    for j in range(ITERS):
        for i in range(j + 1):
            mat[j, i] = wide(k)
            k += 1
    low, inv = {}, []
    for j in range(ITERS):
        pivot = mat[j, j]
        for k in range(j):
            pivot = pivot - low[j, k] * mat[j, k]
        inv.append(1.0 / pivot)
        for i in range(j + 1, ITERS):
            entry = mat[i, j]
            for k in range(j):
                entry = entry - low[j, k] * mat[i, k]
            mat[i, j] = entry
            low[i, j] = entry * inv[j]

    def solve(rhs):
        y = []
        for i in range(ITERS):
            t = rhs[i]
            for k in range(i):
                t = t - low[i, k] * y[k]
            y.append(t)
        out = [None] * ITERS
        for i in range(ITERS - 1, -1, -1):
            t = y[i] * inv[i]
            for k in range(i + 1, ITERS):
                t = t - low[k, i] * out[k]
            out[i] = t
        return out

    return (
        solve([wide(N_RHS + i) for i in range(ITERS)]),
        solve([total[COSTS * j : COSTS * (j + 1), :] for j in range(ITERS)]),
    )


def imaged(coef):
    get = lambda k: coef[k] if 0 <= k < ITERS else None
    out = []
    for k in range(ITERS + 1):
        low, mid, high = get(k - 1), get(k), get(k + 1)
        value = jnp.zeros_like(coef[0]) if mid is None else mid + mid
        if low is not None:
            value = value - (low + low if k == 1 else low)
        if high is not None:
            value = value - high
        out.append(value)
    return out


def mixed(factors, values):
    total = None
    for factor, value in zip(factors, values):
        term = factor * value
        total = term if total is None else total + term
    return total


def adjoint_kernel(
    all_dots, vecs, links, wet, w, wside, ws, wn,
    adj, east, north,
    lam, lam2, cs, slope, lag, rs, ys, ss, ps, acc,
):
    n = pl.program_id(0)
    blocks = range(FRAME // 8)
    tiles = range(TILES)
    lanes_of = lambda t: slice(LANES * t, LANES * (t + 1))

    @pl.when(n == 0)
    def _():
        rows = [all_dots[at : at + 8, :] for at in range(0, all_dots.shape[0], 8)]
        while len(rows) > 1:
            rows = [a + b for a, b in zip(rows[::2], rows[1::2])]
        total = lax.dot_general(
            rows[0], jnp.ones((8, LANES), F32), (((0,), (0,)), ((), ())),
            precision=HIGH, preferred_element_type=F32,
        )
        for rb in range(1, 10):
            here = slice(8 * rb, 8 * rb + 8)
            above = slice(8 * rb + 1, 8 * rb + 9)
            to = slice(8 * rb - 8, 8 * rb)
            for j in range(ITERS):
                v = [vecs[j, t, here, :] for t in tiles]
                if j < ITERS - 1:
                    for t in tiles:
                        later = vecs[j + 1, t, here, :]
                        if j > 0:
                            later = 0.5 * (later + vecs[j - 1, t, here, :])
                        lag[j, t, here, :] = later - v[t]
                if rb < 9:
                    ve = east_of(v)
                    for t in range(2):
                        slope[0, j, t, to, :] = v[t] - ve[t]
                        slope[1, j, t, to, :] = v[t] - vecs[j, t, above, :]
        c, weights = small_solve(total)
        for j in range(ITERS):
            lam[8 * j : 8 * j + 8, :] = weights[j]
            cs[8 * j : 8 * j + 8, :] = c[j]
        for k, value in enumerate(imaged(weights)):
            lam2[8 * k : 8 * k + 8, :] = value
        c2 = imaged(c)
        for rb in blocks:
            here = slice(8 * rb, 8 * rb + 8)
            for t in tiles:
                v = [vecs[k, t, here, :] for k in range(ITERS + 1)]
                rs[t, here, :] = v[0] + v[0] - mixed(c2, v)
        for rb in range(ROWS // 8):
            to = slice(8 * rb, 8 * rb + 8)
            for d in range(2):
                for t in range(2):
                    steps = [slope[d, j, t, to, :] for j in range(ITERS)]
                    slope[d, ITERS - 1, t, to, :] = mixed(c, steps)

    pair = range(PAIR)
    spread = lambda ref, k, h: jnp.broadcast_to(ref[pl.ds(8 * k + PAIR * n + h, 1), :], (8, LANES))
    rows = [[spread(lam, j, h) for j in range(ITERS)] for h in pair]
    rows2 = [[spread(lam2, k, h) for k in range(ITERS + 1)] for h in pair]
    last = ITERS - 1
    c_last = cs[8 * last : 8 * last + 8, :]
    lagged = lambda rb: slice(8 * rb - 8, 8 * rb)
    for rb in blocks:
        at = 8 + 8 * rb
        here = slice(8 * rb, 8 * rb + 8)
        for t in tiles:
            v = [vecs[k, t, here, :] for k in range(ITERS + 1)]
            scale, res = vecs[ITERS + 1, t, here, :], rs[t, here, :]
            for h in pair:
                if t == 2:
                    weight = wside[h, here, :]
                elif rb == 0:
                    weight = ws[8 * h : 8 * h + 8, lanes_of(t)]
                elif rb == 9:
                    weight = wn[8 * h : 8 * h + 8, lanes_of(t)]
                else:
                    weight = w[h, lagged(rb), lanes_of(t)]
                s = scale * weight - mixed(rows2[h], v)
                ss[h, t, here, :] = s
                ps[h, last - 1, t, at : at + 8, :] = c_last * s + rows[h][last] * res
                if rb >= 1:
                    ys[h, t, here, :] = mixed(rows[h], v)
    for rb in range(1, 9):
        here = slice(8 * rb, 8 * rb + 8)
        above = slice(8 * rb + 1, 8 * rb + 9)
        to = lagged(rb)
        for h in pair:
            y = [ys[h, t, here, :] for t in tiles]
            ye = east_of(y)
            for t in range(2):
                acc[h, 0, t, to, :] = (y[t] - ye[t]) * slope[0, last, t, to, :]
                acc[h, 1, t, to, :] = (y[t] - ys[h, t, above, :]) * slope[1, last, t, to, :]
    for j in range(ITERS - 2, -1, -1):
        c_j = cs[8 * j : 8 * j + 8, :]
        for rb in blocks:
            if j == 0 and rb == 0:
                continue
            at = 8 + 8 * rb
            here = slice(8 * rb, 8 * rb + 8)
            p = [[ps[h, j, t, at : at + 8, :] for t in tiles] for h in pair]
            pe, pw = [east_of(q) for q in p], [west_of(q) for q in p]
            for t in tiles:
                link = [links[k, t, here, :] for k in range(4)]
                res = rs[t, here, :]
                if rb >= 1:
                    late = lag[j, t, here, :]
                    if j == 0:
                        v0 = vecs[0, t, here, :]
                inside = 1 <= rb < 9 and t < 2
                if inside:
                    to = lagged(rb)
                    slope_e, slope_n = slope[0, j, t, to, :], slope[1, j, t, to, :]
                for h in pair:
                    here_p = p[h][t]
                    pn = ps[h, j, t, at + 1 : at + 9, :]
                    bar = (
                        link[0] * pe[h][t] + link[1] * pw[h][t]
                        + link[2] * pn + link[3] * ps[h, j, t, at - 1 : at + 7, :]
                    ) + (c_j * ss[h, t, here, :] + rows[h][j] * res)
                    if j < ITERS - 2:
                        bar = bar - ps[h, j + 1, t, at : at + 8, :]
                    if j == 1:
                        bar = 0.5 * bar
                    if j > 0:
                        ps[h, j - 1, t, at : at + 8, :] = bar
                    if rb >= 1:
                        d = here_p * late
                        if j < ITERS - 2:
                            d = acc[h, 2, t, lagged(rb), :] + d
                        if j == 0:
                            g = 0.5 * bar
                            d = d + g * v0
                        acc[h, 2, t, lagged(rb), :] = d
                    if inside:
                        acc[h, 0, t, to, :] = acc[h, 0, t, to, :] + (here_p - pe[h][t]) * slope_e
                        acc[h, 1, t, to, :] = acc[h, 1, t, to, :] + (here_p - pn) * slope_n
                        if j == 0:
                            adj[h, to, lanes_of(t)] = ys[h, t, here, :] + g
    for rb in range(ROWS // 8):
        to = slice(8 * rb, 8 * rb + 8)
        for h in pair:
            d = [acc[h, 2, t, to, :] for t in tiles]
            de = east_of(d)
            for t in range(2):
                above = acc[h, 2, t, 8 * rb + 1 : 8 * rb + 9, :]
                east[h, to, lanes_of(t)] = -wet[0, to, lanes_of(t)] * (acc[h, 0, t, to, :] + d[t] + de[t])
                north[h, to, lanes_of(t)] = -wet[1, to, lanes_of(t)] * (acc[h, 1, t, to, :] + d[t] + above)


def ring(axis, steps):
    count = lax.axis_size(axis)
    return [(source, (source + steps) % count) for source in range(count)]


def struct(*shape):
    return jax.ShapeDtypeStruct(shape, F32)


def whole():
    return pl.BlockSpec(memory_space=pltpu.VMEM)


def body(forcing, depth_east, depth_north, surface_term, ocean_mask, cost_weights):
    args = (forcing, depth_east, depth_north, surface_term, ocean_mask, cost_weights)
    lats = lax.axis_size("lat")
    devices = lats * lax.axis_size("lon")
    small = pltpu.CompilerParams(vmem_limit_bytes=4 << 20)
    to_north, to_south = pl.pallas_call(
        bands_kernel,
        in_specs=[pl.BlockSpec(memory_space=pltpu.HBM)] * 6,
        out_specs=[whole()] * 2,
        out_shape=(struct(MSG, COLS),) * 2,
        scratch_shapes=[
            pltpu.VMEM((2, EDGE, COLS), jnp.int32),
            pltpu.SemaphoreType.DMA((2 * (FIELDS + 1),)),
        ],
        compiler_params=small,
        name="bands",
    )(*[pltpu.with_memory_space_constraint(arg, pltpu.HBM) for arg in args])
    band_s = lax.ppermute(to_north, "lat", ring("lat", 1))
    band_n = lax.ppermute(to_south, "lat", ring("lat", -1))
    east, west = pl.pallas_call(
        strips_kernel,
        in_specs=[whole()] * 6,
        out_specs=[whole()] * 2,
        out_shape=(struct(ROWS, LANES),) * 2,
        compiler_params=small,
        name="strips",
    )(*args)
    to_east, to_west = pl.pallas_call(
        corners_kernel,
        in_specs=[whole()] * 4,
        out_specs=[whole()] * 2,
        out_shape=(struct(TALL, LANES),) * 2,
        compiler_params=small,
        name="corners",
    )(east, west, band_s, band_n)
    side_w = lax.ppermute(to_east, "lon", ring("lon", 1))
    side_e = lax.ppermute(to_west, "lon", ring("lon", -1))
    row = lax.axis_index("lat")
    flags = jnp.stack([row > 0, row < lats - 1, row > 0, row > 0]).astype(F32)
    flags = jnp.broadcast_to(flags[:, None, None], (4, 8, LANES))
    vecs, links, wside, wet, dots = pl.pallas_call(
        forward_kernel,
        in_specs=[whole()] * 11,
        out_specs=[whole()] * 5,
        out_shape=(
            struct(ITERS + 2, TILES, FRAME, LANES), struct(4, TILES, FRAME, LANES),
            struct(COSTS, FRAME, LANES),
            struct(2, ROWS, COLS), struct(devices, LANES),
        ),
        scratch_shapes=[
            pltpu.VMEM((FIELDS, TILES, TALL + 16, LANES), F32),
            pltpu.VMEM((TILES, TALL + 16, LANES), F32),
            pltpu.VMEM((ITERS + 1, TILES, TALL + 16, LANES), F32),
            pltpu.VMEM((4, TILES, TALL + 16, LANES), F32),
            pltpu.VMEM((ROWS, COLS), F32),
            pltpu.VMEM((LANES, LANES), F32),
        ],
        compiler_params=pltpu.CompilerParams(vmem_limit_bytes=14 << 20),
        name="forward",
    )(flags, *args, band_s, band_n, side_w, side_e)
    all_dots = lax.all_to_all(dots, ("lat", "lon"), 0, 0, tiled=True)
    out_spec = pl.BlockSpec((PAIR, ROWS, COLS), lambda n: (n, 0, 0))
    return pl.pallas_call(
        adjoint_kernel,
        grid=(COSTS // PAIR,),
        in_specs=[
            whole(),
            whole(),
            whole(),
            whole(),
            pl.BlockSpec((PAIR, ROWS, COLS), lambda n: (n, 0, 0)),
            pl.BlockSpec((PAIR, FRAME, LANES), lambda n: (n, 0, 0)),
            pl.BlockSpec((8 * PAIR, COLS), lambda n: (MSG_W // (8 * PAIR) + n, 0)),
            pl.BlockSpec((8 * PAIR, COLS), lambda n: (MSG_W // (8 * PAIR) + n, 0)),
        ],
        out_specs=[out_spec] * 3,
        out_shape=(struct(COSTS, ROWS, COLS),) * 3,
        scratch_shapes=[
            pltpu.VMEM((N_LAM, LANES), F32),
            pltpu.VMEM((N_LAM + 8, LANES), F32),
            pltpu.VMEM((8 * ITERS, LANES), F32),
            pltpu.VMEM((2, ITERS, 2, ROWS, LANES), F32),
            pltpu.VMEM((ITERS - 1, TILES, FRAME, LANES), F32),
            pltpu.VMEM((TILES, FRAME, LANES), F32),
            pltpu.VMEM((PAIR, TILES, FRAME, LANES), F32),
            pltpu.VMEM((PAIR, TILES, FRAME, LANES), F32),
            pltpu.VMEM((PAIR, ITERS - 1, TILES, FRAME + 16, LANES), F32),
            pltpu.VMEM((PAIR, 3, TILES, FRAME - 8, LANES), F32),
        ],
        compiler_params=pltpu.CompilerParams(
            dimension_semantics=("arbitrary",), vmem_limit_bytes=18 << 20
        ),
        name="adjoint",
    )(all_dots, vecs, links, wet, cost_weights, wside, band_s, band_n)


def solution(mesh):
    return jax.shard_map(
        body,
        mesh=mesh,
        in_specs=(P("lat", "lon"),) * 5 + (P(None, "lat", "lon"),),
        out_specs=(P(None, "lat", "lon"),) * 3,
        check_vma=False,
    )
```

```python
import functools

import jax
import jax.numpy as jnp
from jax import lax
from jax.experimental import pallas as pl
from jax.experimental.pallas import tpu as pltpu
from jax.sharding import PartitionSpec as P

ITERS = 6
COSTS = 8
ROWS = 64
COLS = 256
LANES = 128
TILES = 3
PAIR = 2
DEEP = 13
SLIM = 6
EDGE = 16
FIELDS = 5
FRAME = 80
TALL = 96
MSG_W = FIELDS * EDGE
MSG = MSG_W + COSTS * 8
N_LAM = COSTS * ITERS
N_RHS = N_LAM
N_MAT = N_LAM + ITERS
F32 = jnp.float32
HIGH = lax.Precision.HIGHEST


def lane_index(rows):
    return lax.broadcasted_iota(jnp.int32, (rows, LANES), 1)


def turn(value, amount):
    return pltpu.roll(value, amount % value.shape[1], 1)


def starts(shift):
    wides = [DEEP] * FIELDS + [SLIM] * COSTS
    firsts = [sum(wides[:k]) - (wides[k] if shift else 0) for k in range(len(wides))]
    return list(zip(firsts, wides))


def pack(rows, tiles, shift):
    lane = lane_index(rows)
    out = jnp.zeros((rows, LANES), F32)
    for entry, (at, wide) in zip(tiles, starts(shift)):
        if entry is not None:
            tile, first = entry
            here = (lane >= at) & (lane < at + wide) if at >= 0 else lane >= at + LANES
            out = jnp.where(here, turn(tile, at - first), out)
    return out


def bands_kernel(f, de, dn, st, mask, w, to_north, to_south, whole_mask, sems):
    copies = []
    for side, out in enumerate((to_north, to_south)):
        low = ROWS - EDGE if side == 0 else 0
        rows = pl.ds(low, EDGE)
        for k, field in enumerate((f, de, dn, st)):
            copies.append((field.at[rows, :], out.at[pl.ds(EDGE * k, EDGE), :]))
        copies.append((mask.at[rows, :], whole_mask.at[side]))
        low = ROWS - 8 if side == 0 else 0
        copies.append((w.at[:, pl.ds(low, 8), :], out.at[pl.ds(MSG_W, 8 * COSTS), :].reshape(COSTS, 8, COLS)))
    copies = [
        pltpu.make_async_copy(src, dst, sems.at[i]) for i, (src, dst) in enumerate(copies)
    ]
    for copy in copies:
        copy.start()
    for copy in copies:
        copy.wait()
    to_north[MSG_W - EDGE : MSG_W, :] = whole_mask[0].astype(F32)
    to_south[MSG_W - EDGE : MSG_W, :] = whole_mask[1].astype(F32)


def strips_kernel(f, de, dn, st, mask, w, east, west):
    fields = [f[...], de[...], dn[...], st[...], mask[...].astype(F32)]
    right = [(v[:, LANES:], LANES - DEEP) for v in fields]
    left = [(v[:, :LANES], 0) for v in fields]
    right += [(w[n, :, LANES:], LANES - SLIM) for n in range(COSTS)]
    left += [(w[n, :, :LANES], 0) for n in range(COSTS)]
    east[...] = pack(ROWS, right, True)
    west[...] = pack(ROWS, left, False)


def corners_kernel(east, west, bs, bn, to_east, to_west):
    for own, out, lanes, first in ((east, to_east, slice(LANES, COLS), True), (west, to_west, slice(0, LANES), False)):
        out[EDGE : EDGE + ROWS, :] = own[...]
        for band, low, slim in ((bs, 0, 1), (bn, EDGE + ROWS, 0)):
            for half in range(2):
                tiles = []
                for k in range(FIELDS):
                    at = EDGE * k + 8 * half
                    tiles.append((band[at : at + 8, lanes], LANES - DEEP if first else 0))
                for n in range(COSTS):
                    at = MSG_W + 8 * n
                    entry = (band[at : at + 8, lanes], LANES - SLIM if first else 0)
                    tiles.append(entry if half == slim else None)
                out[low + 8 * half : low + 8 * half + 8, :] = pack(8, tiles, first)


def side_tile(pw, pe, k):
    lane = lane_index(pw.shape[0])
    at, wide = starts(False)[k]
    both = jnp.where((lane >= at) & (lane < at + wide), pe, pw)
    return jnp.where((lane < wide) | (lane >= LANES - wide), turn(both, -at), 0.0)


def east_of(tiles):
    last = lane_index(8) == LANES - 1
    turned = [pltpu.roll(tile, LANES - 1, 1) for tile in tiles]
    return [jnp.where(last, turned[(t + 1) % TILES], turned[t]) for t in range(TILES)]


def west_of(tiles):
    first = lane_index(8) == 0
    turned = [pltpu.roll(tile, 1, 1) for tile in tiles]
    return [jnp.where(first, turned[t - 1], turned[t]) for t in range(TILES)]


def forward_kernel(
    flags, f, de, dn, st, mask, w, ls, ln, sw, se,
    vecs, links, wside, wet, dots,
    raw, north, vec, link, diag, part,
):
    own = (f, de, dn, st, mask)
    blocks = range(TALL // 8)
    tiles = range(TILES)
    for rb in blocks:
        at = 8 + 8 * rb
        src, off = None, 8 * rb - EDGE
        if rb < 2:
            src, off = ls, 8 * rb
        elif rb >= 10:
            src, off = ln, 8 * rb - 80
        pw, pe = sw[8 * rb : 8 * rb + 8, :], se[8 * rb : 8 * rb + 8, :]
        for k in range(FIELDS):
            values = []
            for t in range(2):
                lanes = slice(LANES * t, LANES * (t + 1))
                if src is None:
                    values.append(own[k][off : off + 8, lanes].astype(F32))
                else:
                    values.append(src[EDGE * k + off : EDGE * k + off + 8, lanes])
            values.append(side_tile(pw, pe, k))
            if k == FIELDS - 1 and src is not None:
                inside = flags[0 if rb < 2 else 1]
                values = [inside * value for value in values]
            for t in tiles:
                raw[k, t, at : at + 8, :] = values[t]
        if 1 <= rb < 11:
            for n in range(COSTS):
                wside[n, 8 * rb - 8 : 8 * rb, :] = side_tile(pw, pe, FIELDS + n)
    for rb in blocks:
        here = slice(8 + 8 * rb, 16 + 8 * rb)
        above = slice(9 + 8 * rb, 17 + 8 * rb)
        for t in tiles:
            mn = raw[4, t, here, :] * raw[4, t, above, :]
            north[t, here, :] = raw[2, t, here, :] * mn
            if 2 <= rb < 10 and t < 2:
                wet[1, 8 * rb - 16 : 8 * rb - 8, LANES * t : LANES * (t + 1)] = mn
    for rb in blocks:
        here = slice(8 + 8 * rb, 16 + 8 * rb)
        below = slice(7 + 8 * rb, 15 + 8 * rb)
        m = [raw[4, t, here, :] for t in tiles]
        me = [a * b for a, b in zip(m, east_of(m))]
        ex = [raw[1, t, here, :] * me[t] for t in tiles]
        exw = west_of(ex)
        for t in tiles:
            ey, eys = north[t, here, :], north[t, below, :]
            total = m[t] * raw[3, t, here, :] + 1.0 - m[t] + ex[t] + exw[t] + ey + eys
            inv = 1.0 / total
            twice = inv + inv
            v0 = raw[0, t, here, :] * inv
            vec[0, t, here, :] = v0
            values = [twice * face for face in (ex[t], exw[t], ey, eys)]
            for k in range(4):
                link[k, t, here, :] = values[k]
            if 1 <= rb < 11:
                to = slice(8 * rb - 8, 8 * rb)
                vecs[0, t, to, :] = v0
                vecs[ITERS + 1, t, to, :] = twice
                for k in range(4):
                    links[k, t, to, :] = values[k]
            if 2 <= rb < 10 and t < 2:
                to, lanes = slice(8 * rb - 16, 8 * rb - 8), slice(LANES * t, LANES * (t + 1))
                wet[0, to, lanes] = me[t]
                diag[to, lanes] = total
    for j in range(ITERS):
        for rb in blocks if j < 3 else blocks[1:-1]:
            here = slice(8 + 8 * rb, 16 + 8 * rb)
            above = slice(9 + 8 * rb, 17 + 8 * rb)
            below = slice(7 + 8 * rb, 15 + 8 * rb)
            v = [vec[j, t, here, :] for t in tiles]
            ve, vw = east_of(v), west_of(v)
            for t in tiles:
                new = (
                    link[0, t, here, :] * ve[t]
                    + link[1, t, here, :] * vw[t]
                    + link[2, t, here, :] * vec[j, t, above, :]
                    + link[3, t, here, :] * vec[j, t, below, :]
                )
                new = 0.5 * new if j == 0 else new - vec[j - 1, t, here, :]
                vec[j + 1, t, here, :] = new
                if 1 <= rb < 11:
                    vecs[j + 1, t, 8 * rb - 8 : 8 * rb, :] = new
    count = ITERS + ITERS * (ITERS + 1) // 2
    own_tiles = [(rb, t) for rb in range(ROWS // 8) for t in range(2)]
    sums = [None] * count
    for rb, t in own_tiles:
        here, lanes = slice(8 * rb, 8 * rb + 8), slice(LANES * t, LANES * (t + 1))
        vs = [vec[j, t, 24 + 8 * rb : 32 + 8 * rb, :] for j in range(ITERS + 1)]
        total = diag[here, lanes]
        forcing = f[here, lanes]
        terms = [forcing * vs[j] for j in range(ITERS)]
        for j in range(ITERS):
            turned = vs[1] if j == 0 else 0.5 * (vs[j + 1] + vs[j - 1])
            image = total * (vs[j] - turned)
            terms += [image * vs[i] for i in range(j + 1)]
        sums = [b if a is None else a + b for a, b in zip(sums, terms)]
    part[N_RHS + count :, :] = jnp.zeros((LANES - N_RHS - count, LANES), F32)
    for k in range(count):
        part[N_RHS + k : N_RHS + k + 1, :] = jnp.sum(sums[k], axis=0, keepdims=True)
    for n in range(COSTS):
        sums = [None] * ITERS
        for rb, t in own_tiles:
            weight = w[n, 8 * rb : 8 * rb + 8, LANES * t : LANES * (t + 1)]
            for j in range(ITERS):
                term = weight * vec[j, t, 24 + 8 * rb : 32 + 8 * rb, :]
                sums[j] = term if sums[j] is None else sums[j] + term
        for j in range(ITERS):
            k = COSTS * j + n
            part[k : k + 1, :] = jnp.sum(sums[j], axis=0, keepdims=True)
    row = lax.dot_general(
        jnp.ones((8, LANES), F32), part[...], (((1,), (1,)), ((), ())),
        precision=HIGH, preferred_element_type=F32,
    )
    for at in range(0, dots.shape[0], 8):
        dots[at : at + 8, :] = row


def small_solve(total):
    wide = lambda k: jnp.broadcast_to(total[k : k + 1, :], (8, LANES))
    mat = {}
    k = N_MAT
    for j in range(ITERS):
        for i in range(j + 1):
            mat[j, i] = wide(k)
            k += 1
    low, inv = {}, []
    for j in range(ITERS):
        pivot = mat[j, j]
        for k in range(j):
            pivot = pivot - low[j, k] * mat[j, k]
        inv.append(1.0 / pivot)
        for i in range(j + 1, ITERS):
            entry = mat[i, j]
            for k in range(j):
                entry = entry - low[j, k] * mat[i, k]
            mat[i, j] = entry
            low[i, j] = entry * inv[j]

    def solve(rhs):
        y = []
        for i in range(ITERS):
            t = rhs[i]
            for k in range(i):
                t = t - low[i, k] * y[k]
            y.append(t)
        out = [None] * ITERS
        for i in range(ITERS - 1, -1, -1):
            t = y[i] * inv[i]
            for k in range(i + 1, ITERS):
                t = t - low[k, i] * out[k]
            out[i] = t
        return out

    return (
        solve([wide(N_RHS + i) for i in range(ITERS)]),
        solve([total[COSTS * j : COSTS * (j + 1), :] for j in range(ITERS)]),
    )


def imaged(coef):
    get = lambda k: coef[k] if 0 <= k < ITERS else None
    out = []
    for k in range(ITERS + 1):
        low, mid, high = get(k - 1), get(k), get(k + 1)
        value = jnp.zeros_like(coef[0]) if mid is None else mid + mid
        if low is not None:
            value = value - (low + low if k == 1 else low)
        if high is not None:
            value = value - high
        out.append(value)
    return out


def mixed(factors, values):
    total = None
    for factor, value in zip(factors, values):
        term = factor * value
        total = term if total is None else total + term
    return total


def adjoint_kernel(
    all_dots, vecs, links, wet, w, wside, ws, wn,
    adj, east, north,
    lam, lam2, cs, slope, lag, rs, ys, ss, ps, acc,
):
    n = pl.program_id(0)
    blocks = range(FRAME // 8)
    tiles = range(TILES)
    lanes_of = lambda t: slice(LANES * t, LANES * (t + 1))

    @pl.when(n == 0)
    def _():
        rows = [all_dots[at : at + 8, :] for at in range(0, all_dots.shape[0], 8)]
        while len(rows) > 1:
            rows = [a + b for a, b in zip(rows[::2], rows[1::2])]
        total, rest = None, rows[0]
        for _ in range(3):
            piece = rest.astype(jnp.bfloat16)
            rest = rest - piece.astype(F32)
            term = lax.dot_general(
                piece, jnp.ones((8, LANES), jnp.bfloat16), (((0,), (0,)), ((), ())),
                preferred_element_type=F32,
            )
            total = term if total is None else total + term
        for rb in range(1, 10):
            here = slice(8 * rb, 8 * rb + 8)
            above = slice(8 * rb + 1, 8 * rb + 9)
            to = slice(8 * rb - 8, 8 * rb)
            for j in range(ITERS):
                v = [vecs[j, t, here, :] for t in tiles]
                if j < ITERS - 1:
                    for t in tiles:
                        later = vecs[j + 1, t, here, :]
                        if j > 0:
                            later = 0.5 * (later + vecs[j - 1, t, here, :])
                        lag[j, t, here, :] = later - v[t]
                if rb < 9:
                    ve = east_of(v)
                    for t in range(2):
                        slope[0, j, t, to, :] = v[t] - ve[t]
                        slope[1, j, t, to, :] = v[t] - vecs[j, t, above, :]
        c, weights = small_solve(total)
        for j in range(ITERS):
            lam[8 * j : 8 * j + 8, :] = weights[j]
            cs[8 * j : 8 * j + 8, :] = c[j]
        for k, value in enumerate(imaged(weights)):
            lam2[8 * k : 8 * k + 8, :] = value
        c2 = imaged(c)
        for rb in blocks:
            here = slice(8 * rb, 8 * rb + 8)
            for t in tiles:
                v = [vecs[k, t, here, :] for k in range(ITERS + 1)]
                rs[t, here, :] = v[0] + v[0] - mixed(c2, v)
        for rb in range(ROWS // 8):
            to = slice(8 * rb, 8 * rb + 8)
            for d in range(2):
                for t in range(2):
                    steps = [slope[d, j, t, to, :] for j in range(ITERS)]
                    slope[d, ITERS - 1, t, to, :] = mixed(c, steps)

    pair = range(PAIR)
    spread = lambda ref, k, h: jnp.broadcast_to(ref[pl.ds(8 * k + PAIR * n + h, 1), :], (8, LANES))
    rows = [[spread(lam, j, h) for j in range(ITERS)] for h in pair]
    rows2 = [[spread(lam2, k, h) for k in range(ITERS + 1)] for h in pair]
    last = ITERS - 1
    c_last = cs[8 * last : 8 * last + 8, :]
    lagged = lambda rb: slice(8 * rb - 8, 8 * rb)
    for rb in blocks:
        at = 8 + 8 * rb
        here = slice(8 * rb, 8 * rb + 8)
        for t in tiles:
            v = [vecs[k, t, here, :] for k in range(ITERS + 1)]
            scale, res = vecs[ITERS + 1, t, here, :], rs[t, here, :]
            for h in pair:
                if t == 2:
                    weight = wside[h, here, :]
                elif rb == 0:
                    weight = ws[8 * h : 8 * h + 8, lanes_of(t)]
                elif rb == 9:
                    weight = wn[8 * h : 8 * h + 8, lanes_of(t)]
                else:
                    weight = w[h, lagged(rb), lanes_of(t)]
                s = scale * weight - mixed(rows2[h], v)
                ss[h, t, here, :] = s
                ps[h, last - 1, t, at : at + 8, :] = c_last * s + rows[h][last] * res
                if rb >= 1:
                    ys[h, t, here, :] = mixed(rows[h], v)
    for rb in range(1, 9):
        here = slice(8 * rb, 8 * rb + 8)
        above = slice(8 * rb + 1, 8 * rb + 9)
        to = lagged(rb)
        for h in pair:
            y = [ys[h, t, here, :] for t in tiles]
            ye = east_of(y)
            for t in range(2):
                acc[h, 0, t, to, :] = (y[t] - ye[t]) * slope[0, last, t, to, :]
                acc[h, 1, t, to, :] = (y[t] - ys[h, t, above, :]) * slope[1, last, t, to, :]
    for j in range(ITERS - 2, -1, -1):
        c_j = cs[8 * j : 8 * j + 8, :]
        for rb in blocks:
            if j == 0 and rb == 0:
                continue
            at = 8 + 8 * rb
            here = slice(8 * rb, 8 * rb + 8)
            p = [[ps[h, j, t, at : at + 8, :] for t in tiles] for h in pair]
            pe, pw = [east_of(q) for q in p], [west_of(q) for q in p]
            for t in tiles:
                link = [links[k, t, here, :] for k in range(4)]
                res = rs[t, here, :]
                if rb >= 1:
                    late = lag[j, t, here, :]
                    if j == 0:
                        v0 = vecs[0, t, here, :]
                inside = 1 <= rb < 9 and t < 2
                if inside:
                    to = lagged(rb)
                    slope_e, slope_n = slope[0, j, t, to, :], slope[1, j, t, to, :]
                for h in pair:
                    here_p = p[h][t]
                    pn = ps[h, j, t, at + 1 : at + 9, :]
                    bar = (
                        link[0] * pe[h][t] + link[1] * pw[h][t]
                        + link[2] * pn + link[3] * ps[h, j, t, at - 1 : at + 7, :]
                    ) + (c_j * ss[h, t, here, :] + rows[h][j] * res)
                    if j < ITERS - 2:
                        bar = bar - ps[h, j + 1, t, at : at + 8, :]
                    if j == 1:
                        bar = 0.5 * bar
                    if j > 0:
                        ps[h, j - 1, t, at : at + 8, :] = bar
                    if rb >= 1:
                        d = here_p * late
                        if j < ITERS - 2:
                            d = acc[h, 2, t, lagged(rb), :] + d
                        if j == 0:
                            g = 0.5 * bar
                            d = d + g * v0
                        acc[h, 2, t, lagged(rb), :] = d
                    if inside:
                        acc[h, 0, t, to, :] = acc[h, 0, t, to, :] + (here_p - pe[h][t]) * slope_e
                        acc[h, 1, t, to, :] = acc[h, 1, t, to, :] + (here_p - pn) * slope_n
                        if j == 0:
                            adj[h, to, lanes_of(t)] = ys[h, t, here, :] + g
    for rb in range(ROWS // 8):
        to = slice(8 * rb, 8 * rb + 8)
        for h in pair:
            d = [acc[h, 2, t, to, :] for t in tiles]
            de = east_of(d)
            for t in range(2):
                above = acc[h, 2, t, 8 * rb + 1 : 8 * rb + 9, :]
                east[h, to, lanes_of(t)] = -wet[0, to, lanes_of(t)] * (acc[h, 0, t, to, :] + d[t] + de[t])
                north[h, to, lanes_of(t)] = -wet[1, to, lanes_of(t)] * (acc[h, 1, t, to, :] + d[t] + above)


def ring(axis, steps):
    count = lax.axis_size(axis)
    return [(source, (source + steps) % count) for source in range(count)]


def struct(*shape):
    return jax.ShapeDtypeStruct(shape, F32)


def whole():
    return pl.BlockSpec(memory_space=pltpu.VMEM)


def body(forcing, depth_east, depth_north, surface_term, ocean_mask, cost_weights):
    args = (forcing, depth_east, depth_north, surface_term, ocean_mask, cost_weights)
    lats = lax.axis_size("lat")
    devices = lats * lax.axis_size("lon")
    small = pltpu.CompilerParams(vmem_limit_bytes=4 << 20)
    to_north, to_south = pl.pallas_call(
        bands_kernel,
        in_specs=[pl.BlockSpec(memory_space=pltpu.HBM)] * 6,
        out_specs=[whole()] * 2,
        out_shape=(struct(MSG, COLS),) * 2,
        scratch_shapes=[
            pltpu.VMEM((2, EDGE, COLS), jnp.int32),
            pltpu.SemaphoreType.DMA((2 * (FIELDS + 1),)),
        ],
        compiler_params=small,
        name="bands",
    )(*[pltpu.with_memory_space_constraint(arg, pltpu.HBM) for arg in args])
    band_s = lax.ppermute(to_north, "lat", ring("lat", 1))
    band_n = lax.ppermute(to_south, "lat", ring("lat", -1))
    east, west = pl.pallas_call(
        strips_kernel,
        in_specs=[whole()] * 6,
        out_specs=[whole()] * 2,
        out_shape=(struct(ROWS, LANES),) * 2,
        compiler_params=small,
        name="strips",
    )(*args)
    to_east, to_west = pl.pallas_call(
        corners_kernel,
        in_specs=[whole()] * 4,
        out_specs=[whole()] * 2,
        out_shape=(struct(TALL, LANES),) * 2,
        compiler_params=small,
        name="corners",
    )(east, west, band_s, band_n)
    side_w = lax.ppermute(to_east, "lon", ring("lon", 1))
    side_e = lax.ppermute(to_west, "lon", ring("lon", -1))
    row = lax.axis_index("lat")
    flags = jnp.stack([row > 0, row < lats - 1, row > 0, row > 0]).astype(F32)
    flags = jnp.broadcast_to(flags[:, None, None], (4, 8, LANES))
    vecs, links, wside, wet, dots = pl.pallas_call(
        forward_kernel,
        in_specs=[whole()] * 11,
        out_specs=[whole()] * 5,
        out_shape=(
            struct(ITERS + 2, TILES, FRAME, LANES), struct(4, TILES, FRAME, LANES),
            struct(COSTS, FRAME, LANES),
            struct(2, ROWS, COLS), struct(devices, LANES),
        ),
        scratch_shapes=[
            pltpu.VMEM((FIELDS, TILES, TALL + 16, LANES), F32),
            pltpu.VMEM((TILES, TALL + 16, LANES), F32),
            pltpu.VMEM((ITERS + 1, TILES, TALL + 16, LANES), F32),
            pltpu.VMEM((4, TILES, TALL + 16, LANES), F32),
            pltpu.VMEM((ROWS, COLS), F32),
            pltpu.VMEM((LANES, LANES), F32),
        ],
        compiler_params=pltpu.CompilerParams(vmem_limit_bytes=14 << 20),
        name="forward",
    )(flags, *args, band_s, band_n, side_w, side_e)
    all_dots = lax.all_to_all(dots, ("lat", "lon"), 0, 0, tiled=True)
    out_spec = pl.BlockSpec((PAIR, ROWS, COLS), lambda n: (n, 0, 0))
    return pl.pallas_call(
        adjoint_kernel,
        grid=(COSTS // PAIR,),
        in_specs=[
            whole(),
            whole(),
            whole(),
            whole(),
            pl.BlockSpec((PAIR, ROWS, COLS), lambda n: (n, 0, 0)),
            pl.BlockSpec((PAIR, FRAME, LANES), lambda n: (n, 0, 0)),
            pl.BlockSpec((8 * PAIR, COLS), lambda n: (MSG_W // (8 * PAIR) + n, 0)),
            pl.BlockSpec((8 * PAIR, COLS), lambda n: (MSG_W // (8 * PAIR) + n, 0)),
        ],
        out_specs=[out_spec] * 3,
        out_shape=(struct(COSTS, ROWS, COLS),) * 3,
        scratch_shapes=[
            pltpu.VMEM((N_LAM, LANES), F32),
            pltpu.VMEM((N_LAM + 8, LANES), F32),
            pltpu.VMEM((8 * ITERS, LANES), F32),
            pltpu.VMEM((2, ITERS, 2, ROWS, LANES), F32),
            pltpu.VMEM((ITERS - 1, TILES, FRAME, LANES), F32),
            pltpu.VMEM((TILES, FRAME, LANES), F32),
            pltpu.VMEM((PAIR, TILES, FRAME, LANES), F32),
            pltpu.VMEM((PAIR, TILES, FRAME, LANES), F32),
            pltpu.VMEM((PAIR, ITERS - 1, TILES, FRAME + 16, LANES), F32),
            pltpu.VMEM((PAIR, 3, TILES, FRAME - 8, LANES), F32),
        ],
        compiler_params=pltpu.CompilerParams(
            dimension_semantics=("arbitrary",), vmem_limit_bytes=18 << 20
        ),
        name="adjoint",
    )(all_dots, vecs, links, wet, cost_weights, wside, band_s, band_n)


def solution(mesh):
    return jax.shard_map(
        body,
        mesh=mesh,
        in_specs=(P("lat", "lon"),) * 5 + (P(None, "lat", "lon"),),
        out_specs=(P(None, "lat", "lon"),) * 3,
        check_vma=False,
    )
```
